256 devices in a mesh: first: 16 (over y, x), second: 16 (over z, core).
Axes of the slice: x: 4, y: 4, z: 8, core: 2. Of those that a mesh axis runs over, the one named last changes fastest.
Arguments:
- pair_state: bfloat16 [768, 768, 128], P('first', 'second'), may hold values from -6 to 6
- in_gain: float32 [128], replicated, may hold values from 0.25 to 1.75
- left_weight: bfloat16 [128, 128], replicated, may hold values from -0.5 to 0.5
- right_weight: bfloat16 [128, 128], replicated, may hold values from -0.5 to 0.5
- mid_gain: float32 [128], replicated, may hold values from 0.25 to 1.75
- out_weight: bfloat16 [128, 128], replicated, may hold values from -0.5 to 0.5
- out_gate: bfloat16 [128, 128], replicated, may hold values from -0.5 to 0.5
Outputs:
- triangle_out: bfloat16 [768, 768, 128], P('first', 'second')
The draws below stay inside these ranges and needn't reach their ends.
All inputs are finite; a program needn't handle non-finite values.
Results may differ from the reference program's by a relative error of at most 0.015.
Values may be sent and summed in bfloat16 or wider, within the bound.
A program may use at most 64 MiB of HBM per device.

```python
import jax
import jax.numpy as jnp
from jax import lax

RESIDUES = 768
PAIR_WIDTH = 128
MIX_WIDTH = 128


def shard_levels(own_key, extent, cuts, smallest, largest):
    def one(axis_at, parts):
        draws = jax.random.uniform(jax.random.fold_in(jax.random.fold_in(own_key, 6), axis_at), (parts,), jnp.float32, smallest / len(cuts), largest / len(cuts))
        return jnp.repeat(jnp.exp(draws), extent[axis_at] // parts).reshape((-1,) + (1,) * (len(extent) - axis_at - 1))

    factor_of = one(*cuts[0])
    for cut in cuts[1:]:
        factor_of = factor_of * one(*cut)
    return factor_of


def scatter_about(key, extent, scale, bound, split=(), kind=jnp.bfloat16):
    gain = shard_levels(key, extent, split, -0.22, 0.18) if split else 1.0
    values = jax.random.normal(key, extent, jnp.float32) * scale * gain
    return jnp.minimum(jnp.maximum(values, -bound), bound).astype(kind)


def setup_inputs(seed: int = 0) -> dict:
    arg_keys = jax.random.split(jax.random.key(seed), 8)
    return {
        "pair_state": scatter_about(arg_keys[0], (RESIDUES, RESIDUES, PAIR_WIDTH), 1.0, 6.0, ((0, 16), (1, 16))),
        "in_gain": jnp.clip(1.0 + 0.15 * jax.random.normal(arg_keys[1], (PAIR_WIDTH,), jnp.float32), 0.25, 1.75),
        "left_weight": scatter_about(arg_keys[2], (PAIR_WIDTH, MIX_WIDTH), PAIR_WIDTH ** -0.5, 0.5),
        "right_weight": scatter_about(arg_keys[3], (PAIR_WIDTH, MIX_WIDTH), PAIR_WIDTH ** -0.5, 0.5),
        "mid_gain": jnp.clip(1.0 + 0.15 * jax.random.normal(arg_keys[4], (MIX_WIDTH,), jnp.float32), 0.25, 1.75),
        "out_weight": scatter_about(arg_keys[5], (MIX_WIDTH, PAIR_WIDTH), MIX_WIDTH ** -0.5, 0.5),
        "out_gate": scatter_about(arg_keys[6], (PAIR_WIDTH, PAIR_WIDTH), PAIR_WIDTH ** -0.5, 0.5),
    }


def unit_channels(values, channel_gain):
    centred = values - lax.optimization_barrier(jnp.mean(values, axis=-1, keepdims=True))
    return centred * lax.rsqrt(lax.optimization_barrier(jnp.mean(centred * centred, axis=-1, keepdims=True)) + 1e-05) * channel_gain

def make_factors(pair_in, in_gain, left_weight, right_weight):
    ready = unit_channels(pair_in.astype(jnp.float32), in_gain).astype(jnp.bfloat16)
    ready = lax.optimization_barrier(ready)
    left = jnp.einsum('ijc,cd->ijd', ready.astype(jnp.float32), left_weight.astype(jnp.float32))
    right = jnp.einsum('ijc,cd->ijd', ready.astype(jnp.float32), right_weight.astype(jnp.float32))
    return (ready, left.astype(jnp.bfloat16), right.astype(jnp.bfloat16))

def finish_pair(mixed, ready, mid_gain, out_weight, out_gate):
    scaled = unit_channels(mixed.astype(jnp.float32), mid_gain).astype(jnp.bfloat16)
    scaled = lax.optimization_barrier(scaled)
    gate = jax.nn.sigmoid(jnp.einsum('ijc,cd->ijd', ready.astype(jnp.float32), out_gate.astype(jnp.float32)))
    return (jnp.einsum('ijd,dc->ijc', scaled.astype(jnp.float32), out_weight.astype(jnp.float32)) * gate).astype(jnp.bfloat16)

def reference(pair_state, in_gain, left_weight, right_weight, mid_gain, out_weight, out_gate):
    ready, left, right = make_factors(pair_state, in_gain, left_weight, right_weight)
    left, right = lax.optimization_barrier((left, right))

    def one_channel(pair_of):
        return (jnp.dot(pair_of[0], pair_of[1].T, preferred_element_type=jnp.float32) * RESIDUES ** (-0.5)).astype(jnp.bfloat16)
    mixed = jnp.moveaxis(lax.map(one_channel, (jnp.moveaxis(left, -1, 0), jnp.moveaxis(right, -1, 0))), 0, -1)
    mixed = lax.optimization_barrier(mixed)
    return finish_pair(mixed, ready, mid_gain, out_weight, out_gate)
```

```python
import functools

import jax
import jax.numpy as jnp
from jax import lax
from jax.experimental import pallas as pl
from jax.experimental.pallas import tpu as pltpu
from jax.sharding import PartitionSpec as P

MESH = pl.DeviceIdType.MESH
F32 = jnp.float32
BF16 = jnp.bfloat16
CORES = 2


SIDE = 4
LANES = 128
GROUP = 16


def unit_rows(values, channel_gain):
    centred = values - jnp.mean(values, axis=-1, keepdims=True)
    return (
        centred
        * lax.rsqrt(jnp.mean(centred * centred, axis=-1, keepdims=True) + 1e-05)
        * channel_gain
    )


def turn_lanes(parts):
    count = len(parts)
    wide = LANES // count
    group = lax.broadcasted_iota(jnp.int32, parts[0].shape, 1) // wide
    parts = list(parts)
    step = 1
    while step < count:
        low = group // step % 2 == 0
        for n in range(count):
            if n // step % 2 == 0:
                one, two = parts[n], parts[n + step]
                parts[n] = jnp.where(low, one, pltpu.roll(two, step * wide, 1))
                parts[n + step] = jnp.where(low, pltpu.roll(one, LANES - step * wide, 1), two)
        step *= 2
    return parts


def triangle_kernel(
    layers, chips, count,
    x_hbm, in_gain_hbm, left_weight_hbm, right_weight_hbm, mid_gain_hbm, out_weight_hbm,
    out_gate_hbm, out_ref,
    x_ref, in_gain, left_weight, right_weight, mid_gain, out_weight, out_gate, fetch_sems,
    both_weight, ready_ref, gate_ref, turn_ref,
    far_send, far_recv, near_send, left_lines, right_lines,
    mix_send, mix_recv, back_send, back_recv,
    far_sems, left_sems, right_sems, mix_sems, back_sems,
):
    rows, cols, width = x_ref.shape
    parts = rows // GROUP
    a = lax.axis_index("first")
    b = lax.axis_index("second")
    z, c = b // CORES, b % CORES
    other = 1 - c
    y, x = a // SIDE, a % SIDE
    side = a % CORES
    pair = a // CORES

    def core_at(first, layer, core):
        return {"first": first, "second": layer * CORES + core}

    def layer_at(s):
        return lax.rem(z + s, layers)

    def chip_at(dy, dx):
        return lax.rem(y + dy, SIDE) * SIDE + lax.rem(x + dx, SIDE)

    hops = [(dy, dx) for dy in (2, 1, 3, 0) for dx in (2, 1, 3, 0) if (dy, dx) != (0, 0)]
    steps = [4, 3, 5, 2, 6, 1, 7] if layers == 8 else list(range(1, layers))

    barrier = pltpu.get_barrier_semaphore()
    peers = [core_at(a, z, other)]
    peers += [core_at(a, layer_at(s), c) for s in steps]
    for hop in hops:
        peers += [core_at(chip_at(*hop), z, c), core_at(chip_at(*hop), z, other)]
    for peer in peers:
        pl.semaphore_signal(barrier, inc=1, device_id=peer, device_id_type=MESH)

    fetches = [
        pltpu.make_async_copy(src, dst, fetch_sems.at[n])
        for n, (src, dst) in enumerate(
            [(x_hbm.at[pl.ds(p * GROUP, GROUP)], x_ref.at[pl.ds(p * GROUP, GROUP)]) for p in range(parts)]
            + [
                (in_gain_hbm, in_gain), (left_weight_hbm, left_weight),
                (right_weight_hbm, right_weight), (out_gate_hbm, out_gate),
                (mid_gain_hbm, mid_gain), (out_weight_hbm, out_weight),
            ]
        )
    ]
    for fetch in fetches:
        fetch.start()
    for fetch in fetches[parts : parts + 3]:
        fetch.wait()

    both_weight[:width, :] = left_weight[...].astype(F32).T.astype(BF16)
    both_weight[width:, :] = right_weight[...].astype(F32).T.astype(BF16)

    def send(src, dst, sems, at, peer):
        return pltpu.make_async_remote_copy(
            src_ref=src, dst_ref=dst, send_sem=sems.at[0, at], recv_sem=sems.at[1, at],
            device_id=peer, device_id_type=MESH,
        )

    def settle(like, sems, way, at):
        pltpu.make_async_copy(like, like, sems.at[way, at]).wait()

    def send_far(f, p):
        for s in steps:
            to = layer_at(s)
            send(
                far_send.at[f, p, to], far_recv.at[f, p, z], far_sems, f * parts + p,
                core_at(a, to, c),
            ).start()

    block = GROUP * GROUP
    for p in range(parts):
        fetches[p].wait()
        values = x_ref[p * GROUP : (p + 1) * GROUP].astype(F32).reshape(GROUP * cols, width)
        ready = unit_rows(values, in_gain[...].reshape(1, width)).astype(BF16)
        ready = ready.reshape(GROUP, parts, GROUP, width)
        for h in range(parts):
            piece = ready[:, h].reshape(block, width)
            ready_ref[h, p * block : (p + 1) * block, :] = piece
            made = lax.dot_general(
                both_weight[...], piece, (((1,), (1,)), ((), ())), preferred_element_type=F32
            ).astype(BF16)
            for f in range(2):
                far_send[f, p, :, :, h * block : (h + 1) * block] = made[
                    f * width : (f + 1) * width
                ].reshape(layers, GROUP, block)
        if p == 0:
            pl.semaphore_wait(barrier, len(peers))
        send_far(0, p)
        for f in range(2):
            far_recv[f, p, z] = far_send[f, p, z]
    for p in range(parts):
        send_far(1, p)

    fetches[parts + 3].wait()
    for h in range(parts):
        gate_ref[h] = jax.nn.sigmoid(
            jnp.dot(ready_ref[h], out_gate[...], preferred_element_type=F32)
        )

    halves = GROUP // layers

    def regroup(f, p):
        def body(h, carry):
            for e in range(halves):
                lanes = pl.ds(pl.multiple_of((h * halves + e) * LANES, LANES), LANES)
                lines = turn_lanes([far_recv[f, p, n, :, lanes].astype(F32) for n in range(layers)])
                for n in range(layers):
                    at = (e * layers + n) * GROUP
                    turn_ref[at : at + GROUP, :] = lines[n]
            lanes = pl.ds(pl.multiple_of(h * LANES, LANES), LANES)
            for d in range(GROUP):
                line = turn_ref[pl.ds(d, GROUP, stride=GROUP), :]
                near_send[f, p, d, :, lanes] = line.astype(BF16)
            return carry

        lax.fori_loop(0, parts, body, 0)

    for p in range(parts):
        settle(far_recv.at[0, p, pl.ds(0, layers - 1)], far_sems, 1, p)
        regroup(0, p)
        mine = c * chips + a
        for hop in hops:
            to = chip_at(*hop)
            for core in (c, other):
                send(
                    near_send.at[0, p, to], left_lines.at[p, mine], left_sems, p,
                    core_at(to, z, core),
                ).start()
        send(
            near_send.at[0, p, a], left_lines.at[p, mine], left_sems, p, core_at(a, z, other)
        ).start()
        left_lines[p, mine] = near_send[0, p, a]

    def give_right(p):
        settle(far_recv.at[1, p, pl.ds(0, layers - 1)], far_sems, 1, parts + p)
        regroup(1, p)
        mine = c * layers + pair
        for hop in hops:
            to = chip_at(*hop)
            send(
                near_send.at[1, p, to], right_lines.at[p, mine], right_sems, p,
                core_at(to, z, side),
            ).start()

        @pl.when(c == side)
        def _():
            right_lines[p, mine] = near_send[1, p, a]

        @pl.when(c != side)
        def _():
            send(
                near_send.at[1, p, a], right_lines.at[p, mine], right_sems, p,
                core_at(a, z, other),
            ).start()

    def meet(p):
        if p == 0:
            for q in range(parts):
                settle(left_lines.at[q, pl.ds(0, CORES * chips - 1)], left_sems, 1, q)

        @pl.when(c == side)
        def _():
            settle(right_lines.at[p, pl.ds(0, chips - 1)], right_sems, 1, p)

        @pl.when(c != side)
        def _():
            settle(right_lines.at[p], right_sems, 1, p)

        deep = near_send.shape[-1]
        for q in range(parts):
            total = None
            for core in range(CORES):
                left = left_lines[q, core * chips : (core + 1) * chips].reshape(chips * GROUP, deep)
                right = right_lines[p, core * layers : (core + 1) * layers].reshape(LANES, deep)
                term = lax.dot_general(
                    left, right, (((1,), (1,)), ((), ())), preferred_element_type=F32
                )
                total = term if total is None else total + term
            mixed = (total * count ** (-0.5)).astype(BF16)
            mix_send[p, :, q] = mixed.reshape(chips, GROUP, LANES)
        for hop in hops:
            to = chip_at(*hop)
            send(mix_send.at[p, to], mix_recv.at[p, a], mix_sems, p, core_at(to, z, c)).start()
        mix_recv[p, a] = mix_send[p, a]

    def give_back(p):
        settle(mix_recv.at[p, pl.ds(0, chips - 1)], mix_sems, 1, p)

        def body(q, carry):
            for d in range(GROUP):
                turn_ref[d * GROUP : (d + 1) * GROUP, :] = mix_recv[p, d, q].astype(F32)
            for e in range(halves):
                lines = turn_lanes([
                    turn_ref[pl.ds(e * layers + n, GROUP, stride=GROUP), :] for n in range(layers)
                ])
                lanes = pl.ds(pl.multiple_of((q * halves + e) * LANES, LANES), LANES)
                for n in range(layers):
                    back_send[p, n, :, lanes] = lines[n].astype(BF16)
            return carry

        lax.fori_loop(0, parts, body, 0)
        for s in steps:
            to = layer_at(s)
            send(back_send.at[p, to], back_recv.at[p, z], back_sems, p, core_at(a, to, c)).start()
        back_recv[p, z] = back_send[p, z]

    def finish(p):
        settle(back_recv.at[p, pl.ds(0, layers - 1)], back_sems, 1, p)
        mixed = back_recv[p].reshape(width, rows * GROUP).astype(F32)
        centred = mixed - jnp.mean(mixed, axis=0, keepdims=True)
        scaled = (
            centred
            * lax.rsqrt(jnp.mean(centred * centred, axis=0, keepdims=True) + 1e-05)
            * mid_gain[...]
        ).astype(BF16)
        result = lax.dot_general(
            scaled, out_weight[...], (((0,), (0,)), ((), ())), preferred_element_type=F32
        )
        result = (result * gate_ref[p]).astype(BF16)
        out_ref[:, p * GROUP : (p + 1) * GROUP, :] = result.reshape(rows, GROUP, width)

    give_right(0)
    for p in range(1, parts):
        give_right(p)
        meet(p - 1)
        if p > 1:
            give_back(p - 2)
    meet(parts - 1)
    fetches[parts + 4].wait()
    fetches[parts + 5].wait()
    for p in range(max(parts - 2, 0), parts):
        give_back(p)
    for p in range(parts):
        finish(p)

    for f in range(2):
        for p in range(parts):
            settle(far_send.at[f, p, pl.ds(0, layers - 1)], far_sems, 0, f * parts + p)
    for p in range(parts):
        settle(left_lines.at[p, pl.ds(0, CORES * chips - 1)], left_sems, 0, p)

        @pl.when(c == side)
        def _(p=p):
            settle(right_lines.at[p, pl.ds(0, chips - 1)], right_sems, 0, p)

        @pl.when(c != side)
        def _(p=p):
            settle(right_lines.at[p], right_sems, 0, p)

        settle(mix_send.at[p, pl.ds(0, chips - 1)], mix_sems, 0, p)
        settle(back_send.at[p, pl.ds(0, layers - 1)], back_sems, 0, p)


def by_kernel(pair_state, in_gain, left_weight, right_weight, mid_gain, out_weight, out_gate):
    rows, cols, width = pair_state.shape
    chips = lax.axis_size("first")
    layers = lax.axis_size("second") // CORES
    count = cols * lax.axis_size("second")
    parts = rows // GROUP
    lanes = parts * GROUP * GROUP
    deep = parts * LANES
    changed = pl.pallas_call(
        functools.partial(triangle_kernel, layers, chips, count),
        out_shape=jax.ShapeDtypeStruct((rows, cols, width), BF16),
        in_specs=[pl.BlockSpec(memory_space=pltpu.MemorySpace.HBM)] * 7,
        out_specs=pl.BlockSpec(memory_space=pltpu.VMEM),
        scratch_shapes=[
            pltpu.VMEM((rows, cols, width), BF16),
            pltpu.VMEM((width,), F32),
            pltpu.VMEM(left_weight.shape, BF16),
            pltpu.VMEM(right_weight.shape, BF16),
            pltpu.VMEM((width, 1), F32),
            pltpu.VMEM(out_weight.shape, BF16),
            pltpu.VMEM(out_gate.shape, BF16),
            pltpu.SemaphoreType.DMA((parts + 6,)),
            pltpu.VMEM((2 * width, width), BF16),
            pltpu.VMEM((parts, rows * GROUP, width), BF16),
            pltpu.VMEM((parts, rows * GROUP, width), F32),
            pltpu.VMEM((GROUP * GROUP, LANES), F32),
            pltpu.VMEM((2, parts, layers, GROUP, lanes), BF16),
            pltpu.VMEM((2, parts, layers, GROUP, lanes), BF16),
            pltpu.VMEM((2, parts, chips, GROUP, deep), BF16),
            pltpu.VMEM((parts, CORES * chips, GROUP, deep), BF16),
            pltpu.VMEM((parts, CORES * layers, GROUP, deep), BF16),
            pltpu.VMEM((parts, chips, parts, GROUP, LANES), BF16),
            pltpu.VMEM((parts, chips, parts, GROUP, LANES), BF16),
            pltpu.VMEM((parts, layers, GROUP, rows * GROUP), BF16),
            pltpu.VMEM((parts, layers, GROUP, rows * GROUP), BF16),
            pltpu.SemaphoreType.DMA((2, 2 * parts)),
            pltpu.SemaphoreType.DMA((2, parts)),
            pltpu.SemaphoreType.DMA((2, parts)),
            pltpu.SemaphoreType.DMA((2, parts)),
            pltpu.SemaphoreType.DMA((2, parts)),
        ],
        compiler_params=pltpu.CompilerParams(
            collective_id=0, has_side_effects=True, vmem_limit_bytes=32 * 1024 * 1024
        ),
    )(
        *(
            pltpu.with_memory_space_constraint(value, pltpu.MemorySpace.HBM)
            for value in (
                pair_state, in_gain, left_weight, right_weight, mid_gain.reshape(width, 1),
                out_weight, out_gate,
            )
        )
    )
    return changed


def unit_channels(values, channel_gain):
    centred = values - jnp.mean(values, axis=-1, keepdims=True)
    return (
        centred
        * lax.rsqrt(jnp.mean(centred * centred, axis=-1, keepdims=True) + 1e-05)
        * channel_gain
    )


def make_factors(pair_in, in_gain, left_weight, right_weight):
    ready = unit_channels(pair_in.astype(jnp.float32), in_gain).astype(jnp.bfloat16)
    ready = lax.optimization_barrier(ready)
    left = jnp.einsum("ijc,cd->ijd", ready, left_weight, preferred_element_type=jnp.float32)
    right = jnp.einsum("ijc,cd->ijd", ready, right_weight, preferred_element_type=jnp.float32)
    return (ready, left.astype(jnp.bfloat16), right.astype(jnp.bfloat16))


def finish_pair(mixed, ready, mid_gain, out_weight, out_gate):
    scaled = unit_channels(mixed.astype(jnp.float32), mid_gain).astype(jnp.bfloat16)
    scaled = lax.optimization_barrier(scaled)
    gate = jax.nn.sigmoid(
        jnp.einsum("ijc,cd->ijd", ready, out_gate, preferred_element_type=jnp.float32)
    )
    return (
        jnp.einsum("ijd,dc->ijc", scaled, out_weight, preferred_element_type=jnp.float32) * gate
    ).astype(jnp.bfloat16)


def by_collectives(pair_state, in_gain, left_weight, right_weight, mid_gain, out_weight, out_gate):
    ready, left, right = make_factors(pair_state, in_gain, left_weight, right_weight)
    count = pair_state.shape[1] * lax.axis_size("second")
    left_lines, right_lines = (
        lax.all_to_all(left, "second", split_axis=2, concat_axis=1, tiled=True),
        lax.all_to_all(right, "second", split_axis=2, concat_axis=1, tiled=True),
    )

    def meet(piece):
        return jnp.einsum("ikd,jkd->ijd", left_lines, piece, preferred_element_type=jnp.float32)

    strip = meet(lax.all_gather(right_lines, "first", axis=0, tiled=True))
    strip = (strip * count ** (-0.5)).astype(jnp.bfloat16)
    mixed = lax.all_to_all(strip, "second", split_axis=1, concat_axis=2, tiled=True)
    return finish_pair(mixed, ready, mid_gain, out_weight, out_gate)


def per_device(pair_state, *rest):
    groups, parts = lax.axis_size("first"), lax.axis_size("second")
    rows, cols, width = pair_state.shape
    left_out = rest[1].shape[1]
    fits = (
        groups == SIDE * SIDE
        and parts == CORES * 8
        and width == GROUP * 8
        and rows == cols
        and rows % GROUP == 0
        and left_out == width
    )
    return (by_kernel if fits else by_collectives)(pair_state, *rest)


def solution(mesh):
    in_specs = (P("first", "second", None), P(), P(), P(), P(), P(), P())
    out_specs = P("first", "second", None)
    return jax.shard_map(
        per_device, mesh=mesh, in_specs=in_specs, out_specs=out_specs, check_vma=False
    )
```

```python
import functools

import jax
import jax.numpy as jnp
from jax import lax
from jax.experimental import pallas as pl
from jax.experimental.pallas import tpu as pltpu
from jax.sharding import PartitionSpec as P

MESH = pl.DeviceIdType.MESH
F32 = jnp.float32
BF16 = jnp.bfloat16
CORES = 2


SIDE = 4
LANES = 128
GROUP = 16
UNIT = 8
LAG = 3


def unit_rows(values, channel_gain):
    centred = values - jnp.mean(values, axis=-1, keepdims=True)
    return (
        centred
        * lax.rsqrt(jnp.mean(centred * centred, axis=-1, keepdims=True) + 1e-05)
        * channel_gain
    )


def turn_lanes(parts):
    count = len(parts)
    wide = LANES // count
    group = lax.broadcasted_iota(jnp.int32, parts[0].shape, 1) // wide
    parts = list(parts)
    step = 1
    while step < count:
        low = group // step % 2 == 0
        for n in range(count):
            if n // step % 2 == 0:
                one, two = parts[n], parts[n + step]
                parts[n] = jnp.where(low, one, pltpu.roll(two, step * wide, 1))
                parts[n + step] = jnp.where(low, pltpu.roll(one, LANES - step * wide, 1), two)
        step *= 2
    return parts


def triangle_kernel(
    layers, chips, count,
    x_hbm, in_gain_hbm, left_weight_hbm, right_weight_hbm, mid_gain_hbm, out_weight_hbm,
    out_gate_hbm, out_ref,
    x_ref, in_gain, left_weight, right_weight, mid_gain, out_weight, out_gate, fetch_sems,
    both_weight, mid_wide, ready_ref, gate_ref, turn_ref,
    far_right, got_right, far_left, got_left, near_right, right_lines, near_left, left_lines,
    mix_send, mix_recv, back_send, back_recv,
    far_right_sems, far_left_sems, right_sems, left_sems, mix_sems, back_sems,
):
    scope = jax.named_scope
    rows, cols, width = x_ref.shape
    parts = rows // GROUP
    units = rows // UNIT
    halves = GROUP // UNIT
    a = lax.axis_index("first")
    b = lax.axis_index("second")
    z, c = b // CORES, b % CORES
    other = 1 - c
    y, x = a // SIDE, a % SIDE
    side = a % CORES
    pair = a // CORES

    def core_at(first, layer, core):
        return {"first": first, "second": layer * CORES + core}

    def layer_at(s):
        return lax.rem(z + s, layers)

    def chip_at(dy, dx):
        return lax.rem(y + dy, SIDE) * SIDE + lax.rem(x + dx, SIDE)

    hops = [(dy, dx) for dy in (2, 1, 3, 0) for dx in (2, 1, 3, 0) if (dy, dx) != (0, 0)]
    steps = [4, 3, 5, 2, 6, 1, 7]

    barrier = pltpu.get_barrier_semaphore()
    peers = [core_at(a, z, other)]
    peers += [core_at(a, layer_at(s), c) for s in steps]
    for hop in hops:
        peers += [core_at(chip_at(*hop), z, c), core_at(chip_at(*hop), z, other)]
    for peer in peers:
        pl.semaphore_signal(barrier, inc=1, device_id=peer, device_id_type=MESH)

    fetches = [
        pltpu.make_async_copy(src, dst, fetch_sems.at[n])
        for n, (src, dst) in enumerate(
            [(x_hbm.at[pl.ds(p * GROUP, GROUP)], x_ref.at[pl.ds(p * GROUP, GROUP)]) for p in range(parts)]
            + [
                (in_gain_hbm, in_gain), (left_weight_hbm, left_weight),
                (right_weight_hbm, right_weight), (out_gate_hbm, out_gate),
                (mid_gain_hbm, mid_gain), (out_weight_hbm, out_weight),
            ]
        )
    ]
    for fetch in fetches:
        fetch.start()
    for fetch in fetches[parts : parts + 3]:
        fetch.wait()

    both_weight[:width, :] = right_weight[...].astype(F32).T.astype(BF16)
    both_weight[width:, :] = left_weight[...].astype(F32).T.astype(BF16)

    def send(src, dst, sems, at, peer):
        pltpu.make_async_remote_copy(
            src_ref=src, dst_ref=dst, send_sem=sems.at[0, at], recv_sem=sems.at[1, at],
            device_id=peer, device_id_type=MESH,
        ).start()

    def settle(like, sems, way, at):
        with scope("wait"):
            pltpu.make_async_copy(like, like, sems.at[way, at]).wait()

    def send_far(src, dst, sems, p):
        for s in steps:
            to = layer_at(s)
            send(src.at[p, to], dst.at[p, z], sems, p, core_at(a, to, c))

    block = GROUP * GROUP
    for p in range(parts):
        fetches[p].wait()
        values = x_ref[p * GROUP : (p + 1) * GROUP].astype(F32).reshape(GROUP * cols, width)
        ready = unit_rows(values, in_gain[...].reshape(1, width)).astype(BF16)
        ready = ready.reshape(GROUP, parts, GROUP, width)
        for h in range(parts):
            piece = ready[:, h].reshape(block, width)
            made = lax.dot_general(
                both_weight[...], piece, (((1,), (1,)), ((), ())), preferred_element_type=F32
            ).astype(BF16)
            far_right[p, :, :, h * block : (h + 1) * block] = made[:width].reshape(
                layers, GROUP, block
            )
            for e in range(halves):
                u = p * halves + e
                ready_ref[u, h * LANES : (h + 1) * LANES, :] = piece[e * LANES : (e + 1) * LANES]
                far_left[u, :, :, h * LANES : (h + 1) * LANES] = made[
                    width:, e * LANES : (e + 1) * LANES
                ].reshape(layers, GROUP, LANES)
        if p == 0:
            with scope("bar"):
                pl.semaphore_wait(barrier, len(peers))
        send_far(far_right, got_right, far_right_sems, p)
        got_right[p, z] = far_right[p, z]
    for u in range(units):
        send_far(far_left, got_left, far_left_sems, u)
        got_left[u, z] = far_left[u, z]

    with scope("gate"):
        fetches[parts + 3].wait()
        for u in range(units):
            gate_ref[u] = jax.nn.sigmoid(
                jnp.dot(ready_ref[u], out_gate[...], preferred_element_type=F32)
            )
        fetches[parts + 4].wait()
        mid_wide[...] = jnp.broadcast_to(mid_gain[...].reshape(1, width), (width, width)).T
        fetches[parts + 5].wait()

    def give_right(p):
        settle(got_right.at[p, pl.ds(0, layers - 1)], far_right_sems, 1, p)

        def body(h, carry):
            for e in range(halves):
                lanes = pl.ds(pl.multiple_of((h * halves + e) * LANES, LANES), LANES)
                lines = turn_lanes([got_right[p, n, :, lanes].astype(F32) for n in range(layers)])
                for n in range(layers):
                    at = (e * layers + n) * GROUP
                    turn_ref[at : at + GROUP, :] = lines[n]
            lanes = pl.ds(pl.multiple_of(h * LANES, LANES), LANES)
            for d in range(GROUP):
                line = turn_ref[pl.ds(d, GROUP, stride=GROUP), :]
                near_right[p, d, :, lanes] = line.astype(BF16)
            return carry

        with scope("regroup"):
            lax.fori_loop(0, parts, body, 0)
        mine = c * chips + side * layers + pair
        for hop in hops:
            to = chip_at(*hop)
            for core in (c, other):
                send(
                    near_right.at[p, to], right_lines.at[p, mine], right_sems, p,
                    core_at(to, z, core),
                )
        send(near_right.at[p, a], right_lines.at[p, mine], right_sems, p, core_at(a, z, other))
        right_lines[p, mine] = near_right[p, a]

    def give_left(u):
        settle(got_left.at[u, pl.ds(0, layers - 1)], far_left_sems, 1, u)
        with scope("regroup"):
            for h in range(parts):
                lanes = slice(h * LANES, (h + 1) * LANES)
                lines = turn_lanes([got_left[u, n, :, lanes].astype(F32) for n in range(layers)])
                for n in range(UNIT):
                    at = (h * UNIT + n) * GROUP
                    turn_ref[at : at + GROUP, :] = lines[n]
                for d in range(GROUP):
                    line = turn_ref[pl.ds(h * UNIT * GROUP + d, UNIT, stride=GROUP), :]
                    near_left[u, d, :, lanes] = line.astype(BF16)
        mine = c * layers + pair
        for hop in hops:
            to = chip_at(*hop)
            send(
                near_left.at[u, to], left_lines.at[u, mine], left_sems, u, core_at(to, z, side)
            )

        @pl.when(c == side)
        def _():
            left_lines[u, mine] = near_left[u, a]

        @pl.when(c != side)
        def _():
            send(
                near_left.at[u, a], left_lines.at[u, mine], left_sems, u, core_at(a, z, other)
            )

    def settle_some(like, sems, way, at):
        @pl.when(c == side)
        def _():
            settle(like.at[at, pl.ds(0, chips - 1)], sems, way, at)

        @pl.when(c != side)
        def _():
            settle(like.at[at], sems, way, at)

    deep = near_left.shape[-1]

    def meet(u):
        if u == 0:
            for q in range(parts):
                settle(right_lines.at[q, pl.ds(0, CORES * chips - 1)], right_sems, 1, q)
        settle_some(left_lines, left_sems, 1, u)
        with scope("meet"):
            for q in range(parts):
                total = None
                for core in range(CORES):
                    left = left_lines[u, core * layers : (core + 1) * layers]
                    right = right_lines[q, core * chips : (core + 1) * chips]
                    term = lax.dot_general(
                        left.reshape(layers * UNIT, deep), right.reshape(chips * GROUP, deep),
                        (((1,), (1,)), ((), ())), preferred_element_type=F32,
                    )
                    total = term if total is None else total + term
                mixed = (total * count ** (-0.5)).astype(BF16)
                for core in range(CORES):
                    mix_send[u, core * layers : (core + 1) * layers, :, q * LANES : (q + 1) * LANES] = mixed[
                        :, core * LANES : (core + 1) * LANES
                    ].reshape(layers, UNIT, LANES)
        shift = lax.rem(c + x, CORES)

        def give(dy, t):
            to = chip_at(dy, shift + CORES * t)
            half = to // CORES
            return to, half

        for dy in (2, 1, 3, 0):
            for t in (1, 0):
                if (dy, t) != (0, 0):
                    to, half = give(dy, t)
                    for core in range(CORES):
                        send(
                            mix_send.at[u, core * layers + half], mix_recv.at[u, a], mix_sems, u,
                            core_at(to, z, core),
                        )
        to, half = give(0, 0)

        @pl.when(c == side)
        def _():
            send(
                mix_send.at[u, other * layers + half], mix_recv.at[u, a], mix_sems, u,
                core_at(a, z, other),
            )
            mix_recv[u, a] = mix_send[u, c * layers + half]

        @pl.when(c != side)
        def _():
            for core in range(CORES):
                send(
                    mix_send.at[u, core * layers + half], mix_recv.at[u, a], mix_sems, u,
                    core_at(to, z, core),
                )

    def give_back(u):
        settle_some(mix_recv, mix_sems, 1, u)
        with scope("back"):
            for h in range(parts):
                lanes = slice(h * LANES, (h + 1) * LANES)
                for d in range(GROUP):
                    at = (h * GROUP + d) * UNIT
                    turn_ref[at : at + UNIT, :] = mix_recv[u, d, :, lanes].astype(F32)
                lines = turn_lanes([
                    turn_ref[pl.ds(h * GROUP * UNIT + n, GROUP, stride=UNIT), :] for n in range(UNIT)
                ])
                for n in range(layers):
                    back_send[u, n, :, lanes] = lines[n].astype(BF16)
        send_far(back_send, back_recv, back_sems, u)
        back_recv[u, z] = back_send[u, z]

    def finish(u):
        settle(back_recv.at[u, pl.ds(0, layers - 1)], back_sems, 1, u)
        with scope("finish"):
            mixed = back_recv[u].reshape(width, parts * LANES).astype(F32)
            centred = mixed - jnp.mean(mixed, axis=0, keepdims=True)
            scaled = centred * lax.rsqrt(jnp.mean(centred * centred, axis=0, keepdims=True) + 1e-05)
            for h in range(parts):
                some = (scaled[:, h * LANES : (h + 1) * LANES] * mid_wide[...]).astype(BF16)
                result = lax.dot_general(
                    some, out_weight[...], (((0,), (0,)), ((), ())), preferred_element_type=F32
                )
                result = (result * gate_ref[u, h * LANES : (h + 1) * LANES, :]).astype(BF16)
                out_ref[u * UNIT : (u + 1) * UNIT, h * GROUP : (h + 1) * GROUP, :] = result.reshape(
                    UNIT, GROUP, width
                )

    for p in range(parts):
        give_right(p)
    lag = LAG
    plan = []
    for t in range(units + 3 * lag):
        for stage, fn in ((0, give_left), (1, meet), (2, give_back), (3, finish)):
            u = t - stage * lag
            if 0 <= u < units:
                plan.append((fn, u))
    for fn, u in plan:
        fn(u)

    for p in range(parts):
        settle(far_right.at[p, pl.ds(0, layers - 1)], far_right_sems, 0, p)
        settle(right_lines.at[p, pl.ds(0, CORES * chips - 1)], right_sems, 0, p)
    for u in range(units):
        settle(far_left.at[u, pl.ds(0, layers - 1)], far_left_sems, 0, u)
        settle_some(left_lines, left_sems, 0, u)
        settle_some(mix_recv, mix_sems, 0, u)
        settle(back_send.at[u, pl.ds(0, layers - 1)], back_sems, 0, u)


def by_kernel(pair_state, in_gain, left_weight, right_weight, mid_gain, out_weight, out_gate):
    rows, cols, width = pair_state.shape
    chips = lax.axis_size("first")
    layers = lax.axis_size("second") // CORES
    count = cols * lax.axis_size("second")
    parts = rows // GROUP
    units = rows // UNIT
    lanes = parts * GROUP * GROUP
    deep = parts * LANES
    changed = pl.pallas_call(
        functools.partial(triangle_kernel, layers, chips, count),
        out_shape=jax.ShapeDtypeStruct((rows, cols, width), BF16),
        in_specs=[pl.BlockSpec(memory_space=pltpu.MemorySpace.HBM)] * 7,
        out_specs=pl.BlockSpec(memory_space=pltpu.VMEM),
        scratch_shapes=[
            pltpu.VMEM((rows, cols, width), BF16),
            pltpu.VMEM((width,), F32),
            pltpu.VMEM(left_weight.shape, BF16),
            pltpu.VMEM(right_weight.shape, BF16),
            pltpu.VMEM((width,), F32),
            pltpu.VMEM(out_weight.shape, BF16),
            pltpu.VMEM(out_gate.shape, BF16),
            pltpu.SemaphoreType.DMA((parts + 6,)),
            pltpu.VMEM((2 * width, width), BF16),
            pltpu.VMEM((width, width), F32),
            pltpu.VMEM((units, deep, width), BF16),
            pltpu.VMEM((units, deep, width), F32),
            pltpu.VMEM((parts * GROUP * GROUP, LANES), F32),
            pltpu.VMEM((parts, layers, GROUP, lanes), BF16),
            pltpu.VMEM((parts, layers, GROUP, lanes), BF16),
            pltpu.VMEM((units, layers, GROUP, deep), BF16),
            pltpu.VMEM((units, layers, GROUP, deep), BF16),
            pltpu.VMEM((parts, chips, GROUP, deep), BF16),
            pltpu.VMEM((parts, CORES * chips, GROUP, deep), BF16),
            pltpu.VMEM((units, chips, UNIT, deep), BF16),
            pltpu.VMEM((units, chips, UNIT, deep), BF16),
            pltpu.VMEM((units, chips, UNIT, deep), BF16),
            pltpu.VMEM((units, chips, UNIT, deep), BF16),
            pltpu.VMEM((units, layers, GROUP, deep), BF16),
            pltpu.VMEM((units, layers, GROUP, deep), BF16),
            pltpu.SemaphoreType.DMA((2, parts)),
            pltpu.SemaphoreType.DMA((2, units)),
            pltpu.SemaphoreType.DMA((2, parts)),
            pltpu.SemaphoreType.DMA((2, units)),
            pltpu.SemaphoreType.DMA((2, units)),
            pltpu.SemaphoreType.DMA((2, units)),
        ],
        compiler_params=pltpu.CompilerParams(
            collective_id=0, has_side_effects=True, vmem_limit_bytes=32 * 1024 * 1024
        ),
    )(
        *(
            pltpu.with_memory_space_constraint(value, pltpu.MemorySpace.HBM)
            for value in (
                pair_state, in_gain, left_weight, right_weight, mid_gain, out_weight, out_gate,
            )
        )
    )
    return changed


def unit_channels(values, channel_gain):
    centred = values - jnp.mean(values, axis=-1, keepdims=True)
    return (
        centred
        * lax.rsqrt(jnp.mean(centred * centred, axis=-1, keepdims=True) + 1e-05)
        * channel_gain
    )


def make_factors(pair_in, in_gain, left_weight, right_weight):
    ready = unit_channels(pair_in.astype(jnp.float32), in_gain).astype(jnp.bfloat16)
    ready = lax.optimization_barrier(ready)
    left = jnp.einsum("ijc,cd->ijd", ready, left_weight, preferred_element_type=jnp.float32)
    right = jnp.einsum("ijc,cd->ijd", ready, right_weight, preferred_element_type=jnp.float32)
    return (ready, left.astype(jnp.bfloat16), right.astype(jnp.bfloat16))


def finish_pair(mixed, ready, mid_gain, out_weight, out_gate):
    scaled = unit_channels(mixed.astype(jnp.float32), mid_gain).astype(jnp.bfloat16)
    scaled = lax.optimization_barrier(scaled)
    gate = jax.nn.sigmoid(
        jnp.einsum("ijc,cd->ijd", ready, out_gate, preferred_element_type=jnp.float32)
    )
    return (
        jnp.einsum("ijd,dc->ijc", scaled, out_weight, preferred_element_type=jnp.float32) * gate
    ).astype(jnp.bfloat16)


def by_collectives(pair_state, in_gain, left_weight, right_weight, mid_gain, out_weight, out_gate):
    ready, left, right = make_factors(pair_state, in_gain, left_weight, right_weight)
    count = pair_state.shape[1] * lax.axis_size("second")
    left_lines, right_lines = (
        lax.all_to_all(left, "second", split_axis=2, concat_axis=1, tiled=True),
        lax.all_to_all(right, "second", split_axis=2, concat_axis=1, tiled=True),
    )

    def meet(piece):
        return jnp.einsum("ikd,jkd->ijd", left_lines, piece, preferred_element_type=jnp.float32)

    strip = meet(lax.all_gather(right_lines, "first", axis=0, tiled=True))
    strip = (strip * count ** (-0.5)).astype(jnp.bfloat16)
    mixed = lax.all_to_all(strip, "second", split_axis=1, concat_axis=2, tiled=True)
    return finish_pair(mixed, ready, mid_gain, out_weight, out_gate)


def per_device(pair_state, *rest):
    groups, parts = lax.axis_size("first"), lax.axis_size("second")
    rows, cols, width = pair_state.shape
    left_out = rest[1].shape[1]
    fits = (
        groups == SIDE * SIDE
        and parts == CORES * 8
        and width == GROUP * 8
        and rows == cols
        and rows % GROUP == 0
        and left_out == width
    )
    return (by_kernel if fits else by_collectives)(pair_state, *rest)


def solution(mesh):
    in_specs = (P("first", "second", None), P(), P(), P(), P(), P(), P())
    out_specs = P("first", "second", None)
    return jax.shard_map(
        per_device, mesh=mesh, in_specs=in_specs, out_specs=out_specs, check_vma=False
    )
```

```python
import functools

import jax
import jax.numpy as jnp
from jax import lax
from jax.experimental import pallas as pl
from jax.experimental.pallas import tpu as pltpu
from jax.sharding import PartitionSpec as P

MESH = pl.DeviceIdType.MESH
F32 = jnp.float32
BF16 = jnp.bfloat16
CORES = 2


SIDE = 4
LANES = 128
GROUP = 16


def unit_rows(values, channel_gain):
    centred = values - jnp.mean(values, axis=-1, keepdims=True)
    return (
        centred
        * lax.rsqrt(jnp.mean(centred * centred, axis=-1, keepdims=True) + 1e-05)
        * channel_gain
    )


def turn_lanes(parts):
    count = len(parts)
    wide = LANES // count
    group = lax.broadcasted_iota(jnp.int32, parts[0].shape, 1) // wide
    parts = list(parts)
    step = 1
    while step < count:
        low = group // step % 2 == 0
        for n in range(count):
            if n // step % 2 == 0:
                one, two = parts[n], parts[n + step]
                parts[n] = jnp.where(low, one, pltpu.roll(two, step * wide, 1))
                parts[n + step] = jnp.where(low, pltpu.roll(one, LANES - step * wide, 1), two)
        step *= 2
    return parts


def triangle_kernel(
    layers, chips, count,
    x_hbm, in_gain_hbm, left_weight_hbm, right_weight_hbm, mid_gain_hbm, out_weight_hbm,
    out_gate_hbm, out_ref,
    x_ref, in_gain, left_weight, right_weight, mid_gain, out_weight, out_gate, fetch_sems,
    left_rows, right_rows, mid_wide, whole_ref, ready_ref, gate_ref, turn_ref,
    far_left, got_left, near_left, left_lines,
    near_right, met_right, far_right, right_lines,
    mix_send, mix_recv, back_send, back_recv,
    far_left_sems, left_sems, near_right_sems, right_sems, mix_sems, back_sems,
):
    scope = jax.named_scope
    rows, cols, width = x_ref.shape
    parts = rows // GROUP
    halves = GROUP // layers
    block = GROUP * GROUP
    a = lax.axis_index("first")
    b = lax.axis_index("second")
    z, c = b // CORES, b % CORES
    other = 1 - c
    y, x = a // SIDE, a % SIDE
    side = a % CORES
    pair = a // CORES

    def core_at(first, layer, core):
        return {"first": first, "second": layer * CORES + core}

    def layer_at(s):
        return lax.rem(z + s, layers)

    def chip_at(dy, dx):
        return lax.rem(y + dy, SIDE) * SIDE + lax.rem(x + dx, SIDE)

    hops = [(dy, dx) for dy in (2, 1, 3, 0) for dx in (2, 1, 3, 0) if (dy, dx) != (0, 0)]
    steps = [4, 3, 5, 2, 6, 1, 7]

    barrier = pltpu.get_barrier_semaphore()
    peers = [core_at(a, z, other)]
    peers += [core_at(a, layer_at(s), c) for s in steps]
    for hop in hops:
        peers += [core_at(chip_at(*hop), z, c), core_at(chip_at(*hop), z, other)]
    for peer in peers:
        pl.semaphore_signal(barrier, inc=1, device_id=peer, device_id_type=MESH)

    fetches = [
        pltpu.make_async_copy(src, dst, fetch_sems.at[n])
        for n, (src, dst) in enumerate(
            [(x_hbm.at[pl.ds(p * GROUP, GROUP)], x_ref.at[pl.ds(p * GROUP, GROUP)]) for p in range(parts)]
            + [
                (in_gain_hbm, in_gain), (left_weight_hbm, left_weight),
                (right_weight_hbm, right_weight), (out_gate_hbm, out_gate),
                (mid_gain_hbm, mid_gain), (out_weight_hbm, out_weight),
            ]
        )
    ]
    for fetch in fetches:
        fetch.start()
    for fetch in fetches[parts : parts + 3]:
        fetch.wait()

    left_rows[...] = left_weight[...].astype(F32).T.astype(BF16)
    turn_ref[:width, :] = right_weight[...].astype(F32).T
    for d in range(chips):
        right_rows[d * layers : (d + 1) * layers, :] = turn_ref[
            pl.ds(d, layers, stride=chips), :
        ].astype(BF16)

    def send(src, dst, sems, at, peer):
        pltpu.make_async_remote_copy(
            src_ref=src, dst_ref=dst, send_sem=sems.at[0, at], recv_sem=sems.at[1, at],
            device_id=peer, device_id_type=MESH,
        ).start()

    def settle(like, sems, way, at):
        with scope("wait"):
            pltpu.make_async_copy(like, like, sems.at[way, at]).wait()

    def settle_some(like, sems, way, at):
        @pl.when(c == side)
        def _():
            settle(like.at[at, pl.ds(0, chips - 1)], sems, way, at)

        @pl.when(c != side)
        def _():
            settle(like.at[at], sems, way, at)

    def send_far(src, dst, sems, p, core):
        for s in steps:
            to = layer_at(s)
            send(src.at[p, to], dst.at[p, z], sems, p, core_at(a, to, core))
        dst[p, z] = src[p, z]

    def project(weight, lines):
        return lax.dot_general(
            weight, lines, (((1,), (1,)), ((), ())), preferred_element_type=F32
        ).astype(BF16)

    def begin(p):
        fetches[p].wait()
        values = x_ref[p * GROUP : (p + 1) * GROUP].astype(F32).reshape(GROUP * cols, width)
        ready = unit_rows(values, in_gain[...].reshape(1, width))
        whole_ref[p] = ready
        ready = ready.astype(BF16).reshape(GROUP, parts, GROUP, width)
        for h in range(parts):
            piece = ready[:, h].reshape(block, width)
            ready_ref[h, p * block : (p + 1) * block, :] = piece
            far_left[p, :, :, h * block : (h + 1) * block] = project(
                left_rows[...], piece
            ).reshape(layers, GROUP, block)

    def begin_right(p):
        turned = jnp.concatenate(
            [whole_ref[p, pl.ds(k, GROUP, stride=cols), :].astype(BF16) for k in range(cols)], axis=0
        )
        near_right[p] = project(right_rows[...], turned).reshape(chips, layers, GROUP * cols)
        mine = c * layers + pair
        for hop in hops:
            to = chip_at(*hop)
            send(
                near_right.at[p, to], met_right.at[p, mine], near_right_sems, p,
                core_at(to, z, side),
            )

        @pl.when(c == side)
        def _():
            met_right[p, mine] = near_right[p, a]

        @pl.when(c != side)
        def _():
            send(
                near_right.at[p, a], met_right.at[p, mine], near_right_sems, p,
                core_at(a, z, other),
            )

    def pass_right(p):
        settle_some(met_right, near_right_sems, 1, p)
        tiles = GROUP * cols // LANES

        def body(core, carry):
            for h in range(tiles):
                lanes = slice(h * LANES, (h + 1) * LANES)
                lines = turn_lanes([
                    met_right[p, core * layers + n, :, lanes].astype(F32) for n in range(layers)
                ])
                for n in range(layers):
                    at = (h * layers + n) * layers
                    turn_ref[at : at + layers, :] = lines[n]
            for h in range(parts):
                for n in range(layers):
                    line = turn_ref[pl.ds(h * GROUP * layers + n, GROUP, stride=layers), :]
                    far_right[p, n, core, h * GROUP : (h + 1) * GROUP, :] = line.astype(BF16)
            return carry

        with scope("rturn"):
            lax.fori_loop(0, CORES, body, 0)
        send_far(far_right, right_lines, right_sems, p, c)

    def give_left(p):
        settle(got_left.at[p, pl.ds(0, layers - 1)], far_left_sems, 1, p)

        def body(h, carry):
            for e in range(halves):
                lanes = pl.ds(pl.multiple_of((h * halves + e) * LANES, LANES), LANES)
                lines = turn_lanes([got_left[p, n, :, lanes].astype(F32) for n in range(layers)])
                for n in range(layers):
                    at = (e * layers + n) * GROUP
                    turn_ref[at : at + GROUP, :] = lines[n]
            lanes = pl.ds(pl.multiple_of(h * LANES, LANES), LANES)
            for d in range(GROUP):
                line = turn_ref[pl.ds(d, GROUP, stride=GROUP), :]
                near_left[p, d, :, lanes] = line.astype(BF16)
            return carry

        with scope("lturn"):
            lax.fori_loop(0, parts, body, 0)
        mine = c * chips + a
        for hop in hops:
            to = chip_at(*hop)
            for core in (c, other):
                send(
                    near_left.at[p, to], left_lines.at[p, mine], left_sems, p,
                    core_at(to, z, core),
                )
        send(near_left.at[p, a], left_lines.at[p, mine], left_sems, p, core_at(a, z, other))
        left_lines[p, mine] = near_left[p, a]

    deep = near_left.shape[-1]

    def meet(q, p):
        if p == 0:
            settle(left_lines.at[q, pl.ds(0, CORES * chips - 1)], left_sems, 1, q)
        if q == 0:
            settle(right_lines.at[p, pl.ds(0, layers - 1)], right_sems, 1, p)
        at = p * parts + q
        with scope("meet"):
            total = None
            for core in range(CORES):
                left = left_lines[q, core * chips : (core + 1) * chips].reshape(block, deep)
                right = jnp.concatenate(
                    [
                        right_lines[p, :, core, h * GROUP : (h + 1) * GROUP, :].reshape(LANES, LANES)
                        for h in range(parts)
                    ],
                    axis=0,
                )
                term = jnp.dot(left, right, preferred_element_type=F32)
                total = term if total is None else total + term
            mixed = (total * count ** (-0.5)).astype(BF16)
            mix_send[at] = mixed.reshape(chips, GROUP, LANES)
        for hop in hops:
            to = chip_at(*hop)
            send(mix_send.at[at, to], mix_recv.at[at, a], mix_sems, at, core_at(to, z, c))
        mix_recv[at, a] = mix_send[at, a]

    def give_back(q, p):
        at = p * parts + q
        settle(mix_recv.at[at, pl.ds(0, chips - 1)], mix_sems, 1, at)
        with scope("back"):
            for d in range(GROUP):
                turn_ref[d * GROUP : (d + 1) * GROUP, :] = mix_recv[at, d].astype(F32)
            for e in range(halves):
                lines = turn_lanes([
                    turn_ref[pl.ds(e * layers + n, GROUP, stride=GROUP), :] for n in range(layers)
                ])
                for n in range(layers):
                    back_send[at, n, :, e * LANES : (e + 1) * LANES] = lines[n].astype(BF16)
        send_far(back_send, back_recv, back_sems, at, c)

    def finish(q, p):
        at = p * parts + q
        settle(back_recv.at[at, pl.ds(0, layers - 1)], back_sems, 1, at)
        with scope("finish"):
            mixed = back_recv[at].reshape(width, block).astype(F32)
            centred = mixed - jnp.mean(mixed, axis=0, keepdims=True)
            scaled = centred * lax.rsqrt(jnp.mean(centred * centred, axis=0, keepdims=True) + 1e-05)
            scaled = jnp.concatenate(
                [scaled[:, e * LANES : (e + 1) * LANES] * mid_wide[...] for e in range(halves)], axis=1
            ).astype(BF16)
            result = lax.dot_general(
                scaled, out_weight[...], (((0,), (0,)), ((), ())), preferred_element_type=F32
            )
            result = (result * gate_ref[p, q * block : (q + 1) * block, :]).astype(BF16)
            out_ref[q * GROUP : (q + 1) * GROUP, p * GROUP : (p + 1) * GROUP, :] = result.reshape(
                GROUP, GROUP, width
            )

    for p in range(parts):
        begin(p)
        if p == 0:
            with scope("bar"):
                pl.semaphore_wait(barrier, len(peers))
        send_far(far_left, got_left, far_left_sems, p, c)
        begin_right(p)

    with scope("gate"):
        fetches[parts + 3].wait()
        for h in range(parts):
            gate_ref[h] = jax.nn.sigmoid(
                jnp.dot(ready_ref[h], out_gate[...], preferred_element_type=F32)
            )
        fetches[parts + 4].wait()
        mid_wide[...] = jnp.broadcast_to(mid_gain[...].reshape(1, width), (width, width)).T
        fetches[parts + 5].wait()

    pass_right(0)
    give_left(0)
    for p in range(1, parts):
        pass_right(p)
    for q in range(1, parts):
        give_left(q)
    last = parts - 1
    for p in range(parts):
        for q in range(parts):
            meet(q, p)
        if p > 0:
            for q in range(parts):
                give_back(q, p - 1)
                if p > 1:
                    finish(q, p - 2)
    for q in range(parts):
        give_back(q, last)
    for p in range(max(last - 1, 0), parts):
        for q in range(parts):
            finish(q, p)

    for p in range(parts):
        settle(far_left.at[p, pl.ds(0, layers - 1)], far_left_sems, 0, p)
        settle(left_lines.at[p, pl.ds(0, CORES * chips - 1)], left_sems, 0, p)
        settle_some(met_right, near_right_sems, 0, p)
        settle(far_right.at[p, pl.ds(0, layers - 1)], right_sems, 0, p)
    for at in range(parts * parts):
        settle(mix_send.at[at, pl.ds(0, chips - 1)], mix_sems, 0, at)
        settle(back_send.at[at, pl.ds(0, layers - 1)], back_sems, 0, at)


def by_kernel(pair_state, in_gain, left_weight, right_weight, mid_gain, out_weight, out_gate):
    rows, cols, width = pair_state.shape
    chips = lax.axis_size("first")
    layers = lax.axis_size("second") // CORES
    count = cols * lax.axis_size("second")
    parts = rows // GROUP
    block = GROUP * GROUP
    lanes = parts * block
    deep = parts * LANES
    changed = pl.pallas_call(
        functools.partial(triangle_kernel, layers, chips, count),
        out_shape=jax.ShapeDtypeStruct((rows, cols, width), BF16),
        in_specs=[pl.BlockSpec(memory_space=pltpu.MemorySpace.HBM)] * 7,
        out_specs=pl.BlockSpec(memory_space=pltpu.VMEM),
        scratch_shapes=[
            pltpu.VMEM((rows, cols, width), BF16),
            pltpu.VMEM((width,), F32),
            pltpu.VMEM(left_weight.shape, BF16),
            pltpu.VMEM(right_weight.shape, BF16),
            pltpu.VMEM((width,), F32),
            pltpu.VMEM(out_weight.shape, BF16),
            pltpu.VMEM(out_gate.shape, BF16),
            pltpu.SemaphoreType.DMA((parts + 6,)),
            pltpu.VMEM((width, width), BF16),
            pltpu.VMEM((width, width), BF16),
            pltpu.VMEM((width, width), F32),
            pltpu.VMEM((parts, GROUP * cols, width), F32),
            pltpu.VMEM((parts, rows * GROUP, width), BF16),
            pltpu.VMEM((parts, rows * GROUP, width), F32),
            pltpu.VMEM((cols * layers, LANES), F32),
            pltpu.VMEM((parts, layers, GROUP, lanes), BF16),
            pltpu.VMEM((parts, layers, GROUP, lanes), BF16),
            pltpu.VMEM((parts, chips, GROUP, deep), BF16),
            pltpu.VMEM((parts, CORES * chips, GROUP, deep), BF16),
            pltpu.VMEM((parts, chips, layers, lanes), BF16),
            pltpu.VMEM((parts, CORES * layers, layers, lanes), BF16),
            pltpu.VMEM((parts, layers, CORES, cols, LANES), BF16),
            pltpu.VMEM((parts, layers, CORES, cols, LANES), BF16),
            pltpu.VMEM((parts * parts, chips, GROUP, LANES), BF16),
            pltpu.VMEM((parts * parts, chips, GROUP, LANES), BF16),
            pltpu.VMEM((parts * parts, layers, GROUP, block), BF16),
            pltpu.VMEM((parts * parts, layers, GROUP, block), BF16),
            pltpu.SemaphoreType.DMA((2, parts)),
            pltpu.SemaphoreType.DMA((2, parts)),
            pltpu.SemaphoreType.DMA((2, parts)),
            pltpu.SemaphoreType.DMA((2, parts)),
            pltpu.SemaphoreType.DMA((2, parts * parts)),
            pltpu.SemaphoreType.DMA((2, parts * parts)),
        ],
        compiler_params=pltpu.CompilerParams(
            collective_id=0, has_side_effects=True, vmem_limit_bytes=32 * 1024 * 1024
        ),
    )(
        *(
            pltpu.with_memory_space_constraint(value, pltpu.MemorySpace.HBM)
            for value in (
                pair_state, in_gain, left_weight, right_weight, mid_gain, out_weight, out_gate,
            )
        )
    )
    return changed


def unit_channels(values, channel_gain):
    centred = values - jnp.mean(values, axis=-1, keepdims=True)
    return (
        centred
        * lax.rsqrt(jnp.mean(centred * centred, axis=-1, keepdims=True) + 1e-05)
        * channel_gain
    )


def make_factors(pair_in, in_gain, left_weight, right_weight):
    ready = unit_channels(pair_in.astype(jnp.float32), in_gain).astype(jnp.bfloat16)
    ready = lax.optimization_barrier(ready)
    left = jnp.einsum("ijc,cd->ijd", ready, left_weight, preferred_element_type=jnp.float32)
    right = jnp.einsum("ijc,cd->ijd", ready, right_weight, preferred_element_type=jnp.float32)
    return (ready, left.astype(jnp.bfloat16), right.astype(jnp.bfloat16))


def finish_pair(mixed, ready, mid_gain, out_weight, out_gate):
    scaled = unit_channels(mixed.astype(jnp.float32), mid_gain).astype(jnp.bfloat16)
    scaled = lax.optimization_barrier(scaled)
    gate = jax.nn.sigmoid(
        jnp.einsum("ijc,cd->ijd", ready, out_gate, preferred_element_type=jnp.float32)
    )
    return (
        jnp.einsum("ijd,dc->ijc", scaled, out_weight, preferred_element_type=jnp.float32) * gate
    ).astype(jnp.bfloat16)


def by_collectives(pair_state, in_gain, left_weight, right_weight, mid_gain, out_weight, out_gate):
    ready, left, right = make_factors(pair_state, in_gain, left_weight, right_weight)
    count = pair_state.shape[1] * lax.axis_size("second")
    left_lines, right_lines = (
        lax.all_to_all(left, "second", split_axis=2, concat_axis=1, tiled=True),
        lax.all_to_all(right, "second", split_axis=2, concat_axis=1, tiled=True),
    )

    def meet(piece):
        return jnp.einsum("ikd,jkd->ijd", left_lines, piece, preferred_element_type=jnp.float32)

    strip = meet(lax.all_gather(right_lines, "first", axis=0, tiled=True))
    strip = (strip * count ** (-0.5)).astype(jnp.bfloat16)
    mixed = lax.all_to_all(strip, "second", split_axis=1, concat_axis=2, tiled=True)
    return finish_pair(mixed, ready, mid_gain, out_weight, out_gate)


def per_device(pair_state, *rest):
    groups, parts = lax.axis_size("first"), lax.axis_size("second")
    rows, cols, width = pair_state.shape
    left_out = rest[1].shape[1]
    fits = (
        groups == SIDE * SIDE
        and parts == CORES * 8
        and width == GROUP * 8
        and rows == cols
        and rows % GROUP == 0
        and left_out == width
    )
    return (by_kernel if fits else by_collectives)(pair_state, *rest)


def solution(mesh):
    in_specs = (P("first", "second", None), P(), P(), P(), P(), P(), P())
    out_specs = P("first", "second", None)
    return jax.shard_map(
        per_device, mesh=mesh, in_specs=in_specs, out_specs=out_specs, check_vma=False
    )
```

```python
import functools

import jax
import jax.numpy as jnp
from jax import lax
from jax.experimental import pallas as pl
from jax.experimental.pallas import tpu as pltpu
from jax.sharding import PartitionSpec as P

MESH = pl.DeviceIdType.MESH
F32 = jnp.float32
BF16 = jnp.bfloat16
CORES = 2


SIDE = 4
LANES = 128
GROUP = 16
UNIT = 8
PLAN = (
    "a0 r0 a1 r1 a2 r2 f0 a3 f1 a4 f2 a5 f3 f4 m00 f5 m10 m20 m01 m11 m21 c00 c10 c20 "
    "m02 m12 m22 c01 c11 c21 d00 d10 c02 c12 c22 d20 d01 d11 d21 d02 d12 d22"
)


def unit_rows(values, channel_gain):
    centred = values - jnp.mean(values, axis=-1, keepdims=True)
    return (
        centred
        * lax.rsqrt(jnp.mean(centred * centred, axis=-1, keepdims=True) + 1e-05)
        * channel_gain
    )


def turn_lanes(parts):
    count = len(parts)
    wide = LANES // count
    group = lax.broadcasted_iota(jnp.int32, parts[0].shape, 1) // wide
    parts = list(parts)
    step = 1
    while step < count:
        low = group // step % 2 == 0
        for n in range(count):
            if n // step % 2 == 0:
                one, two = parts[n], parts[n + step]
                parts[n] = jnp.where(low, one, pltpu.roll(two, step * wide, 1))
                parts[n + step] = jnp.where(low, pltpu.roll(one, LANES - step * wide, 1), two)
        step *= 2
    return parts


def triangle_kernel(
    layers, chips, count,
    x_hbm, in_gain_hbm, left_weight_hbm, right_weight_hbm, mid_gain_hbm, out_weight_hbm,
    out_gate_hbm, out_ref,
    x_ref, in_gain, left_weight, right_weight, mid_gain, out_weight, out_gate, fetch_sems,
    left_rows, right_rows, mid_wide, whole_ref, ready_ref, gate_ref, turn_ref,
    far_left, got_left, near_left, left_lines,
    near_right, met_right, far_right, right_lines,
    mix_send, mix_recv, back_send, back_recv,
    far_left_sems, left_sems, pass_sems, near_right_sems, right_sems, mix_sems, back_sems,
):
    scope = jax.named_scope
    rows, cols, width = x_ref.shape
    parts = rows // GROUP
    units = rows // UNIT
    halves = GROUP // UNIT
    block = GROUP * GROUP
    a = lax.axis_index("first")
    b = lax.axis_index("second")
    z, c = b // CORES, b % CORES
    other = 1 - c
    y, x = a // SIDE, a % SIDE
    side = a % CORES
    pair = a // CORES

    def core_at(first, layer, core):
        return {"first": first, "second": layer * CORES + core}

    def layer_at(s):
        return lax.rem(z + s, layers)

    def chip_at(dy, dx):
        return lax.rem(y + dy, SIDE) * SIDE + lax.rem(x + dx, SIDE)

    hops = [(dy, dx) for dy in (2, 1, 3, 0) for dx in (2, 1, 3, 0) if (dy, dx) != (0, 0)]
    steps = [4, 3, 5, 2, 6, 1, 7]

    barrier = pltpu.get_barrier_semaphore()
    peers = [core_at(a, z, other)]
    peers += [core_at(a, layer_at(s), c) for s in steps]
    for hop in hops:
        peers += [core_at(chip_at(*hop), z, c), core_at(chip_at(*hop), z, other)]
    for peer in peers:
        pl.semaphore_signal(barrier, inc=1, device_id=peer, device_id_type=MESH)

    fetches = [
        pltpu.make_async_copy(src, dst, fetch_sems.at[n])
        for n, (src, dst) in enumerate(
            [(x_hbm.at[pl.ds(p * GROUP, GROUP)], x_ref.at[pl.ds(p * GROUP, GROUP)]) for p in range(parts)]
            + [
                (in_gain_hbm, in_gain), (left_weight_hbm, left_weight),
                (right_weight_hbm, right_weight), (out_gate_hbm, out_gate),
                (mid_gain_hbm, mid_gain), (out_weight_hbm, out_weight),
            ]
        )
    ]
    for fetch in fetches:
        fetch.start()
    for fetch in fetches[parts : parts + 3]:
        fetch.wait()

    left_rows[...] = left_weight[...].astype(F32).T.astype(BF16)
    turn_ref[:width, :] = right_weight[...].astype(F32).T
    for d in range(chips):
        right_rows[d * layers : (d + 1) * layers, :] = turn_ref[
            pl.ds(d, layers, stride=chips), :
        ].astype(BF16)

    def send(src, dst, sems, at, peer):
        pltpu.make_async_remote_copy(
            src_ref=src, dst_ref=dst, send_sem=sems.at[0, at], recv_sem=sems.at[1, at],
            device_id=peer, device_id_type=MESH,
        ).start()

    def settle(like, sems, way, at):
        with scope("wait"):
            pltpu.make_async_copy(like, like, sems.at[way, at]).wait()

    def settle_some(like, sems, way, at):
        @pl.when(c == side)
        def _():
            settle(like.at[at, pl.ds(0, chips - 1)], sems, way, at)

        @pl.when(c != side)
        def _():
            settle(like.at[at], sems, way, at)

    def send_far(src, dst, sems, p, core):
        for s in steps:
            to = layer_at(s)
            send(src.at[p, to], dst.at[p, z], sems, p, core_at(a, to, core))
        dst[p, z] = src[p, z]

    def project(weight, lines):
        return lax.dot_general(
            weight, lines, (((1,), (1,)), ((), ())), preferred_element_type=F32
        ).astype(BF16)

    def begin(p):
        fetches[p].wait()
        values = x_ref[p * GROUP : (p + 1) * GROUP].astype(F32).reshape(GROUP * cols, width)
        ready = unit_rows(values, in_gain[...].reshape(1, width))
        whole_ref[p] = ready
        ready = ready.astype(BF16).reshape(GROUP, parts, GROUP, width)
        for h in range(parts):
            piece = ready[:, h].reshape(block, width)
            ready_ref[h, p * block : (p + 1) * block, :] = piece
            made = project(left_rows[...], piece)
            for e in range(halves):
                far_left[p * halves + e, :, :, h * LANES : (h + 1) * LANES] = made[
                    :, e * LANES : (e + 1) * LANES
                ].reshape(layers, GROUP, LANES)

    def begin_right(p):
        turned = jnp.concatenate(
            [whole_ref[p, pl.ds(k, GROUP, stride=cols), :].astype(BF16) for k in range(cols)], axis=0
        )
        near_right[p] = project(right_rows[...], turned).reshape(chips, layers, GROUP * cols)
        mine = c * layers + pair
        for hop in hops:
            to = chip_at(*hop)
            send(
                near_right.at[p, to], met_right.at[p, mine], near_right_sems, p,
                core_at(to, z, side),
            )

        @pl.when(c == side)
        def _():
            met_right[p, mine] = near_right[p, a]

        @pl.when(c != side)
        def _():
            send(
                near_right.at[p, a], met_right.at[p, mine], near_right_sems, p,
                core_at(a, z, other),
            )

    def pass_right(p):
        settle_some(met_right, near_right_sems, 1, p)
        tiles = GROUP * cols // LANES

        def body(core, carry):
            for h in range(tiles):
                lanes = slice(h * LANES, (h + 1) * LANES)
                lines = turn_lanes([
                    met_right[p, core * layers + n, :, lanes].astype(F32) for n in range(layers)
                ])
                for n in range(layers):
                    at = (h * layers + n) * layers
                    turn_ref[at : at + layers, :] = lines[n]
            for h in range(parts):
                for n in range(layers):
                    line = turn_ref[pl.ds(h * GROUP * layers + n, GROUP, stride=layers), :]
                    far_right[p, n, core, h * GROUP : (h + 1) * GROUP, :] = line.astype(BF16)
            return carry

        with scope("rturn"):
            lax.fori_loop(0, CORES, body, 0)
        send_far(far_right, right_lines, right_sems, p, c)

    def give_left(u):
        settle(got_left.at[u, pl.ds(0, layers - 1)], far_left_sems, 1, u)
        with scope("lturn"):
            for h in range(parts):
                lanes = slice(h * LANES, (h + 1) * LANES)
                lines = turn_lanes([got_left[u, n, :, lanes].astype(F32) for n in range(layers)])
                for n in range(UNIT):
                    at = (h * UNIT + n) * GROUP
                    turn_ref[at : at + GROUP, :] = lines[n]
                for d in range(GROUP):
                    line = turn_ref[pl.ds(h * UNIT * GROUP + d, UNIT, stride=GROUP), :]
                    near_left[u, d, :, lanes] = line.astype(BF16)
        mine = c * chips + a
        for hop in hops:
            to = chip_at(*hop)
            send(
                near_left.at[u, to], left_lines.at[u, mine], left_sems, u, core_at(to, z, c)
            )
        left_lines[u, mine] = near_left[u, a]

    def pass_left(u):
        settle(left_lines.at[u, pl.ds(0, chips - 1)], left_sems, 1, u)
        with scope("pass"):
            own = pl.ds(c * chips, chips)
            send(
                left_lines.at[u, own], left_lines.at[u, own], pass_sems, u, core_at(a, z, other)
            )

    deep = near_left.shape[-1]

    def meet(q, p):
        if p == 0:
            for u in range(q * halves, (q + 1) * halves):
                settle(left_lines.at[u, pl.ds(0, chips)], pass_sems, 1, u)
        if q == 0:
            settle(right_lines.at[p, pl.ds(0, layers - 1)], right_sems, 1, p)
        at = p * parts + q
        with scope("meet"):
            total = None
            for core in range(CORES):
                left = left_lines[
                    q * halves : (q + 1) * halves, core * chips : (core + 1) * chips
                ].reshape(block, deep)
                right = jnp.concatenate(
                    [
                        right_lines[p, :, core, h * GROUP : (h + 1) * GROUP, :].reshape(LANES, LANES)
                        for h in range(parts)
                    ],
                    axis=0,
                )
                term = jnp.dot(left, right, preferred_element_type=F32)
                total = term if total is None else total + term
            mixed = (total * count ** (-0.5)).astype(BF16)
            for e in range(halves):
                mix_send[at, :, e * UNIT : (e + 1) * UNIT, :] = mixed[
                    e * LANES : (e + 1) * LANES
                ].reshape(chips, UNIT, LANES)
        for hop in hops:
            to = chip_at(*hop)
            send(mix_send.at[at, to], mix_recv.at[at, a], mix_sems, at, core_at(to, z, c))
        mix_recv[at, a] = mix_send[at, a]

    def give_back(q, p):
        at = p * parts + q
        settle(mix_recv.at[at, pl.ds(0, chips - 1)], mix_sems, 1, at)
        with scope("back"):
            for d in range(GROUP):
                turn_ref[d * GROUP : (d + 1) * GROUP, :] = mix_recv[at, d].astype(F32)
            for e in range(halves):
                lines = turn_lanes([
                    turn_ref[pl.ds(e * layers + n, GROUP, stride=GROUP), :] for n in range(layers)
                ])
                for n in range(layers):
                    back_send[at, n, :, e * LANES : (e + 1) * LANES] = lines[n].astype(BF16)
        send_far(back_send, back_recv, back_sems, at, c)

    def finish(q, p):
        at = p * parts + q
        settle(back_recv.at[at, pl.ds(0, layers - 1)], back_sems, 1, at)
        with scope("finish"):
            mixed = back_recv[at].reshape(width, block).astype(F32)
            centred = mixed - jnp.mean(mixed, axis=0, keepdims=True)
            scaled = centred * lax.rsqrt(jnp.mean(centred * centred, axis=0, keepdims=True) + 1e-05)
            scaled = jnp.concatenate(
                [scaled[:, e * LANES : (e + 1) * LANES] * mid_wide[...] for e in range(halves)], axis=1
            ).astype(BF16)
            result = lax.dot_general(
                scaled, out_weight[...], (((0,), (0,)), ((), ())), preferred_element_type=F32
            )
            result = (result * gate_ref[p, q * block : (q + 1) * block, :]).astype(BF16)
            out_ref[q * GROUP : (q + 1) * GROUP, p * GROUP : (p + 1) * GROUP, :] = result.reshape(
                GROUP, GROUP, width
            )

    for p in range(parts):
        begin(p)
        if p == 0:
            with scope("bar"):
                pl.semaphore_wait(barrier, len(peers))
        for e in range(halves):
            send_far(far_left, got_left, far_left_sems, p * halves + e, c)
        begin_right(p)

    with scope("gate"):
        fetches[parts + 3].wait()
        for h in range(parts):
            gate_ref[h] = jax.nn.sigmoid(
                jnp.dot(ready_ref[h], out_gate[...], preferred_element_type=F32)
            )
        fetches[parts + 4].wait()
        mid_wide[...] = jnp.broadcast_to(mid_gain[...].reshape(1, width), (width, width)).T
        fetches[parts + 5].wait()

    for step in PLAN.split():
        name, *at = step
        todo = {
            "a": give_left, "r": pass_right, "f": pass_left, "m": meet, "c": give_back, "d": finish,
        }[name]
        todo(*(int(n) for n in at))

    for p in range(parts):
        settle_some(met_right, near_right_sems, 0, p)
        settle(far_right.at[p, pl.ds(0, layers - 1)], right_sems, 0, p)
    for u in range(units):
        settle(far_left.at[u, pl.ds(0, layers - 1)], far_left_sems, 0, u)
        settle(near_left.at[u, pl.ds(0, chips - 1)], left_sems, 0, u)
        settle(left_lines.at[u, pl.ds(0, chips)], pass_sems, 0, u)
    for at in range(parts * parts):
        settle(mix_send.at[at, pl.ds(0, chips - 1)], mix_sems, 0, at)
        settle(back_send.at[at, pl.ds(0, layers - 1)], back_sems, 0, at)


def by_kernel(pair_state, in_gain, left_weight, right_weight, mid_gain, out_weight, out_gate):
    rows, cols, width = pair_state.shape
    chips = lax.axis_size("first")
    layers = lax.axis_size("second") // CORES
    count = cols * lax.axis_size("second")
    parts = rows // GROUP
    units = rows // UNIT
    block = GROUP * GROUP
    lanes = parts * block
    deep = parts * LANES
    changed = pl.pallas_call(
        functools.partial(triangle_kernel, layers, chips, count),
        out_shape=jax.ShapeDtypeStruct((rows, cols, width), BF16),
        in_specs=[pl.BlockSpec(memory_space=pltpu.MemorySpace.HBM)] * 7,
        out_specs=pl.BlockSpec(memory_space=pltpu.VMEM),
        scratch_shapes=[
            pltpu.VMEM((rows, cols, width), BF16),
            pltpu.VMEM((width,), F32),
            pltpu.VMEM(left_weight.shape, BF16),
            pltpu.VMEM(right_weight.shape, BF16),
            pltpu.VMEM((width,), F32),
            pltpu.VMEM(out_weight.shape, BF16),
            pltpu.VMEM(out_gate.shape, BF16),
            pltpu.SemaphoreType.DMA((parts + 6,)),
            pltpu.VMEM((width, width), BF16),
            pltpu.VMEM((width, width), BF16),
            pltpu.VMEM((width, width), F32),
            pltpu.VMEM((parts, GROUP * cols, width), F32),
            pltpu.VMEM((parts, rows * GROUP, width), BF16),
            pltpu.VMEM((parts, rows * GROUP, width), F32),
            pltpu.VMEM((cols * layers, LANES), F32),
            pltpu.VMEM((units, layers, GROUP, deep), BF16),
            pltpu.VMEM((units, layers, GROUP, deep), BF16),
            pltpu.VMEM((units, chips, UNIT, deep), BF16),
            pltpu.VMEM((units, CORES * chips, UNIT, deep), BF16),
            pltpu.VMEM((parts, chips, layers, lanes), BF16),
            pltpu.VMEM((parts, CORES * layers, layers, lanes), BF16),
            pltpu.VMEM((parts, layers, CORES, cols, LANES), BF16),
            pltpu.VMEM((parts, layers, CORES, cols, LANES), BF16),
            pltpu.VMEM((parts * parts, chips, GROUP, LANES), BF16),
            pltpu.VMEM((parts * parts, chips, GROUP, LANES), BF16),
            pltpu.VMEM((parts * parts, layers, GROUP, block), BF16),
            pltpu.VMEM((parts * parts, layers, GROUP, block), BF16),
            pltpu.SemaphoreType.DMA((2, units)),
            pltpu.SemaphoreType.DMA((2, units)),
            pltpu.SemaphoreType.DMA((2, units)),
            pltpu.SemaphoreType.DMA((2, parts)),
            pltpu.SemaphoreType.DMA((2, parts)),
            pltpu.SemaphoreType.DMA((2, parts * parts)),
            pltpu.SemaphoreType.DMA((2, parts * parts)),
        ],
        compiler_params=pltpu.CompilerParams(
            collective_id=0, has_side_effects=True, vmem_limit_bytes=32 * 1024 * 1024
        ),
    )(
        *(
            pltpu.with_memory_space_constraint(value, pltpu.MemorySpace.HBM)
            for value in (
                pair_state, in_gain, left_weight, right_weight, mid_gain, out_weight, out_gate,
            )
        )
    )
    return changed


def unit_channels(values, channel_gain):
    centred = values - jnp.mean(values, axis=-1, keepdims=True)
    return (
        centred
        * lax.rsqrt(jnp.mean(centred * centred, axis=-1, keepdims=True) + 1e-05)
        * channel_gain
    )


def make_factors(pair_in, in_gain, left_weight, right_weight):
    ready = unit_channels(pair_in.astype(jnp.float32), in_gain).astype(jnp.bfloat16)
    ready = lax.optimization_barrier(ready)
    left = jnp.einsum("ijc,cd->ijd", ready, left_weight, preferred_element_type=jnp.float32)
    right = jnp.einsum("ijc,cd->ijd", ready, right_weight, preferred_element_type=jnp.float32)
    return (ready, left.astype(jnp.bfloat16), right.astype(jnp.bfloat16))


def finish_pair(mixed, ready, mid_gain, out_weight, out_gate):
    scaled = unit_channels(mixed.astype(jnp.float32), mid_gain).astype(jnp.bfloat16)
    scaled = lax.optimization_barrier(scaled)
    gate = jax.nn.sigmoid(
        jnp.einsum("ijc,cd->ijd", ready, out_gate, preferred_element_type=jnp.float32)
    )
    return (
        jnp.einsum("ijd,dc->ijc", scaled, out_weight, preferred_element_type=jnp.float32) * gate
    ).astype(jnp.bfloat16)


def by_collectives(pair_state, in_gain, left_weight, right_weight, mid_gain, out_weight, out_gate):
    ready, left, right = make_factors(pair_state, in_gain, left_weight, right_weight)
    count = pair_state.shape[1] * lax.axis_size("second")
    left_lines, right_lines = (
        lax.all_to_all(left, "second", split_axis=2, concat_axis=1, tiled=True),
        lax.all_to_all(right, "second", split_axis=2, concat_axis=1, tiled=True),
    )

    def meet(piece):
        return jnp.einsum("ikd,jkd->ijd", left_lines, piece, preferred_element_type=jnp.float32)

    strip = meet(lax.all_gather(right_lines, "first", axis=0, tiled=True))
    strip = (strip * count ** (-0.5)).astype(jnp.bfloat16)
    mixed = lax.all_to_all(strip, "second", split_axis=1, concat_axis=2, tiled=True)
    return finish_pair(mixed, ready, mid_gain, out_weight, out_gate)


def per_device(pair_state, *rest):
    groups, parts = lax.axis_size("first"), lax.axis_size("second")
    rows, cols, width = pair_state.shape
    left_out = rest[1].shape[1]
    fits = (
        groups == SIDE * SIDE
        and parts == CORES * 8
        and width == GROUP * 8
        and rows == cols
        and rows % GROUP == 0
        and left_out == width
    )
    return (by_kernel if fits else by_collectives)(pair_state, *rest)


def solution(mesh):
    in_specs = (P("first", "second", None), P(), P(), P(), P(), P(), P())
    out_specs = P("first", "second", None)
    return jax.shard_map(
        per_device, mesh=mesh, in_specs=in_specs, out_specs=out_specs, check_vma=False
    )
```

```python
import functools

import jax
import jax.numpy as jnp
from jax import lax
from jax.experimental import pallas as pl
from jax.experimental.pallas import tpu as pltpu
from jax.sharding import PartitionSpec as P

MESH = pl.DeviceIdType.MESH
F32 = jnp.float32
BF16 = jnp.bfloat16
CORES = 2


SIDE = 4
LANES = 128
GROUP = 16
UNIT = 8
PLAN = (
    "a0", "r0", "a1", "r1", "a2", "r2", "f0", "a3", "f1", "a4", "f2", "a5", "f3", "f4",
    "m00", "f5", "m10", "m20", "m01", "m11", "m21", "c00", "c10", "h00", "c20", "h10",
    "m02", "m12", "m22", "c01", "h20", "c11", "c21", "h01", "d00", "d10", "c02", "c12",
    "c22", "h11", "h21", "h02", "h12", "h22", "d20", "d01", "d11", "d21", "d02", "d12",
    "d22",
)


def unit_rows(values, channel_gain):
    centred = values - jnp.mean(values, axis=-1, keepdims=True)
    return (
        centred
        * lax.rsqrt(jnp.mean(centred * centred, axis=-1, keepdims=True) + 1e-05)
        * channel_gain
    )


def turn_lanes(parts):
    count = len(parts)
    wide = LANES // count
    group = lax.broadcasted_iota(jnp.int32, parts[0].shape, 1) // wide
    parts = list(parts)
    step = 1
    while step < count:
        low = group // step % 2 == 0
        for n in range(count):
            if n // step % 2 == 0:
                one, two = parts[n], parts[n + step]
                parts[n] = jnp.where(low, one, pltpu.roll(two, step * wide, 1))
                parts[n + step] = jnp.where(low, pltpu.roll(one, LANES - step * wide, 1), two)
        step *= 2
    return parts


def triangle_kernel(
    layers, chips, count,
    x_hbm, in_gain_hbm, left_weight_hbm, right_weight_hbm, mid_gain_hbm, out_weight_hbm,
    out_gate_hbm, out_ref,
    x_ref, in_gain, left_weight, right_weight, mid_gain, out_weight, out_gate, fetch_sems,
    left_rows, right_rows, mid_wide, whole_ref, ready_ref, gate_ref, turn_ref,
    far_left, got_left, near_left, left_lines,
    near_right, met_right, far_right, right_lines,
    mix_send, mix_recv, back_send, back_recv,
    far_left_sems, left_sems, pass_sems, near_right_sems, right_sems, mix_sems, back_sems,
):
    scope = jax.named_scope
    rows, cols, width = x_ref.shape
    parts = rows // GROUP
    units = rows // UNIT
    halves = GROUP // UNIT
    block = GROUP * GROUP
    a = lax.axis_index("first")
    b = lax.axis_index("second")
    z, c = b // CORES, b % CORES
    other = 1 - c
    y, x = a // SIDE, a % SIDE
    side = a % CORES
    pair = a // CORES

    def core_at(first, layer, core):
        return {"first": first, "second": layer * CORES + core}

    def layer_at(s):
        return lax.rem(z + s, layers)

    def chip_at(dy, dx):
        return lax.rem(y + dy, SIDE) * SIDE + lax.rem(x + dx, SIDE)

    hops = [(dy, dx) for dy in (2, 1, 3, 0) for dx in (2, 1, 3, 0) if (dy, dx) != (0, 0)]
    steps = [4, 3, 5, 2, 6, 1, 7]

    barrier = pltpu.get_barrier_semaphore()
    peers = [core_at(a, z, other)]
    peers += [core_at(a, layer_at(s), c) for s in steps]
    for hop in hops:
        peers += [core_at(chip_at(*hop), z, c), core_at(chip_at(*hop), z, other)]
    for peer in peers:
        pl.semaphore_signal(barrier, inc=1, device_id=peer, device_id_type=MESH)

    fetches = [
        pltpu.make_async_copy(src, dst, fetch_sems.at[n])
        for n, (src, dst) in enumerate(
            [(x_hbm.at[pl.ds(p * GROUP, GROUP)], x_ref.at[pl.ds(p * GROUP, GROUP)]) for p in range(parts)]
            + [
                (in_gain_hbm, in_gain), (left_weight_hbm, left_weight),
                (right_weight_hbm, right_weight), (out_gate_hbm, out_gate),
                (mid_gain_hbm, mid_gain), (out_weight_hbm, out_weight),
            ]
        )
    ]
    for fetch in fetches:
        fetch.start()
    for fetch in fetches[parts : parts + 3]:
        fetch.wait()

    left_rows[...] = left_weight[...].astype(F32).T.astype(BF16)
    turn_ref[:width, :] = right_weight[...].astype(F32).T
    for d in range(chips):
        right_rows[d * layers : (d + 1) * layers, :] = turn_ref[
            pl.ds(d, layers, stride=chips), :
        ].astype(BF16)

    def send(src, dst, sems, at, peer):
        pltpu.make_async_remote_copy(
            src_ref=src, dst_ref=dst, send_sem=sems.at[0, at], recv_sem=sems.at[1, at],
            device_id=peer, device_id_type=MESH,
        ).start()

    def settle(like, sems, way, at):
        with scope("wait"):
            pltpu.make_async_copy(like, like, sems.at[way, at]).wait()

    def settle_some(like, sems, way, at):
        @pl.when(c == side)
        def _():
            settle(like.at[at, pl.ds(0, chips - 1)], sems, way, at)

        @pl.when(c != side)
        def _():
            settle(like.at[at], sems, way, at)

    def send_far(src, dst, sems, p, core):
        for s in steps:
            to = layer_at(s)
            send(src.at[p, to], dst.at[p, z], sems, p, core_at(a, to, core))
        dst[p, z] = src[p, z]

    def project(weight, lines):
        return lax.dot_general(
            weight, lines, (((1,), (1,)), ((), ())), preferred_element_type=F32
        ).astype(BF16)

    def begin(p):
        fetches[p].wait()
        values = x_ref[p * GROUP : (p + 1) * GROUP].astype(F32).reshape(GROUP * cols, width)
        ready = unit_rows(values, in_gain[...].reshape(1, width))
        whole_ref[p] = ready
        ready = ready.astype(BF16).reshape(GROUP, parts, GROUP, width)
        for h in range(parts):
            piece = ready[:, h].reshape(block, width)
            ready_ref[h, p * block : (p + 1) * block, :] = piece
            made = project(left_rows[...], piece)
            for e in range(halves):
                far_left[p * halves + e, :, :, h * LANES : (h + 1) * LANES] = made[
                    :, e * LANES : (e + 1) * LANES
                ].reshape(layers, GROUP, LANES)

    def begin_right(p):
        turned = jnp.concatenate(
            [whole_ref[p, pl.ds(k, GROUP, stride=cols), :].astype(BF16) for k in range(cols)], axis=0
        )
        near_right[p] = project(right_rows[...], turned).reshape(chips, layers, GROUP * cols)
        mine = c * layers + pair
        for hop in hops:
            to = chip_at(*hop)
            send(
                near_right.at[p, to], met_right.at[p, mine], near_right_sems, p,
                core_at(to, z, side),
            )

        @pl.when(c == side)
        def _():
            met_right[p, mine] = near_right[p, a]

        @pl.when(c != side)
        def _():
            send(
                near_right.at[p, a], met_right.at[p, mine], near_right_sems, p,
                core_at(a, z, other),
            )

    def pass_right(p):
        settle_some(met_right, near_right_sems, 1, p)
        tiles = GROUP * cols // LANES

        def body(core, carry):
            for h in range(tiles):
                lanes = slice(h * LANES, (h + 1) * LANES)
                lines = turn_lanes([
                    met_right[p, core * layers + n, :, lanes].astype(F32) for n in range(layers)
                ])
                for n in range(layers):
                    at = (h * layers + n) * layers
                    turn_ref[at : at + layers, :] = lines[n]
            for h in range(parts):
                for n in range(layers):
                    line = turn_ref[pl.ds(h * GROUP * layers + n, GROUP, stride=layers), :]
                    far_right[p, n, core, h * GROUP : (h + 1) * GROUP, :] = line.astype(BF16)
            return carry

        with scope("rturn"):
            lax.fori_loop(0, CORES, body, 0)
        send_far(far_right, right_lines, right_sems, p, c)

    def give_left(u):
        settle(got_left.at[u, pl.ds(0, layers - 1)], far_left_sems, 1, u)
        with scope("lturn"):
            for h in range(parts):
                lanes = slice(h * LANES, (h + 1) * LANES)
                lines = turn_lanes([got_left[u, n, :, lanes].astype(F32) for n in range(layers)])
                for n in range(UNIT):
                    at = (h * UNIT + n) * GROUP
                    turn_ref[at : at + GROUP, :] = lines[n]
                for d in range(GROUP):
                    line = turn_ref[pl.ds(h * UNIT * GROUP + d, UNIT, stride=GROUP), :]
                    near_left[u, d, :, lanes] = line.astype(BF16)
        mine = c * chips + a
        for hop in hops:
            to = chip_at(*hop)
            send(
                near_left.at[u, to], left_lines.at[u, mine], left_sems, u, core_at(to, z, c)
            )
        left_lines[u, mine] = near_left[u, a]

    def pass_left(u):
        settle(left_lines.at[u, pl.ds(0, chips - 1)], left_sems, 1, u)
        with scope("pass"):
            own = pl.ds(c * chips, chips)
            send(
                left_lines.at[u, own], left_lines.at[u, own], pass_sems, u, core_at(a, z, other)
            )

    deep = near_left.shape[-1]

    def meet(q, p):
        if p == 0:
            for u in range(q * halves, (q + 1) * halves):
                settle(left_lines.at[u, pl.ds(0, chips)], pass_sems, 1, u)
        if q == 0:
            settle(right_lines.at[p, pl.ds(0, layers - 1)], right_sems, 1, p)
        at = p * parts + q
        with scope("meet"):
            total = None
            for core in range(CORES):
                left = left_lines[
                    q * halves : (q + 1) * halves, core * chips : (core + 1) * chips
                ].reshape(block, deep)
                right = jnp.concatenate(
                    [
                        right_lines[p, :, core, h * GROUP : (h + 1) * GROUP, :].reshape(LANES, LANES)
                        for h in range(parts)
                    ],
                    axis=0,
                )
                term = jnp.dot(left, right, preferred_element_type=F32)
                total = term if total is None else total + term
            mixed = (total * count ** (-0.5)).astype(BF16)
            for e in range(halves):
                mix_send[at, :, e * UNIT : (e + 1) * UNIT, :] = mixed[
                    e * LANES : (e + 1) * LANES
                ].reshape(chips, UNIT, LANES)
        for hop in hops:
            to = chip_at(*hop)
            send(mix_send.at[at, to], mix_recv.at[at, a], mix_sems, at, core_at(to, z, c))
        mix_recv[at, a] = mix_send[at, a]

    def send_back(at, order):
        for n in order:
            to = n + (n + layers - z) // layers
            send(
                back_send.at[at, to], back_recv.at[at, z], back_sems, at, core_at(a, to, c)
            )

    def give_back(q, p):
        at = p * parts + q
        settle(mix_recv.at[at, pl.ds(0, chips - 1)], mix_sems, 1, at)
        with scope("back"):
            for d in range(GROUP):
                turn_ref[d * GROUP : (d + 1) * GROUP, :] = mix_recv[at, d].astype(F32)
            for e in range(halves):
                lines = turn_lanes([
                    turn_ref[pl.ds(e * layers + n, GROUP, stride=GROUP), :] for n in range(layers)
                ])
                for n in range(layers):
                    back_send[at, n, :, e * LANES : (e + 1) * LANES] = lines[n].astype(BF16)
        send_back(at, range(layers // 2))
        back_recv[at, z] = back_send[at, z]

    def give_high(q, p):
        send_back(p * parts + q, range(layers // 2, layers - 1))

    def finish(q, p):
        at = p * parts + q
        settle(back_recv.at[at, pl.ds(0, layers - 1)], back_sems, 1, at)
        with scope("finish"):
            mixed = back_recv[at].reshape(width, block).astype(F32)
            centred = mixed - jnp.mean(mixed, axis=0, keepdims=True)
            scaled = centred * lax.rsqrt(jnp.mean(centred * centred, axis=0, keepdims=True) + 1e-05)
            scaled = jnp.concatenate(
                [scaled[:, e * LANES : (e + 1) * LANES] * mid_wide[...] for e in range(halves)], axis=1
            ).astype(BF16)
            result = lax.dot_general(
                scaled, out_weight[...], (((0,), (0,)), ((), ())), preferred_element_type=F32
            )
            result = (result * gate_ref[p, q * block : (q + 1) * block, :]).astype(BF16)
            out_ref[q * GROUP : (q + 1) * GROUP, p * GROUP : (p + 1) * GROUP, :] = result.reshape(
                GROUP, GROUP, width
            )

    for p in range(parts):
        begin(p)
        if p == 0:
            with scope("bar"):
                pl.semaphore_wait(barrier, len(peers))
        for e in range(halves):
            send_far(far_left, got_left, far_left_sems, p * halves + e, c)
        begin_right(p)

    with scope("gate"):
        fetches[parts + 3].wait()
        for h in range(parts):
            gate_ref[h] = jax.nn.sigmoid(
                jnp.dot(ready_ref[h], out_gate[...], preferred_element_type=F32)
            )
        fetches[parts + 4].wait()
        mid_wide[...] = jnp.broadcast_to(mid_gain[...].reshape(1, width), (width, width)).T
        fetches[parts + 5].wait()

    for step in PLAN:
        name, *at = step
        todo = {
            "a": give_left, "r": pass_right, "f": pass_left, "m": meet, "c": give_back, "h": give_high,
            "d": finish,
        }[name]
        todo(*(int(n) for n in at))

    for p in range(parts):
        settle_some(met_right, near_right_sems, 0, p)
        settle(far_right.at[p, pl.ds(0, layers - 1)], right_sems, 0, p)
    for u in range(units):
        settle(far_left.at[u, pl.ds(0, layers - 1)], far_left_sems, 0, u)
        settle(near_left.at[u, pl.ds(0, chips - 1)], left_sems, 0, u)
        settle(left_lines.at[u, pl.ds(0, chips)], pass_sems, 0, u)
    for at in range(parts * parts):
        settle(mix_send.at[at, pl.ds(0, chips - 1)], mix_sems, 0, at)
        settle(back_send.at[at, pl.ds(0, layers - 1)], back_sems, 0, at)


def by_kernel(pair_state, in_gain, left_weight, right_weight, mid_gain, out_weight, out_gate):
    rows, cols, width = pair_state.shape
    chips = lax.axis_size("first")
    layers = lax.axis_size("second") // CORES
    count = cols * lax.axis_size("second")
    parts = rows // GROUP
    units = rows // UNIT
    block = GROUP * GROUP
    lanes = parts * block
    deep = parts * LANES
    changed = pl.pallas_call(
        functools.partial(triangle_kernel, layers, chips, count),
        out_shape=jax.ShapeDtypeStruct((rows, cols, width), BF16),
        in_specs=[pl.BlockSpec(memory_space=pltpu.MemorySpace.HBM)] * 7,
        out_specs=pl.BlockSpec(memory_space=pltpu.VMEM),
        scratch_shapes=[
            pltpu.VMEM((rows, cols, width), BF16),
            pltpu.VMEM((width,), F32),
            pltpu.VMEM(left_weight.shape, BF16),
            pltpu.VMEM(right_weight.shape, BF16),
            pltpu.VMEM((width,), F32),
            pltpu.VMEM(out_weight.shape, BF16),
            pltpu.VMEM(out_gate.shape, BF16),
            pltpu.SemaphoreType.DMA((parts + 6,)),
            pltpu.VMEM((width, width), BF16),
            pltpu.VMEM((width, width), BF16),
            pltpu.VMEM((width, width), F32),
            pltpu.VMEM((parts, GROUP * cols, width), F32),
            pltpu.VMEM((parts, rows * GROUP, width), BF16),
            pltpu.VMEM((parts, rows * GROUP, width), F32),
            pltpu.VMEM((cols * layers, LANES), F32),
            pltpu.VMEM((units, layers, GROUP, deep), BF16),
            pltpu.VMEM((units, layers, GROUP, deep), BF16),
            pltpu.VMEM((units, chips, UNIT, deep), BF16),
            pltpu.VMEM((units, CORES * chips, UNIT, deep), BF16),
            pltpu.VMEM((parts, chips, layers, lanes), BF16),
            pltpu.VMEM((parts, CORES * layers, layers, lanes), BF16),
            pltpu.VMEM((parts, layers, CORES, cols, LANES), BF16),
            pltpu.VMEM((parts, layers, CORES, cols, LANES), BF16),
            pltpu.VMEM((parts * parts, chips, GROUP, LANES), BF16),
            pltpu.VMEM((parts * parts, chips, GROUP, LANES), BF16),
            pltpu.VMEM((parts * parts, layers, GROUP, block), BF16),
            pltpu.VMEM((parts * parts, layers, GROUP, block), BF16),
            pltpu.SemaphoreType.DMA((2, units)),
            pltpu.SemaphoreType.DMA((2, units)),
            pltpu.SemaphoreType.DMA((2, units)),
            pltpu.SemaphoreType.DMA((2, parts)),
            pltpu.SemaphoreType.DMA((2, parts)),
            pltpu.SemaphoreType.DMA((2, parts * parts)),
            pltpu.SemaphoreType.DMA((2, parts * parts)),
        ],
        compiler_params=pltpu.CompilerParams(
            collective_id=0, has_side_effects=True, vmem_limit_bytes=32 * 1024 * 1024
        ),
    )(
        *(
            pltpu.with_memory_space_constraint(value, pltpu.MemorySpace.HBM)
            for value in (
                pair_state, in_gain, left_weight, right_weight, mid_gain, out_weight, out_gate,
            )
        )
    )
    return changed


def unit_channels(values, channel_gain):
    centred = values - jnp.mean(values, axis=-1, keepdims=True)
    return (
        centred
        * lax.rsqrt(jnp.mean(centred * centred, axis=-1, keepdims=True) + 1e-05)
        * channel_gain
    )


def make_factors(pair_in, in_gain, left_weight, right_weight):
    ready = unit_channels(pair_in.astype(jnp.float32), in_gain).astype(jnp.bfloat16)
    ready = lax.optimization_barrier(ready)
    left = jnp.einsum("ijc,cd->ijd", ready, left_weight, preferred_element_type=jnp.float32)
    right = jnp.einsum("ijc,cd->ijd", ready, right_weight, preferred_element_type=jnp.float32)
    return (ready, left.astype(jnp.bfloat16), right.astype(jnp.bfloat16))


def finish_pair(mixed, ready, mid_gain, out_weight, out_gate):
    scaled = unit_channels(mixed.astype(jnp.float32), mid_gain).astype(jnp.bfloat16)
    scaled = lax.optimization_barrier(scaled)
    gate = jax.nn.sigmoid(
        jnp.einsum("ijc,cd->ijd", ready, out_gate, preferred_element_type=jnp.float32)
    )
    return (
        jnp.einsum("ijd,dc->ijc", scaled, out_weight, preferred_element_type=jnp.float32) * gate
    ).astype(jnp.bfloat16)


def by_collectives(pair_state, in_gain, left_weight, right_weight, mid_gain, out_weight, out_gate):
    ready, left, right = make_factors(pair_state, in_gain, left_weight, right_weight)
    count = pair_state.shape[1] * lax.axis_size("second")
    left_lines, right_lines = (
        lax.all_to_all(left, "second", split_axis=2, concat_axis=1, tiled=True),
        lax.all_to_all(right, "second", split_axis=2, concat_axis=1, tiled=True),
    )

    def meet(piece):
        return jnp.einsum("ikd,jkd->ijd", left_lines, piece, preferred_element_type=jnp.float32)

    strip = meet(lax.all_gather(right_lines, "first", axis=0, tiled=True))
    strip = (strip * count ** (-0.5)).astype(jnp.bfloat16)
    mixed = lax.all_to_all(strip, "second", split_axis=1, concat_axis=2, tiled=True)
    return finish_pair(mixed, ready, mid_gain, out_weight, out_gate)


def per_device(pair_state, *rest):
    groups, parts = lax.axis_size("first"), lax.axis_size("second")
    rows, cols, width = pair_state.shape
    left_out = rest[1].shape[1]
    fits = (
        groups == SIDE * SIDE
        and parts == CORES * 8
        and width == GROUP * 8
        and rows == cols
        and rows % GROUP == 0
        and left_out == width
    )
    return (by_kernel if fits else by_collectives)(pair_state, *rest)


def solution(mesh):
    in_specs = (P("first", "second", None), P(), P(), P(), P(), P(), P())
    out_specs = P("first", "second", None)
    return jax.shard_map(
        per_device, mesh=mesh, in_specs=in_specs, out_specs=out_specs, check_vma=False
    )
```

```python
import functools

import jax
import jax.numpy as jnp
from jax import lax
from jax.experimental import pallas as pl
from jax.experimental.pallas import tpu as pltpu
from jax.sharding import PartitionSpec as P

MESH = pl.DeviceIdType.MESH
F32 = jnp.float32
BF16 = jnp.bfloat16
CORES = 2


SIDE = 4
LANES = 128
GROUP = 16
UNIT = 8
LEFTS = ((0, 1), (1, 1), (2, 1), (3, 1), (4, 1), (5, 1))
BLOCKS = ((0, 1), (1, 1), (2, 1), (3, 1), (4, 1), (5, 1), (6, 3))
PLAN = (
    "a0", "r0", "a1", "r1", "a2", "r2", "f0", "a3", "f1", "a4", "f2", "a5", "f3", "f4",
    "m0", "f5", "m1", "m2", "m3", "m4", "m5", "c0", "c1", "h0", "c2", "h1", "m6", "c3",
    "h2", "c4", "c5", "h3", "d0", "d1", "h4", "c6", "h5", "h6", "d2", "d3", "d4", "d5",
    "d6",
)


def unit_rows(values, channel_gain):
    centred = values - jnp.mean(values, axis=-1, keepdims=True)
    return (
        centred
        * lax.rsqrt(jnp.mean(centred * centred, axis=-1, keepdims=True) + 1e-05)
        * channel_gain
    )


def turn_lanes(parts):
    count = len(parts)
    wide = LANES // count
    group = lax.broadcasted_iota(jnp.int32, parts[0].shape, 1) // wide
    parts = list(parts)
    step = 1
    while step < count:
        low = group // step % 2 == 0
        for n in range(count):
            if n // step % 2 == 0:
                one, two = parts[n], parts[n + step]
                parts[n] = jnp.where(low, one, pltpu.roll(two, step * wide, 1))
                parts[n + step] = jnp.where(low, pltpu.roll(one, LANES - step * wide, 1), two)
        step *= 2
    return parts


def triangle_kernel(
    layers, chips, count,
    x_hbm, in_gain_hbm, left_weight_hbm, right_weight_hbm, mid_gain_hbm, out_weight_hbm,
    out_gate_hbm, out_ref,
    x_ref, in_gain, left_weight, right_weight, mid_gain, out_weight, out_gate, fetch_sems,
    left_rows, right_rows, mid_wide, whole_ref, ready_ref, gate_ref, turn_ref,
    far_left, got_left, near_left, left_lines,
    near_right, met_right, far_right, right_lines,
    mix_send, mix_recv, back_send, back_recv,
    far_left_sems, left_sems, pass_sems, near_right_sems, right_sems, mix_sems, back_sems,
):
    scope = jax.named_scope
    rows, cols, width = x_ref.shape
    parts = rows // GROUP
    units = rows // UNIT
    halves = GROUP // UNIT
    block = GROUP * GROUP
    a = lax.axis_index("first")
    b = lax.axis_index("second")
    z, c = b // CORES, b % CORES
    other = 1 - c
    y, x = a // SIDE, a % SIDE
    side = a % CORES
    pair = a // CORES

    def core_at(first, layer, core):
        return {"first": first, "second": layer * CORES + core}

    def layer_at(s):
        return lax.rem(z + s, layers)

    def chip_at(dy, dx):
        return lax.rem(y + dy, SIDE) * SIDE + lax.rem(x + dx, SIDE)

    hops = [(dy, dx) for dy in (2, 1, 3, 0) for dx in (2, 1, 3, 0) if (dy, dx) != (0, 0)]
    steps = [4, 3, 5, 2, 6, 1, 7]

    barrier = pltpu.get_barrier_semaphore()
    peers = [core_at(a, z, other)]
    peers += [core_at(a, layer_at(s), c) for s in steps]
    for hop in hops:
        peers += [core_at(chip_at(*hop), z, c), core_at(chip_at(*hop), z, other)]
    for peer in peers:
        pl.semaphore_signal(barrier, inc=1, device_id=peer, device_id_type=MESH)

    fetches = [
        pltpu.make_async_copy(src, dst, fetch_sems.at[n])
        for n, (src, dst) in enumerate(
            [(x_hbm.at[pl.ds(p * GROUP, GROUP)], x_ref.at[pl.ds(p * GROUP, GROUP)]) for p in range(parts)]
            + [
                (in_gain_hbm, in_gain), (left_weight_hbm, left_weight),
                (right_weight_hbm, right_weight), (out_gate_hbm, out_gate),
                (mid_gain_hbm, mid_gain), (out_weight_hbm, out_weight),
            ]
        )
    ]
    for fetch in fetches:
        fetch.start()
    for fetch in fetches[parts : parts + 3]:
        fetch.wait()

    left_rows[...] = left_weight[...].astype(F32).T.astype(BF16)
    turn_ref[:width, :] = right_weight[...].astype(F32).T
    for d in range(chips):
        right_rows[d * layers : (d + 1) * layers, :] = turn_ref[
            pl.ds(d, layers, stride=chips), :
        ].astype(BF16)

    def send(src, dst, sems, at, peer):
        pltpu.make_async_remote_copy(
            src_ref=src, dst_ref=dst, send_sem=sems.at[sems.shape[0] - 1], recv_sem=sems.at[at],
            device_id=peer, device_id_type=MESH,
        ).start()

    def settle(like, sem):
        with scope("wait"):
            pltpu.make_async_copy(like, like, sem).wait()

    def settle_some(like, span, sem):
        @pl.when(c == side)
        def _():
            settle(like.at[span, pl.ds(0, chips - 1)], sem)

        @pl.when(c != side)
        def _():
            settle(like.at[span], sem)

    def sent(sems):
        return sems.at[sems.shape[0] - 1]

    def send_far(src, dst, sems, at, span):
        for s in steps:
            to = layer_at(s)
            send(src.at[span, to], dst.at[span, z], sems, at, core_at(a, to, c))
        dst[span, z] = src[span, z]

    def project(weight, lines):
        return lax.dot_general(
            weight, lines, (((1,), (1,)), ((), ())), preferred_element_type=F32
        ).astype(BF16)

    def begin(p):
        fetches[p].wait()
        values = x_ref[p * GROUP : (p + 1) * GROUP].astype(F32).reshape(GROUP * cols, width)
        ready = unit_rows(values, in_gain[...].reshape(1, width))
        whole_ref[p] = ready
        ready = ready.astype(BF16).reshape(GROUP, parts, GROUP, width)
        for h in range(parts):
            piece = ready[:, h].reshape(block, width)
            ready_ref[h, p * block : (p + 1) * block, :] = piece
            made = project(left_rows[...], piece)
            for e in range(halves):
                far_left[p * halves + e, :, :, h * LANES : (h + 1) * LANES] = made[
                    :, e * LANES : (e + 1) * LANES
                ].reshape(layers, GROUP, LANES)

    def begin_right(p):
        turned = jnp.concatenate(
            [whole_ref[p, pl.ds(k, GROUP, stride=cols), :].astype(BF16) for k in range(cols)], axis=0
        )
        near_right[p] = project(right_rows[...], turned).reshape(chips, layers, GROUP * cols)
        mine = c * layers + pair
        for hop in hops:
            to = chip_at(*hop)
            send(
                near_right.at[p, to], met_right.at[p, mine], near_right_sems, p,
                core_at(to, z, side),
            )

        @pl.when(c == side)
        def _():
            met_right[p, mine] = near_right[p, a]

        @pl.when(c != side)
        def _():
            send(
                near_right.at[p, a], met_right.at[p, mine], near_right_sems, p,
                core_at(a, z, other),
            )

    def pass_right(p):
        settle_some(met_right, pl.ds(p, 1), near_right_sems.at[p])
        tiles = GROUP * cols // LANES

        def body(core, carry):
            for h in range(tiles):
                lanes = slice(h * LANES, (h + 1) * LANES)
                lines = turn_lanes([
                    met_right[p, core * layers + n, :, lanes].astype(F32) for n in range(layers)
                ])
                for n in range(layers):
                    at = (h * layers + n) * layers
                    turn_ref[at : at + layers, :] = lines[n]
            for h in range(parts):
                for n in range(layers):
                    line = turn_ref[pl.ds(h * GROUP * layers + n, GROUP, stride=layers), :]
                    far_right[p, n, core, h * GROUP : (h + 1) * GROUP, :] = line.astype(BF16)
            return carry

        with scope("rturn"):
            lax.fori_loop(0, CORES, body, 0)
        send_far(far_right, right_lines, right_sems, p, pl.ds(p, 1))

    def give_left(g):
        first, size = LEFTS[g]
        span = pl.ds(first, size)
        settle(got_left.at[span, pl.ds(0, layers - 1)], far_left_sems.at[g])
        with scope("lturn"):
            for u in range(first, first + size):
                for h in range(parts):
                    lanes = slice(h * LANES, (h + 1) * LANES)
                    lines = turn_lanes([
                        got_left[u, n, :, lanes].astype(F32) for n in range(layers)
                    ])
                    for n in range(UNIT):
                        at = (h * UNIT + n) * GROUP
                        turn_ref[at : at + GROUP, :] = lines[n]
                    for d in range(GROUP):
                        line = turn_ref[pl.ds(h * UNIT * GROUP + d, UNIT, stride=GROUP), :]
                        near_left[u, d, :, lanes] = line.astype(BF16)
        mine = c * chips + a
        for hop in hops:
            to = chip_at(*hop)
            send(
                near_left.at[span, to], left_lines.at[span, mine], left_sems, g,
                core_at(to, z, c),
            )
        left_lines[span, mine] = near_left[span, a]

    def pass_left(g):
        first, size = LEFTS[g]
        span = pl.ds(first, size)
        settle(left_lines.at[span, pl.ds(0, chips - 1)], left_sems.at[g])
        with scope("pass"):
            own = left_lines.at[span, pl.ds(c * chips, chips)]
            send(own, own, pass_sems, g, core_at(a, z, other))

    deep = near_left.shape[-1]

    met = set()

    def meet(g):
        first, size = BLOCKS[g]
        span = pl.ds(first, size)
        for at in range(first, first + size):
            p, q = at // parts, at % parts
            for n, (unit, many) in enumerate(LEFTS):
                if unit < (q + 1) * halves and ("left", n) not in met:
                    met.add(("left", n))
                    settle(left_lines.at[pl.ds(unit, many), pl.ds(0, chips)], pass_sems.at[n])
            if ("right", p) not in met:
                met.add(("right", p))
                settle(right_lines.at[p, pl.ds(0, layers - 1)], right_sems.at[p])
            with scope("meet"):
                total = None
                for core in range(CORES):
                    left = left_lines[
                        q * halves : (q + 1) * halves, core * chips : (core + 1) * chips
                    ].reshape(block, deep)
                    right = jnp.concatenate(
                        [
                            right_lines[p, :, core, h * GROUP : (h + 1) * GROUP, :].reshape(LANES, LANES)
                            for h in range(parts)
                        ],
                        axis=0,
                    )
                    term = jnp.dot(left, right, preferred_element_type=F32)
                    total = term if total is None else total + term
                mixed = (total * count ** (-0.5)).astype(BF16)
                for e in range(halves):
                    mix_send[at, :, e * UNIT : (e + 1) * UNIT, :] = mixed[
                        e * LANES : (e + 1) * LANES
                    ].reshape(chips, UNIT, LANES)
        for hop in hops:
            to = chip_at(*hop)
            send(
                mix_send.at[span, to], mix_recv.at[span, a], mix_sems, g, core_at(to, z, c)
            )
        mix_recv[span, a] = mix_send[span, a]

    def send_back(g, order):
        span = pl.ds(*BLOCKS[g])
        for n in order:
            to = n + (n + layers - z) // layers
            send(
                back_send.at[span, to], back_recv.at[span, z], back_sems, g, core_at(a, to, c)
            )

    def give_back(g):
        first, size = BLOCKS[g]
        span = pl.ds(first, size)
        settle(mix_recv.at[span, pl.ds(0, chips - 1)], mix_sems.at[g])
        with scope("back"):
            for at in range(first, first + size):
                for d in range(GROUP):
                    turn_ref[d * GROUP : (d + 1) * GROUP, :] = mix_recv[at, d].astype(F32)
                for e in range(halves):
                    lines = turn_lanes([
                        turn_ref[pl.ds(e * layers + n, GROUP, stride=GROUP), :]
                        for n in range(layers)
                    ])
                    for n in range(layers):
                        back_send[at, n, :, e * LANES : (e + 1) * LANES] = lines[n].astype(BF16)
        send_back(g, range(layers // 2))
        back_recv[span, z] = back_send[span, z]

    def give_high(g):
        send_back(g, range(layers // 2, layers - 1))

    def finish(g):
        first, size = BLOCKS[g]
        settle(back_recv.at[pl.ds(first, size), pl.ds(0, layers - 1)], back_sems.at[g])
        with scope("finish"):
            for at in range(first, first + size):
                p, q = at // parts, at % parts
                mixed = back_recv[at].reshape(width, block).astype(F32)
                centred = mixed - jnp.mean(mixed, axis=0, keepdims=True)
                scaled = centred * lax.rsqrt(
                    jnp.mean(centred * centred, axis=0, keepdims=True) + 1e-05
                )
                scaled = jnp.concatenate(
                    [scaled[:, e * LANES : (e + 1) * LANES] * mid_wide[...] for e in range(halves)],
                    axis=1,
                ).astype(BF16)
                result = lax.dot_general(
                    scaled, out_weight[...], (((0,), (0,)), ((), ())), preferred_element_type=F32
                )
                result = (result * gate_ref[p, q * block : (q + 1) * block, :]).astype(BF16)
                out_ref[
                    q * GROUP : (q + 1) * GROUP, p * GROUP : (p + 1) * GROUP, :
                ] = result.reshape(GROUP, GROUP, width)

    for p in range(parts):
        begin(p)
        if p == 0:
            with scope("bar"):
                pl.semaphore_wait(barrier, len(peers))
        for g, (first, size) in enumerate(LEFTS):
            if p * halves < first + size <= (p + 1) * halves:
                send_far(far_left, got_left, far_left_sems, g, pl.ds(first, size))
        begin_right(p)

    with scope("gate"):
        fetches[parts + 3].wait()
        for h in range(parts):
            gate_ref[h] = jax.nn.sigmoid(
                jnp.dot(ready_ref[h], out_gate[...], preferred_element_type=F32)
            )
        fetches[parts + 4].wait()
        mid_wide[...] = jnp.broadcast_to(mid_gain[...].reshape(1, width), (width, width)).T
        fetches[parts + 5].wait()

    for step in PLAN:
        todo = {
            "a": give_left, "r": pass_right, "f": pass_left, "m": meet, "c": give_back,
            "h": give_high, "d": finish,
        }[step[0]]
        todo(int(step[1:]))

    others = pl.ds(0, layers - 1)
    settle(far_left.at[:, others], sent(far_left_sems))
    settle(near_left.at[:, pl.ds(0, chips - 1)], sent(left_sems))
    settle(left_lines.at[:, pl.ds(0, chips)], sent(pass_sems))
    settle_some(met_right, pl.ds(0, parts), sent(near_right_sems))
    settle(far_right.at[:, others], sent(right_sems))
    settle(mix_send.at[:, pl.ds(0, chips - 1)], sent(mix_sems))
    settle(back_send.at[:, others], sent(back_sems))


def by_kernel(pair_state, in_gain, left_weight, right_weight, mid_gain, out_weight, out_gate):
    rows, cols, width = pair_state.shape
    chips = lax.axis_size("first")
    layers = lax.axis_size("second") // CORES
    count = cols * lax.axis_size("second")
    parts = rows // GROUP
    units = rows // UNIT
    block = GROUP * GROUP
    lanes = parts * block
    deep = parts * LANES
    changed = pl.pallas_call(
        functools.partial(triangle_kernel, layers, chips, count),
        out_shape=jax.ShapeDtypeStruct((rows, cols, width), BF16),
        in_specs=[pl.BlockSpec(memory_space=pltpu.MemorySpace.HBM)] * 7,
        out_specs=pl.BlockSpec(memory_space=pltpu.VMEM),
        scratch_shapes=[
            pltpu.VMEM((rows, cols, width), BF16),
            pltpu.VMEM((width,), F32),
            pltpu.VMEM(left_weight.shape, BF16),
            pltpu.VMEM(right_weight.shape, BF16),
            pltpu.VMEM((width,), F32),
            pltpu.VMEM(out_weight.shape, BF16),
            pltpu.VMEM(out_gate.shape, BF16),
            pltpu.SemaphoreType.DMA((parts + 6,)),
            pltpu.VMEM((width, width), BF16),
            pltpu.VMEM((width, width), BF16),
            pltpu.VMEM((width, width), F32),
            pltpu.VMEM((parts, GROUP * cols, width), F32),
            pltpu.VMEM((parts, rows * GROUP, width), BF16),
            pltpu.VMEM((parts, rows * GROUP, width), F32),
            pltpu.VMEM((cols * layers, LANES), F32),
            pltpu.VMEM((units, layers, GROUP, deep), BF16),
            pltpu.VMEM((units, layers, GROUP, deep), BF16),
            pltpu.VMEM((units, chips, UNIT, deep), BF16),
            pltpu.VMEM((units, CORES * chips, UNIT, deep), BF16),
            pltpu.VMEM((parts, chips, layers, lanes), BF16),
            pltpu.VMEM((parts, CORES * layers, layers, lanes), BF16),
            pltpu.VMEM((parts, layers, CORES, cols, LANES), BF16),
            pltpu.VMEM((parts, layers, CORES, cols, LANES), BF16),
            pltpu.VMEM((parts * parts, chips, GROUP, LANES), BF16),
            pltpu.VMEM((parts * parts, chips, GROUP, LANES), BF16),
            pltpu.VMEM((parts * parts, layers, GROUP, block), BF16),
            pltpu.VMEM((parts * parts, layers, GROUP, block), BF16),
            pltpu.SemaphoreType.DMA((len(LEFTS) + 1,)),
            pltpu.SemaphoreType.DMA((len(LEFTS) + 1,)),
            pltpu.SemaphoreType.DMA((len(LEFTS) + 1,)),
            pltpu.SemaphoreType.DMA((parts + 1,)),
            pltpu.SemaphoreType.DMA((parts + 1,)),
            pltpu.SemaphoreType.DMA((len(BLOCKS) + 1,)),
            pltpu.SemaphoreType.DMA((len(BLOCKS) + 1,)),
        ],
        compiler_params=pltpu.CompilerParams(
            collective_id=0, has_side_effects=True, vmem_limit_bytes=32 * 1024 * 1024
        ),
    )(
        *(
            pltpu.with_memory_space_constraint(value, pltpu.MemorySpace.HBM)
            for value in (
                pair_state, in_gain, left_weight, right_weight, mid_gain, out_weight, out_gate,
            )
        )
    )
    return changed


def unit_channels(values, channel_gain):
    centred = values - jnp.mean(values, axis=-1, keepdims=True)
    return (
        centred
        * lax.rsqrt(jnp.mean(centred * centred, axis=-1, keepdims=True) + 1e-05)
        * channel_gain
    )


def make_factors(pair_in, in_gain, left_weight, right_weight):
    ready = unit_channels(pair_in.astype(jnp.float32), in_gain).astype(jnp.bfloat16)
    ready = lax.optimization_barrier(ready)
    left = jnp.einsum("ijc,cd->ijd", ready, left_weight, preferred_element_type=jnp.float32)
    right = jnp.einsum("ijc,cd->ijd", ready, right_weight, preferred_element_type=jnp.float32)
    return (ready, left.astype(jnp.bfloat16), right.astype(jnp.bfloat16))


def finish_pair(mixed, ready, mid_gain, out_weight, out_gate):
    scaled = unit_channels(mixed.astype(jnp.float32), mid_gain).astype(jnp.bfloat16)
    scaled = lax.optimization_barrier(scaled)
    gate = jax.nn.sigmoid(
        jnp.einsum("ijc,cd->ijd", ready, out_gate, preferred_element_type=jnp.float32)
    )
    return (
        jnp.einsum("ijd,dc->ijc", scaled, out_weight, preferred_element_type=jnp.float32) * gate
    ).astype(jnp.bfloat16)


def by_collectives(pair_state, in_gain, left_weight, right_weight, mid_gain, out_weight, out_gate):
    ready, left, right = make_factors(pair_state, in_gain, left_weight, right_weight)
    count = pair_state.shape[1] * lax.axis_size("second")
    left_lines, right_lines = (
        lax.all_to_all(left, "second", split_axis=2, concat_axis=1, tiled=True),
        lax.all_to_all(right, "second", split_axis=2, concat_axis=1, tiled=True),
    )

    def meet(piece):
        return jnp.einsum("ikd,jkd->ijd", left_lines, piece, preferred_element_type=jnp.float32)

    strip = meet(lax.all_gather(right_lines, "first", axis=0, tiled=True))
    strip = (strip * count ** (-0.5)).astype(jnp.bfloat16)
    mixed = lax.all_to_all(strip, "second", split_axis=1, concat_axis=2, tiled=True)
    return finish_pair(mixed, ready, mid_gain, out_weight, out_gate)


def per_device(pair_state, *rest):
    groups, parts = lax.axis_size("first"), lax.axis_size("second")
    rows, cols, width = pair_state.shape
    left_out = rest[1].shape[1]
    fits = (
        groups == SIDE * SIDE
        and parts == CORES * 8
        and width == GROUP * 8
        and rows == cols
        and rows == 3 * GROUP
        and left_out == width
    )
    return (by_kernel if fits else by_collectives)(pair_state, *rest)


def solution(mesh):
    in_specs = (P("first", "second", None), P(), P(), P(), P(), P(), P())
    out_specs = P("first", "second", None)
    return jax.shard_map(
        per_device, mesh=mesh, in_specs=in_specs, out_specs=out_specs, check_vma=False
    )
```

```python
import functools

import jax
import jax.numpy as jnp
from jax import lax
from jax.experimental import pallas as pl
from jax.experimental.pallas import tpu as pltpu
from jax.sharding import PartitionSpec as P

MESH = pl.DeviceIdType.MESH
F32 = jnp.float32
BF16 = jnp.bfloat16
CORES = 2


SIDE = 4
LANES = 128
GROUP = 16
UNIT = 8
LEFTS = ((0, 1), (1, 1), (2, 1), (3, 1), (4, 1), (5, 1))
BLOCKS = ((0, 1), (1, 1), (2, 1), (3, 1), (4, 1), (5, 1), (6, 3))
PLAN = (
    "a0", "r0", "a1", "r1", "a2", "r2", "f0", "a3", "f1", "a4", "f2", "a5", "f3", "f4",
    "m0", "m1", "f5", "m2", "m3", "m4", "m5", "c0", "c1", "h0", "c2", "h1", "m6", "c3",
    "h2", "c4", "c5", "h3", "d0", "d1", "h4", "c6", "h5", "h6", "d2", "d3", "d4", "d5",
    "d6",
)


def unit_rows(values, channel_gain):
    centred = values - jnp.mean(values, axis=-1, keepdims=True)
    return (
        centred
        * lax.rsqrt(jnp.mean(centred * centred, axis=-1, keepdims=True) + 1e-05)
        * channel_gain
    )


def turn_lanes(parts):
    count = len(parts)
    wide = LANES // count
    group = lax.broadcasted_iota(jnp.int32, parts[0].shape, 1) // wide
    parts = list(parts)
    step = 1
    while step < count:
        low = group // step % 2 == 0
        for n in range(count):
            if n // step % 2 == 0:
                one, two = parts[n], parts[n + step]
                parts[n] = jnp.where(low, one, pltpu.roll(two, step * wide, 1))
                parts[n + step] = jnp.where(low, pltpu.roll(one, LANES - step * wide, 1), two)
        step *= 2
    return parts


def triangle_kernel(
    layers, chips, count,
    x_hbm, in_gain_hbm, left_weight_hbm, right_weight_hbm, mid_gain_hbm, out_weight_hbm,
    out_gate_hbm, out_ref,
    x_ref, in_gain, left_weight, right_weight, mid_gain, out_weight, out_gate, fetch_sems,
    left_rows, right_rows, mid_wide, whole_ref, ready_ref, gate_ref, turn_ref,
    far_left, got_left, near_left, left_lines,
    near_right, met_right, far_right, right_lines,
    mix_send, mix_recv, back_send, back_recv,
    far_left_sems, left_sems, pass_sems, near_right_sems, right_sems, mix_sems, back_sems,
):
    scope = jax.named_scope
    rows, cols, width = x_ref.shape
    parts = rows // GROUP
    units = rows // UNIT
    halves = GROUP // UNIT
    block = GROUP * GROUP
    a = lax.axis_index("first")
    b = lax.axis_index("second")
    z, c = b // CORES, b % CORES
    other = 1 - c
    y, x = a // SIDE, a % SIDE
    side = a % CORES
    pair = a // CORES

    def core_at(first, layer, core):
        return {"first": first, "second": layer * CORES + core}

    def layer_at(s):
        return lax.rem(z + s, layers)

    def chip_at(dy, dx):
        return lax.rem(y + dy, SIDE) * SIDE + lax.rem(x + dx, SIDE)

    hops = [(dy, dx) for dy in (2, 1, 3, 0) for dx in (2, 1, 3, 0) if (dy, dx) != (0, 0)]
    steps = [4, 3, 5, 2, 6, 1, 7]

    barrier = pltpu.get_barrier_semaphore()
    peers = [(0, core_at(a, z, other))]
    peers += [(min(s, layers - s), core_at(a, layer_at(s), c)) for s in steps]
    for dy, dx in hops:
        away = min(dy, SIDE - dy) + min(dx, SIDE - dx)
        peers += [(away, core_at(chip_at(dy, dx), z, core)) for core in (other, c)]
    peers = [peer for _, peer in sorted(peers, key=lambda pair: -pair[0])]
    for peer in peers:
        pl.semaphore_signal(barrier, inc=1, device_id=peer, device_id_type=MESH)

    fetches = [
        pltpu.make_async_copy(src, dst, fetch_sems.at[n])
        for n, (src, dst) in enumerate(
            [(x_hbm.at[pl.ds(p * GROUP, GROUP)], x_ref.at[pl.ds(p * GROUP, GROUP)]) for p in range(parts)]
            + [
                (in_gain_hbm, in_gain), (left_weight_hbm, left_weight),
                (right_weight_hbm, right_weight), (out_gate_hbm, out_gate),
                (mid_gain_hbm, mid_gain), (out_weight_hbm, out_weight),
            ]
        )
    ]
    for fetch in fetches:
        fetch.start()
    for fetch in fetches[parts : parts + 3]:
        fetch.wait()

    left_rows[...] = left_weight[...].astype(F32).T.astype(BF16)
    turn_ref[:width, :] = right_weight[...].astype(F32).T
    for d in range(chips):
        right_rows[d * layers : (d + 1) * layers, :] = turn_ref[
            pl.ds(d, layers, stride=chips), :
        ].astype(BF16)

    def send(src, dst, sems, at, peer):
        pltpu.make_async_remote_copy(
            src_ref=src, dst_ref=dst, send_sem=sems.at[sems.shape[0] - 1], recv_sem=sems.at[at],
            device_id=peer, device_id_type=MESH,
        ).start()

    def settle(like, sem):
        with scope("wait"):
            pltpu.make_async_copy(like, like, sem).wait()

    def settle_some(like, span, sem):
        @pl.when(c == side)
        def _():
            settle(like.at[span, pl.ds(0, chips - 1)], sem)

        @pl.when(c != side)
        def _():
            settle(like.at[span], sem)

    def sent(sems):
        return sems.at[sems.shape[0] - 1]

    def send_far(src, dst, sems, at, span):
        for s in steps:
            to = layer_at(s)
            send(src.at[span, to], dst.at[span, z], sems, at, core_at(a, to, c))
        dst[span, z] = src[span, z]

    def project(weight, lines):
        return lax.dot_general(
            weight, lines, (((1,), (1,)), ((), ())), preferred_element_type=F32
        ).astype(BF16)

    def begin(p):
        fetches[p].wait()
        values = x_ref[p * GROUP : (p + 1) * GROUP].astype(F32).reshape(GROUP * cols, width)
        ready = unit_rows(values, in_gain[...].reshape(1, width))
        whole_ref[p] = ready
        ready = ready.astype(BF16).reshape(GROUP, parts, GROUP, width)
        for h in range(parts):
            piece = ready[:, h].reshape(block, width)
            ready_ref[h, p * block : (p + 1) * block, :] = piece
            made = project(left_rows[...], piece)
            for e in range(halves):
                far_left[p * halves + e, :, :, h * LANES : (h + 1) * LANES] = made[
                    :, e * LANES : (e + 1) * LANES
                ].reshape(layers, GROUP, LANES)

    def begin_right(p):
        turned = jnp.concatenate(
            [whole_ref[p, pl.ds(k, GROUP, stride=cols), :].astype(BF16) for k in range(cols)], axis=0
        )
        near_right[p] = project(right_rows[...], turned).reshape(chips, layers, GROUP * cols)
        mine = c * layers + pair
        for hop in hops:
            to = chip_at(*hop)
            send(
                near_right.at[p, to], met_right.at[p, mine], near_right_sems, p,
                core_at(to, z, side),
            )

        @pl.when(c == side)
        def _():
            met_right[p, mine] = near_right[p, a]

        @pl.when(c != side)
        def _():
            send(
                near_right.at[p, a], met_right.at[p, mine], near_right_sems, p,
                core_at(a, z, other),
            )

    def pass_right(p):
        settle_some(met_right, pl.ds(p, 1), near_right_sems.at[p])
        tiles = GROUP * cols // LANES

        def body(core, carry):
            for h in range(tiles):
                lanes = slice(h * LANES, (h + 1) * LANES)
                lines = turn_lanes([
                    met_right[p, core * layers + n, :, lanes].astype(F32) for n in range(layers)
                ])
                for n in range(layers):
                    at = (h * layers + n) * layers
                    turn_ref[at : at + layers, :] = lines[n]
            for h in range(parts):
                for n in range(layers):
                    line = turn_ref[pl.ds(h * GROUP * layers + n, GROUP, stride=layers), :]
                    far_right[p, n, core, h * GROUP : (h + 1) * GROUP, :] = line.astype(BF16)
            return carry

        with scope("rturn"):
            lax.fori_loop(0, CORES, body, 0)
        send_far(far_right, right_lines, right_sems, p, pl.ds(p, 1))

    def give_left(g):
        first, size = LEFTS[g]
        span = pl.ds(first, size)
        settle(got_left.at[span, pl.ds(0, layers - 1)], far_left_sems.at[g])
        with scope("lturn"):
            for u in range(first, first + size):
                for h in range(parts):
                    lanes = slice(h * LANES, (h + 1) * LANES)
                    lines = turn_lanes([
                        got_left[u, n, :, lanes].astype(F32) for n in range(layers)
                    ])
                    for n in range(UNIT):
                        at = (h * UNIT + n) * GROUP
                        turn_ref[at : at + GROUP, :] = lines[n]
                    for d in range(GROUP):
                        line = turn_ref[pl.ds(h * UNIT * GROUP + d, UNIT, stride=GROUP), :]
                        near_left[u, d, :, lanes] = line.astype(BF16)
        mine = c * chips + a
        for hop in hops:
            to = chip_at(*hop)
            send(
                near_left.at[span, to], left_lines.at[span, mine], left_sems, g,
                core_at(to, z, c),
            )
        left_lines[span, mine] = near_left[span, a]

    def pass_left(g):
        first, size = LEFTS[g]
        span = pl.ds(first, size)
        settle(left_lines.at[span, pl.ds(0, chips - 1)], left_sems.at[g])
        with scope("pass"):
            own = left_lines.at[span, pl.ds(c * chips, chips)]
            send(own, own, pass_sems, g, core_at(a, z, other))

    deep = near_left.shape[-1]

    met = set()

    def meet(g):
        first, size = BLOCKS[g]
        span = pl.ds(first, size)
        for at in range(first, first + size):
            p, q = at // parts, at % parts
            for n, (unit, many) in enumerate(LEFTS):
                if unit < (q + 1) * halves and ("left", n) not in met:
                    met.add(("left", n))
                    settle(left_lines.at[pl.ds(unit, many), pl.ds(0, chips)], pass_sems.at[n])
            if ("right", p) not in met:
                met.add(("right", p))
                settle(right_lines.at[p, pl.ds(0, layers - 1)], right_sems.at[p])
            with scope("meet"):
                total = None
                for core in range(CORES):
                    left = left_lines[
                        q * halves : (q + 1) * halves, core * chips : (core + 1) * chips
                    ].reshape(block, deep)
                    right = jnp.concatenate(
                        [
                            right_lines[p, :, core, h * GROUP : (h + 1) * GROUP, :].reshape(LANES, LANES)
                            for h in range(parts)
                        ],
                        axis=0,
                    )
                    term = jnp.dot(left, right, preferred_element_type=F32)
                    total = term if total is None else total + term
                mixed = (total * count ** (-0.5)).astype(BF16)
                for e in range(halves):
                    mix_send[at, :, e * UNIT : (e + 1) * UNIT, :] = mixed[
                        e * LANES : (e + 1) * LANES
                    ].reshape(chips, UNIT, LANES)
        for hop in hops:
            to = chip_at(*hop)
            send(
                mix_send.at[span, to], mix_recv.at[span, a], mix_sems, g, core_at(to, z, c)
            )
        mix_recv[span, a] = mix_send[span, a]

    def send_back(g, order):
        span = pl.ds(*BLOCKS[g])
        for n in order:
            to = n + (n + layers - z) // layers
            send(
                back_send.at[span, to], back_recv.at[span, z], back_sems, g, core_at(a, to, c)
            )

    def give_back(g):
        first, size = BLOCKS[g]
        span = pl.ds(first, size)
        settle(mix_recv.at[span, pl.ds(0, chips - 1)], mix_sems.at[g])
        with scope("back"):
            for at in range(first, first + size):
                for d in range(GROUP):
                    turn_ref[d * GROUP : (d + 1) * GROUP, :] = mix_recv[at, d].astype(F32)
                for e in range(halves):
                    lines = turn_lanes([
                        turn_ref[pl.ds(e * layers + n, GROUP, stride=GROUP), :]
                        for n in range(layers)
                    ])
                    for n in range(layers):
                        back_send[at, n, :, e * LANES : (e + 1) * LANES] = lines[n].astype(BF16)
        send_back(g, range(layers // 2))
        back_recv[span, z] = back_send[span, z]

    def give_high(g):
        send_back(g, range(layers // 2, layers - 1))

    def finish(g):
        first, size = BLOCKS[g]
        settle(back_recv.at[pl.ds(first, size), pl.ds(0, layers - 1)], back_sems.at[g])
        with scope("finish"):
            for at in range(first, first + size):
                p, q = at // parts, at % parts
                mixed = back_recv[at].reshape(width, block).astype(F32)
                centred = mixed - jnp.mean(mixed, axis=0, keepdims=True)
                scaled = centred * lax.rsqrt(
                    jnp.mean(centred * centred, axis=0, keepdims=True) + 1e-05
                )
                scaled = jnp.concatenate(
                    [scaled[:, e * LANES : (e + 1) * LANES] * mid_wide[...] for e in range(halves)],
                    axis=1,
                ).astype(BF16)
                result = lax.dot_general(
                    scaled, out_weight[...], (((0,), (0,)), ((), ())), preferred_element_type=F32
                )
                result = (result * gate_ref[p, q * block : (q + 1) * block, :]).astype(BF16)
                out_ref[
                    q * GROUP : (q + 1) * GROUP, p * GROUP : (p + 1) * GROUP, :
                ] = result.reshape(GROUP, GROUP, width)

    for p in range(parts):
        begin(p)
        if p == 0:
            with scope("bar"):
                pl.semaphore_wait(barrier, len(peers))
        for g, (first, size) in enumerate(LEFTS):
            if p * halves < first + size <= (p + 1) * halves:
                send_far(far_left, got_left, far_left_sems, g, pl.ds(first, size))
        begin_right(p)

    with scope("gate"):
        fetches[parts + 3].wait()
        for h in range(parts):
            gate_ref[h] = jax.nn.sigmoid(
                jnp.dot(ready_ref[h], out_gate[...], preferred_element_type=F32)
            )
        fetches[parts + 4].wait()
        mid_wide[...] = jnp.broadcast_to(mid_gain[...].reshape(1, width), (width, width)).T
        fetches[parts + 5].wait()

    for step in PLAN:
        todo = {
            "a": give_left, "r": pass_right, "f": pass_left, "m": meet, "c": give_back,
            "h": give_high, "d": finish,
        }[step[0]]
        todo(int(step[1:]))

    others = pl.ds(0, layers - 1)
    settle(far_left.at[:, others], sent(far_left_sems))
    settle(near_left.at[:, pl.ds(0, chips - 1)], sent(left_sems))
    settle(left_lines.at[:, pl.ds(0, chips)], sent(pass_sems))
    settle_some(met_right, pl.ds(0, parts), sent(near_right_sems))
    settle(far_right.at[:, others], sent(right_sems))
    settle(mix_send.at[:, pl.ds(0, chips - 1)], sent(mix_sems))
    settle(back_send.at[:, others], sent(back_sems))


def by_kernel(pair_state, in_gain, left_weight, right_weight, mid_gain, out_weight, out_gate):
    rows, cols, width = pair_state.shape
    chips = lax.axis_size("first")
    layers = lax.axis_size("second") // CORES
    count = cols * lax.axis_size("second")
    parts = rows // GROUP
    units = rows // UNIT
    block = GROUP * GROUP
    lanes = parts * block
    deep = parts * LANES
    changed = pl.pallas_call(
        functools.partial(triangle_kernel, layers, chips, count),
        out_shape=jax.ShapeDtypeStruct((rows, cols, width), BF16),
        in_specs=[pl.BlockSpec(memory_space=pltpu.MemorySpace.HBM)] * 7,
        out_specs=pl.BlockSpec(memory_space=pltpu.VMEM),
        scratch_shapes=[
            pltpu.VMEM((rows, cols, width), BF16),
            pltpu.VMEM((width,), F32),
            pltpu.VMEM(left_weight.shape, BF16),
            pltpu.VMEM(right_weight.shape, BF16),
            pltpu.VMEM((width,), F32),
            pltpu.VMEM(out_weight.shape, BF16),
            pltpu.VMEM(out_gate.shape, BF16),
            pltpu.SemaphoreType.DMA((parts + 6,)),
            pltpu.VMEM((width, width), BF16),
            pltpu.VMEM((width, width), BF16),
            pltpu.VMEM((width, width), F32),
            pltpu.VMEM((parts, GROUP * cols, width), F32),
            pltpu.VMEM((parts, rows * GROUP, width), BF16),
            pltpu.VMEM((parts, rows * GROUP, width), F32),
            pltpu.VMEM((cols * layers, LANES), F32),
            pltpu.VMEM((units, layers, GROUP, deep), BF16),
            pltpu.VMEM((units, layers, GROUP, deep), BF16),
            pltpu.VMEM((units, chips, UNIT, deep), BF16),
            pltpu.VMEM((units, CORES * chips, UNIT, deep), BF16),
            pltpu.VMEM((parts, chips, layers, lanes), BF16),
            pltpu.VMEM((parts, CORES * layers, layers, lanes), BF16),
            pltpu.VMEM((parts, layers, CORES, cols, LANES), BF16),
            pltpu.VMEM((parts, layers, CORES, cols, LANES), BF16),
            pltpu.VMEM((parts * parts, chips, GROUP, LANES), BF16),
            pltpu.VMEM((parts * parts, chips, GROUP, LANES), BF16),
            pltpu.VMEM((parts * parts, layers, GROUP, block), BF16),
            pltpu.VMEM((parts * parts, layers, GROUP, block), BF16),
            pltpu.SemaphoreType.DMA((len(LEFTS) + 1,)),
            pltpu.SemaphoreType.DMA((len(LEFTS) + 1,)),
            pltpu.SemaphoreType.DMA((len(LEFTS) + 1,)),
            pltpu.SemaphoreType.DMA((parts + 1,)),
            pltpu.SemaphoreType.DMA((parts + 1,)),
            pltpu.SemaphoreType.DMA((len(BLOCKS) + 1,)),
            pltpu.SemaphoreType.DMA((len(BLOCKS) + 1,)),
        ],
        compiler_params=pltpu.CompilerParams(
            collective_id=0, has_side_effects=True, vmem_limit_bytes=32 * 1024 * 1024
        ),
    )(
        *(
            pltpu.with_memory_space_constraint(value, pltpu.MemorySpace.HBM)
            for value in (
                pair_state, in_gain, left_weight, right_weight, mid_gain, out_weight, out_gate,
            )
        )
    )
    return changed


def unit_channels(values, channel_gain):
    centred = values - jnp.mean(values, axis=-1, keepdims=True)
    return (
        centred
        * lax.rsqrt(jnp.mean(centred * centred, axis=-1, keepdims=True) + 1e-05)
        * channel_gain
    )


def make_factors(pair_in, in_gain, left_weight, right_weight):
    ready = unit_channels(pair_in.astype(jnp.float32), in_gain).astype(jnp.bfloat16)
    ready = lax.optimization_barrier(ready)
    left = jnp.einsum("ijc,cd->ijd", ready, left_weight, preferred_element_type=jnp.float32)
    right = jnp.einsum("ijc,cd->ijd", ready, right_weight, preferred_element_type=jnp.float32)
    return (ready, left.astype(jnp.bfloat16), right.astype(jnp.bfloat16))


def finish_pair(mixed, ready, mid_gain, out_weight, out_gate):
    scaled = unit_channels(mixed.astype(jnp.float32), mid_gain).astype(jnp.bfloat16)
    scaled = lax.optimization_barrier(scaled)
    gate = jax.nn.sigmoid(
        jnp.einsum("ijc,cd->ijd", ready, out_gate, preferred_element_type=jnp.float32)
    )
    return (
        jnp.einsum("ijd,dc->ijc", scaled, out_weight, preferred_element_type=jnp.float32) * gate
    ).astype(jnp.bfloat16)


def by_collectives(pair_state, in_gain, left_weight, right_weight, mid_gain, out_weight, out_gate):
    ready, left, right = make_factors(pair_state, in_gain, left_weight, right_weight)
    count = pair_state.shape[1] * lax.axis_size("second")
    left_lines, right_lines = (
        lax.all_to_all(left, "second", split_axis=2, concat_axis=1, tiled=True),
        lax.all_to_all(right, "second", split_axis=2, concat_axis=1, tiled=True),
    )

    def meet(piece):
        return jnp.einsum("ikd,jkd->ijd", left_lines, piece, preferred_element_type=jnp.float32)

    strip = meet(lax.all_gather(right_lines, "first", axis=0, tiled=True))
    strip = (strip * count ** (-0.5)).astype(jnp.bfloat16)
    mixed = lax.all_to_all(strip, "second", split_axis=1, concat_axis=2, tiled=True)
    return finish_pair(mixed, ready, mid_gain, out_weight, out_gate)


def per_device(pair_state, *rest):
    groups, parts = lax.axis_size("first"), lax.axis_size("second")
    rows, cols, width = pair_state.shape
    left_out = rest[1].shape[1]
    fits = (
        groups == SIDE * SIDE
        and parts == CORES * 8
        and width == GROUP * 8
        and rows == cols
        and rows == 3 * GROUP
        and left_out == width
    )
    return (by_kernel if fits else by_collectives)(pair_state, *rest)


def solution(mesh):
    in_specs = (P("first", "second", None), P(), P(), P(), P(), P(), P())
    out_specs = P("first", "second", None)
    return jax.shard_map(
        per_device, mesh=mesh, in_specs=in_specs, out_specs=out_specs, check_vma=False
    )
```

```python
import functools

import jax
import jax.numpy as jnp
from jax import lax
from jax.experimental import pallas as pl
from jax.experimental.pallas import tpu as pltpu
from jax.sharding import PartitionSpec as P

MESH = pl.DeviceIdType.MESH
F32 = jnp.float32
BF16 = jnp.bfloat16
CORES = 2


SIDE = 4
LANES = 128
GROUP = 16
UNIT = 8
LEFTS = ((0, 1), (1, 1), (2, 1), (3, 1), (4, 1), (5, 1))
BLOCKS = ((0, 1), (1, 1), (2, 1), (3, 1), (4, 1), (5, 1), (6, 3))
PLAN = (
    "a0", "a1", "r0", "r1", "a2", "r2", "a3", "f0", "f1", "a4", "f2", "a5", "f3", "f4",
    "m0", "m1", "f5", "m2", "m3", "m4", "m5", "c0", "c1", "h0", "c2", "h1", "m6", "c3",
    "h2", "c4", "c5", "h3", "d0", "d1", "h4", "c6", "h5", "h6", "d2", "d3", "d4", "d5",
    "d6",
)


def unit_rows(values, channel_gain):
    centred = values - jnp.mean(values, axis=-1, keepdims=True)
    return (
        centred
        * lax.rsqrt(jnp.mean(centred * centred, axis=-1, keepdims=True) + 1e-05)
        * channel_gain
    )


def turn_lanes(parts):
    count = len(parts)
    wide = LANES // count
    group = lax.broadcasted_iota(jnp.int32, parts[0].shape, 1) // wide
    parts = list(parts)
    step = 1
    while step < count:
        low = group // step % 2 == 0
        for n in range(count):
            if n // step % 2 == 0:
                one, two = parts[n], parts[n + step]
                parts[n] = jnp.where(low, one, pltpu.roll(two, step * wide, 1))
                parts[n + step] = jnp.where(low, pltpu.roll(one, LANES - step * wide, 1), two)
        step *= 2
    return parts


def triangle_kernel(
    layers, chips, count,
    x_hbm, in_gain_hbm, left_weight_hbm, right_weight_hbm, mid_gain_hbm, out_weight_hbm,
    out_gate_hbm, out_ref,
    x_ref, in_gain, left_weight, right_weight, mid_gain, out_weight, out_gate, fetch_sems,
    left_rows, right_rows, mid_wide, whole_ref, ready_ref, gate_ref, turn_ref,
    far_left, got_left, near_left, left_lines,
    near_right, met_right, far_right, right_lines,
    mix_send, mix_recv, back_send, back_recv,
    far_left_sems, left_sems, pass_sems, near_right_sems, right_sems, mix_sems, back_sems,
):
    scope = jax.named_scope
    rows, cols, width = x_ref.shape
    parts = rows // GROUP
    units = rows // UNIT
    halves = GROUP // UNIT
    block = GROUP * GROUP
    a = lax.axis_index("first")
    b = lax.axis_index("second")
    z, c = b // CORES, b % CORES
    other = 1 - c
    y, x = a // SIDE, a % SIDE
    side = a % CORES
    pair = a // CORES

    def core_at(first, layer, core):
        return {"first": first, "second": layer * CORES + core}

    def layer_at(s):
        return lax.rem(z + s, layers)

    def chip_at(dy, dx):
        return lax.rem(y + dy, SIDE) * SIDE + lax.rem(x + dx, SIDE)

    hops = [(dy, dx) for dy in (2, 1, 3, 0) for dx in (2, 1, 3, 0) if (dy, dx) != (0, 0)]
    steps = [4, 3, 5, 2, 6, 1, 7]

    barrier = pltpu.get_barrier_semaphore()
    peers = [(0, core_at(a, z, other))]
    peers += [(min(s, layers - s), core_at(a, layer_at(s), c)) for s in steps]
    for dy, dx in hops:
        away = min(dy, SIDE - dy) + min(dx, SIDE - dx)
        peers += [(away, core_at(chip_at(dy, dx), z, core)) for core in (other, c)]
    peers = [peer for _, peer in sorted(peers, key=lambda pair: -pair[0])]
    for peer in peers:
        pl.semaphore_signal(barrier, inc=1, device_id=peer, device_id_type=MESH)

    fetches = [
        pltpu.make_async_copy(src, dst, fetch_sems.at[n])
        for n, (src, dst) in enumerate(
            [(x_hbm.at[pl.ds(p * GROUP, GROUP)], x_ref.at[pl.ds(p * GROUP, GROUP)]) for p in range(parts)]
            + [
                (in_gain_hbm, in_gain), (left_weight_hbm, left_weight),
                (right_weight_hbm, right_weight), (out_gate_hbm, out_gate),
                (mid_gain_hbm, mid_gain), (out_weight_hbm, out_weight),
            ]
        )
    ]
    for fetch in fetches:
        fetch.start()
    for fetch in fetches[parts : parts + 3]:
        fetch.wait()

    left_rows[...] = left_weight[...].astype(F32).T.astype(BF16)
    turn_ref[:width, :] = right_weight[...].astype(F32).T
    for d in range(chips):
        right_rows[d * layers : (d + 1) * layers, :] = turn_ref[
            pl.ds(d, layers, stride=chips), :
        ].astype(BF16)

    def send(src, dst, sems, at, peer):
        pltpu.make_async_remote_copy(
            src_ref=src, dst_ref=dst, send_sem=sems.at[sems.shape[0] - 1], recv_sem=sems.at[at],
            device_id=peer, device_id_type=MESH,
        ).start()

    def settle(like, sem):
        with scope("wait"):
            pltpu.make_async_copy(like, like, sem).wait()

    def settle_some(like, span, sem):
        @pl.when(c == side)
        def _():
            settle(like.at[span, pl.ds(0, chips - 1)], sem)

        @pl.when(c != side)
        def _():
            settle(like.at[span], sem)

    def sent(sems):
        return sems.at[sems.shape[0] - 1]

    def send_far(src, dst, sems, at, span):
        for s in steps:
            to = layer_at(s)
            send(src.at[span, to], dst.at[span, z], sems, at, core_at(a, to, c))
        dst[span, z] = src[span, z]

    def project(weight, lines):
        return lax.dot_general(
            weight, lines, (((1,), (1,)), ((), ())), preferred_element_type=F32
        ).astype(BF16)

    def begin(p):
        fetches[p].wait()
        values = x_ref[p * GROUP : (p + 1) * GROUP].astype(F32).reshape(GROUP * cols, width)
        ready = unit_rows(values, in_gain[...].reshape(1, width))
        whole_ref[p] = ready
        ready = ready.astype(BF16).reshape(GROUP, parts, GROUP, width)
        for h in range(parts):
            piece = ready[:, h].reshape(block, width)
            ready_ref[h, p * block : (p + 1) * block, :] = piece
            made = project(left_rows[...], piece)
            for e in range(halves):
                far_left[p * halves + e, :, :, h * LANES : (h + 1) * LANES] = made[
                    :, e * LANES : (e + 1) * LANES
                ].reshape(layers, GROUP, LANES)

    def begin_right(p):
        turned = jnp.concatenate(
            [whole_ref[p, pl.ds(k, GROUP, stride=cols), :].astype(BF16) for k in range(cols)], axis=0
        )
        near_right[p] = project(right_rows[...], turned).reshape(chips, layers, GROUP * cols)
        mine = c * layers + pair
        for hop in hops:
            to = chip_at(*hop)
            send(
                near_right.at[p, to], met_right.at[p, mine], near_right_sems, p,
                core_at(to, z, side),
            )

        @pl.when(c == side)
        def _():
            met_right[p, mine] = near_right[p, a]

        @pl.when(c != side)
        def _():
            send(
                near_right.at[p, a], met_right.at[p, mine], near_right_sems, p,
                core_at(a, z, other),
            )

    def pass_right(p):
        settle_some(met_right, pl.ds(p, 1), near_right_sems.at[p])
        tiles = GROUP * cols // LANES

        def body(core, carry):
            for h in range(tiles):
                lanes = slice(h * LANES, (h + 1) * LANES)
                lines = turn_lanes([
                    met_right[p, core * layers + n, :, lanes].astype(F32) for n in range(layers)
                ])
                for n in range(layers):
                    at = (h * layers + n) * layers
                    turn_ref[at : at + layers, :] = lines[n]
            for h in range(parts):
                for n in range(layers):
                    line = turn_ref[pl.ds(h * GROUP * layers + n, GROUP, stride=layers), :]
                    far_right[p, n, core, h * GROUP : (h + 1) * GROUP, :] = line.astype(BF16)
            return carry

        with scope("rturn"):
            lax.fori_loop(0, CORES, body, 0)
        send_far(far_right, right_lines, right_sems, p, pl.ds(p, 1))

    def give_left(g):
        first, size = LEFTS[g]
        span = pl.ds(first, size)
        settle(got_left.at[span, pl.ds(0, layers - 1)], far_left_sems.at[g])
        with scope("lturn"):
            for u in range(first, first + size):
                for h in range(parts):
                    lanes = slice(h * LANES, (h + 1) * LANES)
                    lines = turn_lanes([
                        got_left[u, n, :, lanes].astype(F32) for n in range(layers)
                    ])
                    for n in range(UNIT):
                        at = (h * UNIT + n) * GROUP
                        turn_ref[at : at + GROUP, :] = lines[n]
                    for d in range(GROUP):
                        line = turn_ref[pl.ds(h * UNIT * GROUP + d, UNIT, stride=GROUP), :]
                        near_left[u, d, :, lanes] = line.astype(BF16)
        mine = c * chips + a
        for hop in hops:
            to = chip_at(*hop)
            send(
                near_left.at[span, to], left_lines.at[span, mine], left_sems, g,
                core_at(to, z, c),
            )
        left_lines[span, mine] = near_left[span, a]

    def pass_left(g):
        first, size = LEFTS[g]
        span = pl.ds(first, size)
        settle(left_lines.at[span, pl.ds(0, chips - 1)], left_sems.at[g])
        with scope("pass"):
            own = left_lines.at[span, pl.ds(c * chips, chips)]
            send(own, own, pass_sems, g, core_at(a, z, other))

    deep = near_left.shape[-1]

    met = set()

    def meet(g):
        first, size = BLOCKS[g]
        span = pl.ds(first, size)
        for at in range(first, first + size):
            p, q = at // parts, at % parts
            for n, (unit, many) in enumerate(LEFTS):
                if unit < (q + 1) * halves and ("left", n) not in met:
                    met.add(("left", n))
                    settle(left_lines.at[pl.ds(unit, many), pl.ds(0, chips)], pass_sems.at[n])
            if ("right", p) not in met:
                met.add(("right", p))
                settle(right_lines.at[p, pl.ds(0, layers - 1)], right_sems.at[p])
            with scope("meet"):
                total = None
                for core in range(CORES):
                    left = left_lines[
                        q * halves : (q + 1) * halves, core * chips : (core + 1) * chips
                    ].reshape(block, deep)
                    right = jnp.concatenate(
                        [
                            right_lines[p, :, core, h * GROUP : (h + 1) * GROUP, :].reshape(LANES, LANES)
                            for h in range(parts)
                        ],
                        axis=0,
                    )
                    term = jnp.dot(left, right, preferred_element_type=F32)
                    total = term if total is None else total + term
                mixed = (total * count ** (-0.5)).astype(BF16)
                for e in range(halves):
                    mix_send[at, :, e * UNIT : (e + 1) * UNIT, :] = mixed[
                        e * LANES : (e + 1) * LANES
                    ].reshape(chips, UNIT, LANES)
        for hop in hops:
            to = chip_at(*hop)
            send(
                mix_send.at[span, to], mix_recv.at[span, a], mix_sems, g, core_at(to, z, c)
            )
        mix_recv[span, a] = mix_send[span, a]

    def send_back(g, order):
        span = pl.ds(*BLOCKS[g])
        for n in order:
            to = n + (n + layers - z) // layers
            send(
                back_send.at[span, to], back_recv.at[span, z], back_sems, g, core_at(a, to, c)
            )

    def give_back(g):
        first, size = BLOCKS[g]
        span = pl.ds(first, size)
        settle(mix_recv.at[span, pl.ds(0, chips - 1)], mix_sems.at[g])
        with scope("back"):
            for at in range(first, first + size):
                for d in range(GROUP):
                    turn_ref[d * GROUP : (d + 1) * GROUP, :] = mix_recv[at, d].astype(F32)
                for e in range(halves):
                    lines = turn_lanes([
                        turn_ref[pl.ds(e * layers + n, GROUP, stride=GROUP), :]
                        for n in range(layers)
                    ])
                    for n in range(layers):
                        back_send[at, n, :, e * LANES : (e + 1) * LANES] = lines[n].astype(BF16)
        send_back(g, range(layers // 2))
        back_recv[span, z] = back_send[span, z]

    def give_high(g):
        send_back(g, range(layers // 2, layers - 1))

    def finish(g):
        first, size = BLOCKS[g]
        settle(back_recv.at[pl.ds(first, size), pl.ds(0, layers - 1)], back_sems.at[g])
        with scope("finish"):
            for at in range(first, first + size):
                p, q = at // parts, at % parts
                mixed = back_recv[at].reshape(width, block).astype(F32)
                centred = mixed - jnp.mean(mixed, axis=0, keepdims=True)
                scaled = centred * lax.rsqrt(
                    jnp.mean(centred * centred, axis=0, keepdims=True) + 1e-05
                )
                scaled = jnp.concatenate(
                    [scaled[:, e * LANES : (e + 1) * LANES] * mid_wide[...] for e in range(halves)],
                    axis=1,
                ).astype(BF16)
                result = lax.dot_general(
                    scaled, out_weight[...], (((0,), (0,)), ((), ())), preferred_element_type=F32
                )
                result = (result * gate_ref[p, q * block : (q + 1) * block, :]).astype(BF16)
                out_ref[
                    q * GROUP : (q + 1) * GROUP, p * GROUP : (p + 1) * GROUP, :
                ] = result.reshape(GROUP, GROUP, width)

    for p in range(parts):
        begin(p)
        if p == 0:
            with scope("bar"):
                pl.semaphore_wait(barrier, len(peers))
        for g, (first, size) in enumerate(LEFTS):
            if p * halves < first + size <= (p + 1) * halves:
                send_far(far_left, got_left, far_left_sems, g, pl.ds(first, size))
        begin_right(p)

    with scope("gate"):
        fetches[parts + 3].wait()
        for h in range(parts):
            gate_ref[h] = jax.nn.sigmoid(
                jnp.dot(ready_ref[h], out_gate[...], preferred_element_type=F32)
            )
        fetches[parts + 4].wait()
        mid_wide[...] = jnp.broadcast_to(mid_gain[...].reshape(1, width), (width, width)).T
        fetches[parts + 5].wait()

    for step in PLAN:
        todo = {
            "a": give_left, "r": pass_right, "f": pass_left, "m": meet, "c": give_back,
            "h": give_high, "d": finish,
        }[step[0]]
        todo(int(step[1:]))

    others = pl.ds(0, layers - 1)
    settle(far_left.at[:, others], sent(far_left_sems))
    settle(near_left.at[:, pl.ds(0, chips - 1)], sent(left_sems))
    settle(left_lines.at[:, pl.ds(0, chips)], sent(pass_sems))
    settle_some(met_right, pl.ds(0, parts), sent(near_right_sems))
    settle(far_right.at[:, others], sent(right_sems))
    settle(mix_send.at[:, pl.ds(0, chips - 1)], sent(mix_sems))
    settle(back_send.at[:, others], sent(back_sems))


def by_kernel(pair_state, in_gain, left_weight, right_weight, mid_gain, out_weight, out_gate):
    rows, cols, width = pair_state.shape
    chips = lax.axis_size("first")
    layers = lax.axis_size("second") // CORES
    count = cols * lax.axis_size("second")
    parts = rows // GROUP
    units = rows // UNIT
    block = GROUP * GROUP
    lanes = parts * block
    deep = parts * LANES
    changed = pl.pallas_call(
        functools.partial(triangle_kernel, layers, chips, count),
        out_shape=jax.ShapeDtypeStruct((rows, cols, width), BF16),
        in_specs=[pl.BlockSpec(memory_space=pltpu.MemorySpace.HBM)] * 7,
        out_specs=pl.BlockSpec(memory_space=pltpu.VMEM),
        scratch_shapes=[
            pltpu.VMEM((rows, cols, width), BF16),
            pltpu.VMEM((width,), F32),
            pltpu.VMEM(left_weight.shape, BF16),
            pltpu.VMEM(right_weight.shape, BF16),
            pltpu.VMEM((width,), F32),
            pltpu.VMEM(out_weight.shape, BF16),
            pltpu.VMEM(out_gate.shape, BF16),
            pltpu.SemaphoreType.DMA((parts + 6,)),
            pltpu.VMEM((width, width), BF16),
            pltpu.VMEM((width, width), BF16),
            pltpu.VMEM((width, width), F32),
            pltpu.VMEM((parts, GROUP * cols, width), F32),
            pltpu.VMEM((parts, rows * GROUP, width), BF16),
            pltpu.VMEM((parts, rows * GROUP, width), F32),
            pltpu.VMEM((cols * layers, LANES), F32),
            pltpu.VMEM((units, layers, GROUP, deep), BF16),
            pltpu.VMEM((units, layers, GROUP, deep), BF16),
            pltpu.VMEM((units, chips, UNIT, deep), BF16),
            pltpu.VMEM((units, CORES * chips, UNIT, deep), BF16),
            pltpu.VMEM((parts, chips, layers, lanes), BF16),
            pltpu.VMEM((parts, CORES * layers, layers, lanes), BF16),
            pltpu.VMEM((parts, layers, CORES, cols, LANES), BF16),
            pltpu.VMEM((parts, layers, CORES, cols, LANES), BF16),
            pltpu.VMEM((parts * parts, chips, GROUP, LANES), BF16),
            pltpu.VMEM((parts * parts, chips, GROUP, LANES), BF16),
            pltpu.VMEM((parts * parts, layers, GROUP, block), BF16),
            pltpu.VMEM((parts * parts, layers, GROUP, block), BF16),
            pltpu.SemaphoreType.DMA((len(LEFTS) + 1,)),
            pltpu.SemaphoreType.DMA((len(LEFTS) + 1,)),
            pltpu.SemaphoreType.DMA((len(LEFTS) + 1,)),
            pltpu.SemaphoreType.DMA((parts + 1,)),
            pltpu.SemaphoreType.DMA((parts + 1,)),
            pltpu.SemaphoreType.DMA((len(BLOCKS) + 1,)),
            pltpu.SemaphoreType.DMA((len(BLOCKS) + 1,)),
        ],
        compiler_params=pltpu.CompilerParams(
            collective_id=0, has_side_effects=True, vmem_limit_bytes=32 * 1024 * 1024
        ),
    )(
        *(
            pltpu.with_memory_space_constraint(value, pltpu.MemorySpace.HBM)
            for value in (
                pair_state, in_gain, left_weight, right_weight, mid_gain, out_weight, out_gate,
            )
        )
    )
    return changed


def unit_channels(values, channel_gain):
    centred = values - jnp.mean(values, axis=-1, keepdims=True)
    return (
        centred
        * lax.rsqrt(jnp.mean(centred * centred, axis=-1, keepdims=True) + 1e-05)
        * channel_gain
    )


def make_factors(pair_in, in_gain, left_weight, right_weight):
    ready = unit_channels(pair_in.astype(jnp.float32), in_gain).astype(jnp.bfloat16)
    ready = lax.optimization_barrier(ready)
    left = jnp.einsum("ijc,cd->ijd", ready, left_weight, preferred_element_type=jnp.float32)
    right = jnp.einsum("ijc,cd->ijd", ready, right_weight, preferred_element_type=jnp.float32)
    return (ready, left.astype(jnp.bfloat16), right.astype(jnp.bfloat16))


def finish_pair(mixed, ready, mid_gain, out_weight, out_gate):
    scaled = unit_channels(mixed.astype(jnp.float32), mid_gain).astype(jnp.bfloat16)
    scaled = lax.optimization_barrier(scaled)
    gate = jax.nn.sigmoid(
        jnp.einsum("ijc,cd->ijd", ready, out_gate, preferred_element_type=jnp.float32)
    )
    return (
        jnp.einsum("ijd,dc->ijc", scaled, out_weight, preferred_element_type=jnp.float32) * gate
    ).astype(jnp.bfloat16)


def by_collectives(pair_state, in_gain, left_weight, right_weight, mid_gain, out_weight, out_gate):
    ready, left, right = make_factors(pair_state, in_gain, left_weight, right_weight)
    count = pair_state.shape[1] * lax.axis_size("second")
    left_lines, right_lines = (
        lax.all_to_all(left, "second", split_axis=2, concat_axis=1, tiled=True),
        lax.all_to_all(right, "second", split_axis=2, concat_axis=1, tiled=True),
    )

    def meet(piece):
        return jnp.einsum("ikd,jkd->ijd", left_lines, piece, preferred_element_type=jnp.float32)

    strip = meet(lax.all_gather(right_lines, "first", axis=0, tiled=True))
    strip = (strip * count ** (-0.5)).astype(jnp.bfloat16)
    mixed = lax.all_to_all(strip, "second", split_axis=1, concat_axis=2, tiled=True)
    return finish_pair(mixed, ready, mid_gain, out_weight, out_gate)


def per_device(pair_state, *rest):
    groups, parts = lax.axis_size("first"), lax.axis_size("second")
    rows, cols, width = pair_state.shape
    left_out = rest[1].shape[1]
    fits = (
        groups == SIDE * SIDE
        and parts == CORES * 8
        and width == GROUP * 8
        and rows == cols
        and rows == 3 * GROUP
        and left_out == width
    )
    return (by_kernel if fits else by_collectives)(pair_state, *rest)


def solution(mesh):
    in_specs = (P("first", "second", None), P(), P(), P(), P(), P(), P())
    out_specs = P("first", "second", None)
    return jax.shard_map(
        per_device, mesh=mesh, in_specs=in_specs, out_specs=out_specs, check_vma=False
    )
```

```python
import functools

import jax
import jax.numpy as jnp
from jax import lax
from jax.experimental import pallas as pl
from jax.experimental.pallas import tpu as pltpu
from jax.sharding import PartitionSpec as P

MESH = pl.DeviceIdType.MESH
F32 = jnp.float32
BF16 = jnp.bfloat16
CORES = 2


SIDE = 4
LANES = 128
GROUP = 16
UNIT = 8
LEFTS = ((0, 1), (1, 1), (2, 1), (3, 1), (4, 1), (5, 1))
BLOCKS = ((0, 1), (1, 1), (2, 1), (3, 1), (4, 1), (5, 1), (6, 3))
PLAN = (
    "a0", "a1", "r0", "r1", "a2", "r2", "a3", "f0", "f1", "a4", "f2", "a5", "f3", "f4",
    "m0", "m1", "f5", "m2", "m3", "m4", "m5", "c0", "c1", "h0", "c2", "h1", "m6", "c3",
    "h2", "c4", "c5", "h3", "d0", "d1", "h4", "c6", "h5", "h6", "d2", "d3", "d4", "d5",
    "d6",
)


def unit_rows(values, channel_gain):
    centred = values - jnp.mean(values, axis=-1, keepdims=True)
    return (
        centred
        * lax.rsqrt(jnp.mean(centred * centred, axis=-1, keepdims=True) + 1e-05)
        * channel_gain
    )


def turn_lanes(parts):
    count = len(parts)
    wide = LANES // count
    group = lax.broadcasted_iota(jnp.int32, parts[0].shape, 1) // wide
    parts = list(parts)
    step = 1
    while step < count:
        low = group // step % 2 == 0
        for n in range(count):
            if n // step % 2 == 0:
                one, two = parts[n], parts[n + step]
                parts[n] = jnp.where(low, one, pltpu.roll(two, step * wide, 1))
                parts[n + step] = jnp.where(low, pltpu.roll(one, LANES - step * wide, 1), two)
        step *= 2
    return parts


def triangle_kernel(
    layers, chips, count,
    x_hbm, in_gain_hbm, left_weight_hbm, right_weight_hbm, mid_gain_hbm, out_weight_hbm,
    out_gate_hbm, out_ref,
    x_ref, in_gain, left_weight, right_weight, mid_gain, out_weight, out_gate, fetch_sems,
    left_rows, right_rows, mid_wide, whole_ref, ready_ref, gate_ref, turn_ref,
    far_left, got_left, near_left, left_lines,
    near_right, met_right, far_right, right_lines,
    mix_send, mix_recv, back_send, back_recv,
    far_left_sems, left_sems, pass_sems, near_right_sems, right_sems, mix_sems, back_sems,
):
    scope = jax.named_scope
    rows, cols, width = x_ref.shape
    parts = rows // GROUP
    units = rows // UNIT
    halves = GROUP // UNIT
    block = GROUP * GROUP
    a = lax.axis_index("first")
    b = lax.axis_index("second")
    z, c = b // CORES, b % CORES
    other = 1 - c
    y, x = a // SIDE, a % SIDE
    side = a % CORES
    pair = a // CORES

    def core_at(first, layer, core):
        return {"first": first, "second": layer * CORES + core}

    def layer_at(s):
        return lax.rem(z + s, layers)

    def chip_at(dy, dx):
        return lax.rem(y + dy, SIDE) * SIDE + lax.rem(x + dx, SIDE)

    hops = [(dy, dx) for dy in (2, 1, 3, 0) for dx in (2, 1, 3, 0) if (dy, dx) != (0, 0)]
    steps = [4, 3, 5, 2, 6, 1, 7]

    barrier = pltpu.get_barrier_semaphore()
    peers = [(0, core_at(a, z, other))]
    peers += [(min(s, layers - s), core_at(a, layer_at(s), c)) for s in steps]
    for dy, dx in hops:
        away = min(dy, SIDE - dy) + min(dx, SIDE - dx)
        peers += [(away, core_at(chip_at(dy, dx), z, core)) for core in (other, c)]
    peers = [peer for _, peer in sorted(peers, key=lambda pair: -pair[0])]
    for peer in peers:
        pl.semaphore_signal(barrier, inc=1, device_id=peer, device_id_type=MESH)

    fetches = [
        pltpu.make_async_copy(src, dst, fetch_sems.at[n])
        for n, (src, dst) in enumerate(
            [(x_hbm.at[pl.ds(p * GROUP, GROUP)], x_ref.at[pl.ds(p * GROUP, GROUP)]) for p in range(parts)]
            + [
                (in_gain_hbm, in_gain), (left_weight_hbm, left_weight),
                (right_weight_hbm, right_weight), (out_gate_hbm, out_gate),
                (mid_gain_hbm, mid_gain), (out_weight_hbm, out_weight),
            ]
        )
    ]
    for fetch in fetches:
        fetch.start()
    for fetch in fetches[parts : parts + 3]:
        fetch.wait()

    left_rows[...] = left_weight[...].astype(F32).T.astype(BF16)
    turn_ref[:width, :] = right_weight[...].astype(F32).T
    for d in range(chips):
        right_rows[d * layers : (d + 1) * layers, :] = turn_ref[
            pl.ds(d, layers, stride=chips), :
        ].astype(BF16)

    def send(src, dst, sems, at, peer):
        pltpu.make_async_remote_copy(
            src_ref=src, dst_ref=dst, send_sem=sems.at[sems.shape[0] - 1], recv_sem=sems.at[at],
            device_id=peer, device_id_type=MESH,
        ).start()

    def settle(like, sem):
        with scope("wait"):
            pltpu.make_async_copy(like, like, sem).wait()

    def settle_some(like, span, sem):
        @pl.when(c == side)
        def _():
            settle(like.at[span, pl.ds(0, chips - 1)], sem)

        @pl.when(c != side)
        def _():
            settle(like.at[span], sem)

    def sent(sems):
        return sems.at[sems.shape[0] - 1]

    def send_far(src, dst, sems, at, span):
        for s in steps:
            to = layer_at(s)
            send(src.at[span, to], dst.at[span, z], sems, at, core_at(a, to, c))
        dst[span, z] = src[span, z]

    def project(weight, lines):
        return lax.dot_general(
            weight, lines, (((1,), (1,)), ((), ())), preferred_element_type=F32
        ).astype(BF16)

    def begin(p):
        fetches[p].wait()
        values = x_ref[p * GROUP : (p + 1) * GROUP].astype(F32).reshape(GROUP * cols, width)
        ready = unit_rows(values, in_gain[...].reshape(1, width))
        whole_ref[p] = ready
        ready = ready.astype(BF16).reshape(GROUP, parts, GROUP, width)
        for h in range(parts):
            piece = ready[:, h].reshape(block, width)
            ready_ref[h, p * block : (p + 1) * block, :] = piece
            made = project(left_rows[...], piece)
            for e in range(halves):
                far_left[p * halves + e, :, :, h * LANES : (h + 1) * LANES] = made[
                    :, e * LANES : (e + 1) * LANES
                ].reshape(layers, GROUP, LANES)

    def begin_right(p):
        turned = jnp.concatenate(
            [whole_ref[p, pl.ds(k, GROUP, stride=cols), :].astype(BF16) for k in range(cols)], axis=0
        )
        near_right[p] = project(right_rows[...], turned).reshape(chips, layers, GROUP * cols)
        mine = c * layers + pair
        for hop in hops:
            to = chip_at(*hop)
            send(
                near_right.at[p, to], met_right.at[p, mine], near_right_sems, p,
                core_at(to, z, side),
            )

        @pl.when(c == side)
        def _():
            met_right[p, mine] = near_right[p, a]

        @pl.when(c != side)
        def _():
            send(
                near_right.at[p, a], met_right.at[p, mine], near_right_sems, p,
                core_at(a, z, other),
            )

    def pass_right(p):
        settle_some(met_right, pl.ds(p, 1), near_right_sems.at[p])
        tiles = GROUP * cols // LANES

        def body(core, carry):
            for h in range(tiles):
                lanes = slice(h * LANES, (h + 1) * LANES)
                lines = turn_lanes([
                    met_right[p, core * layers + n, :, lanes].astype(F32) for n in range(layers)
                ])
                for n in range(layers):
                    at = (h * layers + n) * layers
                    turn_ref[at : at + layers, :] = lines[n]
            for h in range(parts):
                for n in range(layers):
                    line = turn_ref[pl.ds(h * GROUP * layers + n, GROUP, stride=layers), :]
                    far_right[p, n, core, h * GROUP : (h + 1) * GROUP, :] = line.astype(BF16)
            return carry

        with scope("rturn"):
            lax.fori_loop(0, CORES, body, 0)
        send_far(far_right, right_lines, right_sems, p, pl.ds(p, 1))

    def give_left(g):
        first, size = LEFTS[g]
        span = pl.ds(first, size)
        settle(got_left.at[span, pl.ds(0, layers - 1)], far_left_sems.at[g])
        with scope("lturn"):
            for u in range(first, first + size):
                for h in range(parts):
                    lanes = slice(h * LANES, (h + 1) * LANES)
                    lines = turn_lanes([
                        got_left[u, n, :, lanes] for n in range(layers)
                    ])
                    for n in range(UNIT):
                        at = (h * UNIT + n) * GROUP
                        turn_ref[at : at + GROUP, :] = lines[n].astype(F32)
                    for d in range(GROUP):
                        line = turn_ref[pl.ds(h * UNIT * GROUP + d, UNIT, stride=GROUP), :]
                        near_left[u, d, :, lanes] = line.astype(BF16)
        mine = c * chips + a
        for hop in hops:
            to = chip_at(*hop)
            send(
                near_left.at[span, to], left_lines.at[span, mine], left_sems, g,
                core_at(to, z, c),
            )
        left_lines[span, mine] = near_left[span, a]

    def pass_left(g):
        first, size = LEFTS[g]
        span = pl.ds(first, size)
        settle(left_lines.at[span, pl.ds(0, chips - 1)], left_sems.at[g])
        with scope("pass"):
            own = left_lines.at[span, pl.ds(c * chips, chips)]
            send(own, own, pass_sems, g, core_at(a, z, other))

    deep = near_left.shape[-1]

    met = set()

    def meet(g):
        first, size = BLOCKS[g]
        span = pl.ds(first, size)
        for at in range(first, first + size):
            p, q = at // parts, at % parts
            for n, (unit, many) in enumerate(LEFTS):
                if unit < (q + 1) * halves and ("left", n) not in met:
                    met.add(("left", n))
                    settle(left_lines.at[pl.ds(unit, many), pl.ds(0, chips)], pass_sems.at[n])
            if ("right", p) not in met:
                met.add(("right", p))
                settle(right_lines.at[p, pl.ds(0, layers - 1)], right_sems.at[p])
            with scope("meet"):
                total = None
                for core in range(CORES):
                    left = left_lines[
                        q * halves : (q + 1) * halves, core * chips : (core + 1) * chips
                    ].reshape(block, deep)
                    right = jnp.concatenate(
                        [
                            right_lines[p, :, core, h * GROUP : (h + 1) * GROUP, :].reshape(LANES, LANES)
                            for h in range(parts)
                        ],
                        axis=0,
                    )
                    term = jnp.dot(left, right, preferred_element_type=F32)
                    total = term if total is None else total + term
                mixed = (total * count ** (-0.5)).astype(BF16)
                for e in range(halves):
                    mix_send[at, :, e * UNIT : (e + 1) * UNIT, :] = mixed[
                        e * LANES : (e + 1) * LANES
                    ].reshape(chips, UNIT, LANES)
        for hop in hops:
            to = chip_at(*hop)
            send(
                mix_send.at[span, to], mix_recv.at[span, a], mix_sems, g, core_at(to, z, c)
            )
        mix_recv[span, a] = mix_send[span, a]

    def send_back(g, order):
        span = pl.ds(*BLOCKS[g])
        for n in order:
            to = n + (n + layers - z) // layers
            send(
                back_send.at[span, to], back_recv.at[span, z], back_sems, g, core_at(a, to, c)
            )

    def give_back(g):
        first, size = BLOCKS[g]
        span = pl.ds(first, size)
        settle(mix_recv.at[span, pl.ds(0, chips - 1)], mix_sems.at[g])
        with scope("back"):
            for at in range(first, first + size):
                for d in range(GROUP):
                    turn_ref[d * GROUP : (d + 1) * GROUP, :] = mix_recv[at, d].astype(F32)
                for e in range(halves):
                    lines = turn_lanes([
                        turn_ref[pl.ds(e * layers + n, GROUP, stride=GROUP), :].astype(BF16)
                        for n in range(layers)
                    ])
                    for n in range(layers):
                        back_send[at, n, :, e * LANES : (e + 1) * LANES] = lines[n]
        send_back(g, range(layers // 2))
        back_recv[span, z] = back_send[span, z]

    def give_high(g):
        send_back(g, range(layers // 2, layers - 1))

    def finish(g):
        first, size = BLOCKS[g]
        settle(back_recv.at[pl.ds(first, size), pl.ds(0, layers - 1)], back_sems.at[g])
        with scope("finish"):
            for at in range(first, first + size):
                p, q = at // parts, at % parts
                mixed = back_recv[at].reshape(width, block).astype(F32)
                centred = mixed - jnp.mean(mixed, axis=0, keepdims=True)
                scaled = centred * lax.rsqrt(
                    jnp.mean(centred * centred, axis=0, keepdims=True) + 1e-05
                )
                scaled = jnp.concatenate(
                    [scaled[:, e * LANES : (e + 1) * LANES] * mid_wide[...] for e in range(halves)],
                    axis=1,
                ).astype(BF16)
                result = lax.dot_general(
                    scaled, out_weight[...], (((0,), (0,)), ((), ())), preferred_element_type=F32
                )
                result = (result * gate_ref[p, q * block : (q + 1) * block, :]).astype(BF16)
                out_ref[
                    q * GROUP : (q + 1) * GROUP, p * GROUP : (p + 1) * GROUP, :
                ] = result.reshape(GROUP, GROUP, width)

    for p in range(parts):
        begin(p)
        if p == 0:
            with scope("bar"):
                pl.semaphore_wait(barrier, len(peers))
        for g, (first, size) in enumerate(LEFTS):
            if p * halves < first + size <= (p + 1) * halves:
                send_far(far_left, got_left, far_left_sems, g, pl.ds(first, size))
        begin_right(p)

    with scope("gate"):
        fetches[parts + 3].wait()
        for h in range(parts):
            gate_ref[h] = jax.nn.sigmoid(
                jnp.dot(ready_ref[h], out_gate[...], preferred_element_type=F32)
            )
        fetches[parts + 4].wait()
        mid_wide[...] = jnp.broadcast_to(mid_gain[...].reshape(1, width), (width, width)).T
        fetches[parts + 5].wait()

    for step in PLAN:
        todo = {
            "a": give_left, "r": pass_right, "f": pass_left, "m": meet, "c": give_back,
            "h": give_high, "d": finish,
        }[step[0]]
        todo(int(step[1:]))

    others = pl.ds(0, layers - 1)
    settle(far_left.at[:, others], sent(far_left_sems))
    settle(near_left.at[:, pl.ds(0, chips - 1)], sent(left_sems))
    settle(left_lines.at[:, pl.ds(0, chips)], sent(pass_sems))
    settle_some(met_right, pl.ds(0, parts), sent(near_right_sems))
    settle(far_right.at[:, others], sent(right_sems))
    settle(mix_send.at[:, pl.ds(0, chips - 1)], sent(mix_sems))
    settle(back_send.at[:, others], sent(back_sems))


def by_kernel(pair_state, in_gain, left_weight, right_weight, mid_gain, out_weight, out_gate):
    rows, cols, width = pair_state.shape
    chips = lax.axis_size("first")
    layers = lax.axis_size("second") // CORES
    count = cols * lax.axis_size("second")
    parts = rows // GROUP
    units = rows // UNIT
    block = GROUP * GROUP
    lanes = parts * block
    deep = parts * LANES
    changed = pl.pallas_call(
        functools.partial(triangle_kernel, layers, chips, count),
        out_shape=jax.ShapeDtypeStruct((rows, cols, width), BF16),
        in_specs=[pl.BlockSpec(memory_space=pltpu.MemorySpace.HBM)] * 7,
        out_specs=pl.BlockSpec(memory_space=pltpu.VMEM),
        scratch_shapes=[
            pltpu.VMEM((rows, cols, width), BF16),
            pltpu.VMEM((width,), F32),
            pltpu.VMEM(left_weight.shape, BF16),
            pltpu.VMEM(right_weight.shape, BF16),
            pltpu.VMEM((width,), F32),
            pltpu.VMEM(out_weight.shape, BF16),
            pltpu.VMEM(out_gate.shape, BF16),
            pltpu.SemaphoreType.DMA((parts + 6,)),
            pltpu.VMEM((width, width), BF16),
            pltpu.VMEM((width, width), BF16),
            pltpu.VMEM((width, width), F32),
            pltpu.VMEM((parts, GROUP * cols, width), F32),
            pltpu.VMEM((parts, rows * GROUP, width), BF16),
            pltpu.VMEM((parts, rows * GROUP, width), F32),
            pltpu.VMEM((cols * layers, LANES), F32),
            pltpu.VMEM((units, layers, GROUP, deep), BF16),
            pltpu.VMEM((units, layers, GROUP, deep), BF16),
            pltpu.VMEM((units, chips, UNIT, deep), BF16),
            pltpu.VMEM((units, CORES * chips, UNIT, deep), BF16),
            pltpu.VMEM((parts, chips, layers, lanes), BF16),
            pltpu.VMEM((parts, CORES * layers, layers, lanes), BF16),
            pltpu.VMEM((parts, layers, CORES, cols, LANES), BF16),
            pltpu.VMEM((parts, layers, CORES, cols, LANES), BF16),
            pltpu.VMEM((parts * parts, chips, GROUP, LANES), BF16),
            pltpu.VMEM((parts * parts, chips, GROUP, LANES), BF16),
            pltpu.VMEM((parts * parts, layers, GROUP, block), BF16),
            pltpu.VMEM((parts * parts, layers, GROUP, block), BF16),
            pltpu.SemaphoreType.DMA((len(LEFTS) + 1,)),
            pltpu.SemaphoreType.DMA((len(LEFTS) + 1,)),
            pltpu.SemaphoreType.DMA((len(LEFTS) + 1,)),
            pltpu.SemaphoreType.DMA((parts + 1,)),
            pltpu.SemaphoreType.DMA((parts + 1,)),
            pltpu.SemaphoreType.DMA((len(BLOCKS) + 1,)),
            pltpu.SemaphoreType.DMA((len(BLOCKS) + 1,)),
        ],
        compiler_params=pltpu.CompilerParams(
            collective_id=0, has_side_effects=True, vmem_limit_bytes=32 * 1024 * 1024
        ),
    )(
        *(
            pltpu.with_memory_space_constraint(value, pltpu.MemorySpace.HBM)
            for value in (
                pair_state, in_gain, left_weight, right_weight, mid_gain, out_weight, out_gate,
            )
        )
    )
    return changed


def unit_channels(values, channel_gain):
    centred = values - jnp.mean(values, axis=-1, keepdims=True)
    return (
        centred
        * lax.rsqrt(jnp.mean(centred * centred, axis=-1, keepdims=True) + 1e-05)
        * channel_gain
    )


def make_factors(pair_in, in_gain, left_weight, right_weight):
    ready = unit_channels(pair_in.astype(jnp.float32), in_gain).astype(jnp.bfloat16)
    ready = lax.optimization_barrier(ready)
    left = jnp.einsum("ijc,cd->ijd", ready, left_weight, preferred_element_type=jnp.float32)
    right = jnp.einsum("ijc,cd->ijd", ready, right_weight, preferred_element_type=jnp.float32)
    return (ready, left.astype(jnp.bfloat16), right.astype(jnp.bfloat16))


def finish_pair(mixed, ready, mid_gain, out_weight, out_gate):
    scaled = unit_channels(mixed.astype(jnp.float32), mid_gain).astype(jnp.bfloat16)
    scaled = lax.optimization_barrier(scaled)
    gate = jax.nn.sigmoid(
        jnp.einsum("ijc,cd->ijd", ready, out_gate, preferred_element_type=jnp.float32)
    )
    return (
        jnp.einsum("ijd,dc->ijc", scaled, out_weight, preferred_element_type=jnp.float32) * gate
    ).astype(jnp.bfloat16)


def by_collectives(pair_state, in_gain, left_weight, right_weight, mid_gain, out_weight, out_gate):
    ready, left, right = make_factors(pair_state, in_gain, left_weight, right_weight)
    count = pair_state.shape[1] * lax.axis_size("second")
    left_lines, right_lines = (
        lax.all_to_all(left, "second", split_axis=2, concat_axis=1, tiled=True),
        lax.all_to_all(right, "second", split_axis=2, concat_axis=1, tiled=True),
    )

    def meet(piece):
        return jnp.einsum("ikd,jkd->ijd", left_lines, piece, preferred_element_type=jnp.float32)

    strip = meet(lax.all_gather(right_lines, "first", axis=0, tiled=True))
    strip = (strip * count ** (-0.5)).astype(jnp.bfloat16)
    mixed = lax.all_to_all(strip, "second", split_axis=1, concat_axis=2, tiled=True)
    return finish_pair(mixed, ready, mid_gain, out_weight, out_gate)


def per_device(pair_state, *rest):
    groups, parts = lax.axis_size("first"), lax.axis_size("second")
    rows, cols, width = pair_state.shape
    left_out = rest[1].shape[1]
    fits = (
        groups == SIDE * SIDE
        and parts == CORES * 8
        and width == GROUP * 8
        and rows == cols
        and rows == 3 * GROUP
        and left_out == width
    )
    return (by_kernel if fits else by_collectives)(pair_state, *rest)


def solution(mesh):
    in_specs = (P("first", "second", None), P(), P(), P(), P(), P(), P())
    out_specs = P("first", "second", None)
    return jax.shard_map(
        per_device, mesh=mesh, in_specs=in_specs, out_specs=out_specs, check_vma=False
    )
```

```python
import functools

import jax
import jax.numpy as jnp
from jax import lax
from jax.experimental import pallas as pl
from jax.experimental.pallas import tpu as pltpu
from jax.sharding import PartitionSpec as P

MESH = pl.DeviceIdType.MESH
F32 = jnp.float32
BF16 = jnp.bfloat16
CORES = 2


SIDE = 4
LANES = 128
GROUP = 16
UNIT = 8
LEFTS = ((0, 1), (1, 1), (2, 1), (3, 1), (4, 1), (5, 1))
BLOCKS = ((0, 1), (1, 1), (2, 1), (3, 1), (4, 1), (5, 1), (6, 3))
PLAN = (
    "a0", "a1", "r0", "r1", "a2", "r2", "a3", "f0", "f1", "a4", "f2", "a5", "f3", "f4",
    "m0", "m1", "f5", "m2", "m3", "m4", "c0", "m5", "c1", "h0", "c2", "h1", "m6", "c3",
    "h2", "c4", "c5", "h3", "d0", "d1", "h4", "c6", "h5", "h6", "d2", "d3", "d4", "d5",
    "d6",
)


def unit_rows(values, channel_gain):
    centred = values - jnp.mean(values, axis=-1, keepdims=True)
    return (
        centred
        * lax.rsqrt(jnp.mean(centred * centred, axis=-1, keepdims=True) + 1e-05)
        * channel_gain
    )


def turn_lanes(parts):
    count = len(parts)
    wide = LANES // count
    group = lax.broadcasted_iota(jnp.int32, parts[0].shape, 1) // wide
    parts = list(parts)
    step = 1
    while step < count:
        low = group // step % 2 == 0
        for n in range(count):
            if n // step % 2 == 0:
                one, two = parts[n], parts[n + step]
                parts[n] = jnp.where(low, one, pltpu.roll(two, step * wide, 1))
                parts[n + step] = jnp.where(low, pltpu.roll(one, LANES - step * wide, 1), two)
        step *= 2
    return parts


def triangle_kernel(
    layers, chips, count,
    x_hbm, in_gain_hbm, left_weight_hbm, right_weight_hbm, mid_gain_hbm, out_weight_hbm,
    out_gate_hbm, out_ref,
    x_ref, in_gain, left_weight, right_weight, mid_gain, out_weight, out_gate, fetch_sems,
    left_rows, right_rows, mid_wide, whole_ref, ready_ref, gate_ref, turn_ref,
    far_left, got_left, near_left, left_lines,
    near_right, met_right, far_right, right_lines,
    mix_send, mix_recv, back_send, back_recv,
    far_left_sems, left_sems, pass_sems, near_right_sems, right_sems, mix_sems, back_sems,
):
    scope = jax.named_scope
    rows, cols, width = x_ref.shape
    parts = rows // GROUP
    units = rows // UNIT
    halves = GROUP // UNIT
    block = GROUP * GROUP
    a = lax.axis_index("first")
    b = lax.axis_index("second")
    z, c = b // CORES, b % CORES
    other = 1 - c
    y, x = a // SIDE, a % SIDE
    side = a % CORES
    pair = a // CORES

    def core_at(first, layer, core):
        return {"first": first, "second": layer * CORES + core}

    def layer_at(s):
        return lax.rem(z + s, layers)

    def chip_at(dy, dx):
        return lax.rem(y + dy, SIDE) * SIDE + lax.rem(x + dx, SIDE)

    hops = [(dy, dx) for dy in (2, 1, 3, 0) for dx in (2, 1, 3, 0) if (dy, dx) != (0, 0)]
    steps = [4, 3, 5, 2, 6, 1, 7]

    barrier = pltpu.get_barrier_semaphore()
    peers = [(0, core_at(a, z, other))]
    peers += [(min(s, layers - s), core_at(a, layer_at(s), c)) for s in steps]
    for dy, dx in hops:
        away = min(dy, SIDE - dy) + min(dx, SIDE - dx)
        peers += [(away, core_at(chip_at(dy, dx), z, core)) for core in (other, c)]
    peers = [peer for _, peer in sorted(peers, key=lambda pair: -pair[0])]
    for peer in peers:
        pl.semaphore_signal(barrier, inc=1, device_id=peer, device_id_type=MESH)

    fetches = [
        pltpu.make_async_copy(src, dst, fetch_sems.at[n])
        for n, (src, dst) in enumerate(
            [(x_hbm.at[pl.ds(p * GROUP, GROUP)], x_ref.at[pl.ds(p * GROUP, GROUP)]) for p in range(parts)]
            + [
                (in_gain_hbm, in_gain), (left_weight_hbm, left_weight),
                (right_weight_hbm, right_weight), (out_gate_hbm, out_gate),
                (mid_gain_hbm, mid_gain), (out_weight_hbm, out_weight),
            ]
        )
    ]
    for fetch in fetches:
        fetch.start()
    for fetch in fetches[parts : parts + 3]:
        fetch.wait()

    left_rows[...] = left_weight[...].astype(F32).T.astype(BF16)
    turn_ref[:width, :] = right_weight[...].astype(F32).T
    for d in range(chips):
        right_rows[d * layers : (d + 1) * layers, :] = turn_ref[
            pl.ds(d, layers, stride=chips), :
        ].astype(BF16)

    def send(src, dst, sems, at, peer):
        pltpu.make_async_remote_copy(
            src_ref=src, dst_ref=dst, send_sem=sems.at[sems.shape[0] - 1], recv_sem=sems.at[at],
            device_id=peer, device_id_type=MESH,
        ).start()

    def settle(like, sem):
        with scope("wait"):
            pltpu.make_async_copy(like, like, sem).wait()

    def settle_some(like, span, sem):
        @pl.when(c == side)
        def _():
            settle(like.at[span, pl.ds(0, chips - 1)], sem)

        @pl.when(c != side)
        def _():
            settle(like.at[span], sem)

    def sent(sems):
        return sems.at[sems.shape[0] - 1]

    def send_far(src, dst, sems, at, span):
        for s in steps:
            to = layer_at(s)
            send(src.at[span, to], dst.at[span, z], sems, at, core_at(a, to, c))
        dst[span, z] = src[span, z]

    def project(weight, lines):
        return lax.dot_general(
            weight, lines, (((1,), (1,)), ((), ())), preferred_element_type=F32
        ).astype(BF16)

    def begin(p):
        fetches[p].wait()
        values = x_ref[p * GROUP : (p + 1) * GROUP].astype(F32).reshape(GROUP * cols, width)
        ready = unit_rows(values, in_gain[...].reshape(1, width))
        whole_ref[p] = ready
        ready = ready.astype(BF16).reshape(GROUP, parts, GROUP, width)
        for h in range(parts):
            piece = ready[:, h].reshape(block, width)
            ready_ref[h, p * block : (p + 1) * block, :] = piece
            made = project(left_rows[...], piece)
            for e in range(halves):
                far_left[p * halves + e, :, :, h * LANES : (h + 1) * LANES] = made[
                    :, e * LANES : (e + 1) * LANES
                ].reshape(layers, GROUP, LANES)

    def begin_right(p):
        turned = jnp.concatenate(
            [whole_ref[p, pl.ds(k, GROUP, stride=cols), :].astype(BF16) for k in range(cols)], axis=0
        )
        near_right[p] = project(right_rows[...], turned).reshape(chips, layers, GROUP * cols)
        mine = c * layers + pair
        for hop in hops:
            to = chip_at(*hop)
            send(
                near_right.at[p, to], met_right.at[p, mine], near_right_sems, p,
                core_at(to, z, side),
            )

        @pl.when(c == side)
        def _():
            met_right[p, mine] = near_right[p, a]

        @pl.when(c != side)
        def _():
            send(
                near_right.at[p, a], met_right.at[p, mine], near_right_sems, p,
                core_at(a, z, other),
            )

    def pass_right(p):
        settle_some(met_right, pl.ds(p, 1), near_right_sems.at[p])
        tiles = GROUP * cols // LANES

        def body(core, carry):
            for h in range(tiles):
                lanes = slice(h * LANES, (h + 1) * LANES)
                lines = turn_lanes([
                    met_right[p, core * layers + n, :, lanes].astype(F32) for n in range(layers)
                ])
                for n in range(layers):
                    at = (h * layers + n) * layers
                    turn_ref[at : at + layers, :] = lines[n]
            for h in range(parts):
                for n in range(layers):
                    line = turn_ref[pl.ds(h * GROUP * layers + n, GROUP, stride=layers), :]
                    far_right[p, n, core, h * GROUP : (h + 1) * GROUP, :] = line.astype(BF16)
            return carry

        with scope("rturn"):
            lax.fori_loop(0, CORES, body, 0)
        send_far(far_right, right_lines, right_sems, p, pl.ds(p, 1))

    def give_left(g):
        first, size = LEFTS[g]
        span = pl.ds(first, size)
        settle(got_left.at[span, pl.ds(0, layers - 1)], far_left_sems.at[g])
        with scope("lturn"):
            for u in range(first, first + size):
                for h in range(parts):
                    lanes = slice(h * LANES, (h + 1) * LANES)
                    lines = turn_lanes([
                        got_left[u, n, :, lanes] for n in range(layers)
                    ])
                    for n in range(UNIT):
                        at = (h * UNIT + n) * GROUP
                        turn_ref[at : at + GROUP, :] = lines[n].astype(F32)
                    for d in range(GROUP):
                        line = turn_ref[pl.ds(h * UNIT * GROUP + d, UNIT, stride=GROUP), :]
                        near_left[u, d, :, lanes] = line.astype(BF16)
        mine = c * chips + a
        for hop in hops:
            to = chip_at(*hop)
            send(
                near_left.at[span, to], left_lines.at[span, mine], left_sems, g,
                core_at(to, z, c),
            )
        left_lines[span, mine] = near_left[span, a]

    def pass_left(g):
        first, size = LEFTS[g]
        span = pl.ds(first, size)
        settle(left_lines.at[span, pl.ds(0, chips - 1)], left_sems.at[g])
        with scope("pass"):
            own = left_lines.at[span, pl.ds(c * chips, chips)]
            send(own, own, pass_sems, g, core_at(a, z, other))

    deep = near_left.shape[-1]

    met = set()

    def meet(g):
        first, size = BLOCKS[g]
        span = pl.ds(first, size)
        for at in range(first, first + size):
            p, q = at // parts, at % parts
            for n, (unit, many) in enumerate(LEFTS):
                if unit < (q + 1) * halves and ("left", n) not in met:
                    met.add(("left", n))
                    settle(left_lines.at[pl.ds(unit, many), pl.ds(0, chips)], pass_sems.at[n])
            if ("right", p) not in met:
                met.add(("right", p))
                settle(right_lines.at[p, pl.ds(0, layers - 1)], right_sems.at[p])
            with scope("meet"):
                total = None
                for core in range(CORES):
                    left = left_lines[
                        q * halves : (q + 1) * halves, core * chips : (core + 1) * chips
                    ].reshape(block, deep)
                    right = jnp.concatenate(
                        [
                            right_lines[p, :, core, h * GROUP : (h + 1) * GROUP, :].reshape(LANES, LANES)
                            for h in range(parts)
                        ],
                        axis=0,
                    )
                    term = jnp.dot(left, right, preferred_element_type=F32)
                    total = term if total is None else total + term
                mixed = (total * count ** (-0.5)).astype(BF16)
                for e in range(halves):
                    mix_send[at, :, e * UNIT : (e + 1) * UNIT, :] = mixed[
                        e * LANES : (e + 1) * LANES
                    ].reshape(chips, UNIT, LANES)
        for hop in hops:
            to = chip_at(*hop)
            send(
                mix_send.at[span, to], mix_recv.at[span, a], mix_sems, g, core_at(to, z, c)
            )
        mix_recv[span, a] = mix_send[span, a]

    def send_back(g, order):
        span = pl.ds(*BLOCKS[g])
        for n in order:
            to = n + (n + layers - z) // layers
            send(
                back_send.at[span, to], back_recv.at[span, z], back_sems, g, core_at(a, to, c)
            )

    def give_back(g):
        first, size = BLOCKS[g]
        span = pl.ds(first, size)
        settle(mix_recv.at[span, pl.ds(0, chips - 1)], mix_sems.at[g])
        with scope("back"):
            for at in range(first, first + size):
                for d in range(GROUP):
                    turn_ref[d * GROUP : (d + 1) * GROUP, :] = mix_recv[at, d].astype(F32)
                for e in range(halves):
                    lines = turn_lanes([
                        turn_ref[pl.ds(e * layers + n, GROUP, stride=GROUP), :].astype(BF16)
                        for n in range(layers)
                    ])
                    for n in range(layers):
                        back_send[at, n, :, e * LANES : (e + 1) * LANES] = lines[n]
        send_back(g, range(layers // 2))
        back_recv[span, z] = back_send[span, z]

    def give_high(g):
        send_back(g, range(layers // 2, layers - 1))

    def finish(g):
        first, size = BLOCKS[g]
        settle(back_recv.at[pl.ds(first, size), pl.ds(0, layers - 1)], back_sems.at[g])
        with scope("finish"):
            for at in range(first, first + size):
                p, q = at // parts, at % parts
                mixed = back_recv[at].reshape(width, block).astype(F32)
                centred = mixed - jnp.mean(mixed, axis=0, keepdims=True)
                scaled = centred * lax.rsqrt(
                    jnp.mean(centred * centred, axis=0, keepdims=True) + 1e-05
                )
                scaled = jnp.concatenate(
                    [scaled[:, e * LANES : (e + 1) * LANES] * mid_wide[...] for e in range(halves)],
                    axis=1,
                ).astype(BF16)
                result = lax.dot_general(
                    scaled, out_weight[...], (((0,), (0,)), ((), ())), preferred_element_type=F32
                )
                result = (result * gate_ref[p, q * block : (q + 1) * block, :]).astype(BF16)
                out_ref[
                    q * GROUP : (q + 1) * GROUP, p * GROUP : (p + 1) * GROUP, :
                ] = result.reshape(GROUP, GROUP, width)

    for p in range(parts):
        begin(p)
        if p == 0:
            with scope("bar"):
                pl.semaphore_wait(barrier, len(peers))
        for g, (first, size) in enumerate(LEFTS):
            if p * halves < first + size <= (p + 1) * halves:
                send_far(far_left, got_left, far_left_sems, g, pl.ds(first, size))
        begin_right(p)

    with scope("gate"):
        fetches[parts + 3].wait()
        for h in range(parts):
            gate_ref[h] = jax.nn.sigmoid(
                jnp.dot(ready_ref[h], out_gate[...], preferred_element_type=F32)
            )
        fetches[parts + 4].wait()
        mid_wide[...] = jnp.broadcast_to(mid_gain[...].reshape(1, width), (width, width)).T
        fetches[parts + 5].wait()

    for step in PLAN:
        todo = {
            "a": give_left, "r": pass_right, "f": pass_left, "m": meet, "c": give_back,
            "h": give_high, "d": finish,
        }[step[0]]
        todo(int(step[1:]))

    others = pl.ds(0, layers - 1)
    settle(far_left.at[:, others], sent(far_left_sems))
    settle(near_left.at[:, pl.ds(0, chips - 1)], sent(left_sems))
    settle(left_lines.at[:, pl.ds(0, chips)], sent(pass_sems))
    settle_some(met_right, pl.ds(0, parts), sent(near_right_sems))
    settle(far_right.at[:, others], sent(right_sems))
    settle(mix_send.at[:, pl.ds(0, chips - 1)], sent(mix_sems))
    settle(back_send.at[:, others], sent(back_sems))


def by_kernel(pair_state, in_gain, left_weight, right_weight, mid_gain, out_weight, out_gate):
    rows, cols, width = pair_state.shape
    chips = lax.axis_size("first")
    layers = lax.axis_size("second") // CORES
    count = cols * lax.axis_size("second")
    parts = rows // GROUP
    units = rows // UNIT
    block = GROUP * GROUP
    lanes = parts * block
    deep = parts * LANES
    changed = pl.pallas_call(
        functools.partial(triangle_kernel, layers, chips, count),
        out_shape=jax.ShapeDtypeStruct((rows, cols, width), BF16),
        in_specs=[pl.BlockSpec(memory_space=pltpu.MemorySpace.HBM)] * 7,
        out_specs=pl.BlockSpec(memory_space=pltpu.VMEM),
        scratch_shapes=[
            pltpu.VMEM((rows, cols, width), BF16),
            pltpu.VMEM((width,), F32),
            pltpu.VMEM(left_weight.shape, BF16),
            pltpu.VMEM(right_weight.shape, BF16),
            pltpu.VMEM((width,), F32),
            pltpu.VMEM(out_weight.shape, BF16),
            pltpu.VMEM(out_gate.shape, BF16),
            pltpu.SemaphoreType.DMA((parts + 6,)),
            pltpu.VMEM((width, width), BF16),
            pltpu.VMEM((width, width), BF16),
            pltpu.VMEM((width, width), F32),
            pltpu.VMEM((parts, GROUP * cols, width), F32),
            pltpu.VMEM((parts, rows * GROUP, width), BF16),
            pltpu.VMEM((parts, rows * GROUP, width), F32),
            pltpu.VMEM((cols * layers, LANES), F32),
            pltpu.VMEM((units, layers, GROUP, deep), BF16),
            pltpu.VMEM((units, layers, GROUP, deep), BF16),
            pltpu.VMEM((units, chips, UNIT, deep), BF16),
            pltpu.VMEM((units, CORES * chips, UNIT, deep), BF16),
            pltpu.VMEM((parts, chips, layers, lanes), BF16),
            pltpu.VMEM((parts, CORES * layers, layers, lanes), BF16),
            pltpu.VMEM((parts, layers, CORES, cols, LANES), BF16),
            pltpu.VMEM((parts, layers, CORES, cols, LANES), BF16),
            pltpu.VMEM((parts * parts, chips, GROUP, LANES), BF16),
            pltpu.VMEM((parts * parts, chips, GROUP, LANES), BF16),
            pltpu.VMEM((parts * parts, layers, GROUP, block), BF16),
            pltpu.VMEM((parts * parts, layers, GROUP, block), BF16),
            pltpu.SemaphoreType.DMA((len(LEFTS) + 1,)),
            pltpu.SemaphoreType.DMA((len(LEFTS) + 1,)),
            pltpu.SemaphoreType.DMA((len(LEFTS) + 1,)),
            pltpu.SemaphoreType.DMA((parts + 1,)),
            pltpu.SemaphoreType.DMA((parts + 1,)),
            pltpu.SemaphoreType.DMA((len(BLOCKS) + 1,)),
            pltpu.SemaphoreType.DMA((len(BLOCKS) + 1,)),
        ],
        compiler_params=pltpu.CompilerParams(
            collective_id=0, has_side_effects=True, vmem_limit_bytes=32 * 1024 * 1024
        ),
    )(
        *(
            pltpu.with_memory_space_constraint(value, pltpu.MemorySpace.HBM)
            for value in (
                pair_state, in_gain, left_weight, right_weight, mid_gain, out_weight, out_gate,
            )
        )
    )
    return changed


def unit_channels(values, channel_gain):
    centred = values - jnp.mean(values, axis=-1, keepdims=True)
    return (
        centred
        * lax.rsqrt(jnp.mean(centred * centred, axis=-1, keepdims=True) + 1e-05)
        * channel_gain
    )


def make_factors(pair_in, in_gain, left_weight, right_weight):
    ready = unit_channels(pair_in.astype(jnp.float32), in_gain).astype(jnp.bfloat16)
    ready = lax.optimization_barrier(ready)
    left = jnp.einsum("ijc,cd->ijd", ready, left_weight, preferred_element_type=jnp.float32)
    right = jnp.einsum("ijc,cd->ijd", ready, right_weight, preferred_element_type=jnp.float32)
    return (ready, left.astype(jnp.bfloat16), right.astype(jnp.bfloat16))


def finish_pair(mixed, ready, mid_gain, out_weight, out_gate):
    scaled = unit_channels(mixed.astype(jnp.float32), mid_gain).astype(jnp.bfloat16)
    scaled = lax.optimization_barrier(scaled)
    gate = jax.nn.sigmoid(
        jnp.einsum("ijc,cd->ijd", ready, out_gate, preferred_element_type=jnp.float32)
    )
    return (
        jnp.einsum("ijd,dc->ijc", scaled, out_weight, preferred_element_type=jnp.float32) * gate
    ).astype(jnp.bfloat16)


def by_collectives(pair_state, in_gain, left_weight, right_weight, mid_gain, out_weight, out_gate):
    ready, left, right = make_factors(pair_state, in_gain, left_weight, right_weight)
    count = pair_state.shape[1] * lax.axis_size("second")
    left_lines, right_lines = (
        lax.all_to_all(left, "second", split_axis=2, concat_axis=1, tiled=True),
        lax.all_to_all(right, "second", split_axis=2, concat_axis=1, tiled=True),
    )

    def meet(piece):
        return jnp.einsum("ikd,jkd->ijd", left_lines, piece, preferred_element_type=jnp.float32)

    strip = meet(lax.all_gather(right_lines, "first", axis=0, tiled=True))
    strip = (strip * count ** (-0.5)).astype(jnp.bfloat16)
    mixed = lax.all_to_all(strip, "second", split_axis=1, concat_axis=2, tiled=True)
    return finish_pair(mixed, ready, mid_gain, out_weight, out_gate)


def per_device(pair_state, *rest):
    groups, parts = lax.axis_size("first"), lax.axis_size("second")
    rows, cols, width = pair_state.shape
    left_out = rest[1].shape[1]
    fits = (
        groups == SIDE * SIDE
        and parts == CORES * 8
        and width == GROUP * 8
        and rows == cols
        and rows == 3 * GROUP
        and left_out == width
    )
    return (by_kernel if fits else by_collectives)(pair_state, *rest)


def solution(mesh):
    in_specs = (P("first", "second", None), P(), P(), P(), P(), P(), P())
    out_specs = P("first", "second", None)
    return jax.shard_map(
        per_device, mesh=mesh, in_specs=in_specs, out_specs=out_specs, check_vma=False
    )
```
